32 devices in a mesh: ang: 4 (over y, x), rad: 8 (over z, core).
Axes of the slice: x: 2, y: 2, z: 4, core: 2. Of those that a mesh axis runs over, the one named last changes fastest.
Arguments:
- right_side: float32 [1024, 4096], P('rad', 'ang'), may hold values from -6 to 7
- guess: float32 [1024, 4096], P('rad', 'ang'), may hold values from -6 to 6
Outputs:
- solution: float32 [1024, 4096], P('rad', 'ang')
- residual: float32 [1024, 4096], P('rad', 'ang')
The draws below stay inside these ranges and needn't reach their ends.
All inputs are finite; a program needn't handle non-finite values.
Results may differ from the reference program's by a relative error of at most 0.007.
Values sent between devices are 32-bit elements; how exact they have to be, the bound alone decides.
A program may use at most 128 MiB of HBM per device.

```python
import math
import jax
import jax.numpy as jnp

LEVELS = 8
PRE = 2
POST = 2
COARSE_SWEEPS = 8
NR = 1024
NT = 4096


def draw_right_side(key, part):
    rough_part = jnp.clip(jax.random.normal(key, (NR, NT), jnp.float32), -6.0, 6.0)
    return rough_part


def levels(key, dims, cuts, low, top_value):
    gain, own = 1.0, jax.random.fold_in(key, 6)
    for position, blocks in cuts:
        steps = jnp.exp(jax.random.uniform(jax.random.fold_in(own, position), (blocks,), jnp.float32, low / len(cuts), top_value / len(cuts)))
        gain = gain * jnp.repeat(steps, dims[position] // blocks).reshape([-1 if axis == position else 1 for axis in range(len(dims))])
    return gain


def normal_values(rng, extent, width, most, pieces=(), kind=jnp.bfloat16):
    gain = levels(rng, extent, pieces, -0.22, 0.18) if pieces else 1.0
    array = jax.random.normal(rng, extent, jnp.float32) * width * gain
    return jnp.minimum(jnp.maximum(array, -most), most).astype(kind)


def setup_inputs(seed: int = 0) -> dict:
    seeds = jax.random.split(jax.random.key(seed), 3)
    return {
        "right_side": draw_right_side(jax.random.fold_in(seeds[2], 71), 0),
        "guess": normal_values(seeds[1], (NR, NT), 1.0, 6.0, ((0, 8), (1, 4)), jnp.float32),
    }


def coefficients(row_float, spacing):
    radius = 1.0 + (row_float + 0.5) * spacing
    offset_ratio = 0.5 * spacing / radius
    outward = 1.0 + offset_ratio
    inward = 1.0 - offset_ratio
    angular = 1.0 / (radius * radius)
    centre = 2.0 + 2.0 * angular
    return outward, inward, angular, centre


def relax_cells(padded, source, stencil, chosen):
    outward, inward, angular, centre = stencil
    middle = padded[1:-1, 1:-1]
    updated = (source + outward * padded[2:, 1:-1] + inward * padded[:-2, 1:-1]
               + angular * (padded[1:-1, 2:] + padded[1:-1, :-2])) / centre
    return jnp.where(chosen, updated, middle)


def apply_operator(padded, stencil):
    outward, inward, angular, centre = stencil
    middle = padded[1:-1, 1:-1]
    return (centre * middle - outward * padded[2:, 1:-1] - inward * padded[:-2, 1:-1]
            - angular * (padded[1:-1, 2:] + padded[1:-1, :-2]))


def restrict_grid(padded):
    height = padded.shape[0] - 2
    breadth = padded.shape[1] - 2
    row_sum = (padded[0:height:2] + 3.0 * padded[1:height + 1:2] + 3.0 * padded[2:height + 2:2]
               + padded[3:height + 3:2]) * 0.125
    col_sum = (row_sum[:, 0:breadth:2] + 3.0 * row_sum[:, 1:breadth + 1:2] + 3.0 * row_sum[:, 2:breadth + 2:2]
               + row_sum[:, 3:breadth + 3:2]) * 0.125
    return 4.0 * col_sum


def prolong_grid(padded):
    centre_rep = jnp.repeat(padded[1:-1], 2, axis=0)
    below_rep = jnp.repeat(padded[:-2], 2, axis=0)
    above_rep = jnp.repeat(padded[2:], 2, axis=0)
    row_ids = jnp.arange(centre_rep.shape[0], dtype=jnp.int32)[:, None]
    stretched = 0.75 * centre_rep + 0.25 * jnp.where(row_ids % 2 == 0, below_rep, above_rep)
    mid_cols = jnp.repeat(stretched[:, 1:-1], 2, axis=1)
    left_cols = jnp.repeat(stretched[:, :-2], 2, axis=1)
    right_cols = jnp.repeat(stretched[:, 2:], 2, axis=1)
    col_ids = jnp.arange(mid_cols.shape[1], dtype=jnp.int32)[None, :]
    return 0.75 * mid_cols + 0.25 * jnp.where(col_ids % 2 == 0, left_cols, right_cols)


def wrap_pad(values, margin):
    values = jnp.pad(values, ((0, 0), (margin, margin)), mode="wrap")
    return jnp.pad(values, ((margin, margin), (0, 0)))


def cycle_local(level_at, iterate, source):
    height, breadth = source.shape
    spacing = 2.0 * math.pi / breadth
    row_ids = jnp.arange(height, dtype=jnp.int32)[:, None]
    col_ids = jnp.arange(breadth, dtype=jnp.int32)[None, :]
    stencil = coefficients(row_ids.astype(jnp.float32), spacing)
    red_cells = (row_ids + col_ids) % 2 == 0
    black_cells = jnp.logical_not(red_cells)

    def colour_sweep(values):
        values = relax_cells(wrap_pad(values, 1), source, stencil, red_cells)
        return relax_cells(wrap_pad(values, 1), source, stencil, black_cells)

    if level_at == LEVELS - 1:
        for _ in range(COARSE_SWEEPS):
            iterate = colour_sweep(iterate)
        return iterate
    for _ in range(PRE):
        iterate = colour_sweep(iterate)
    remainder = source - apply_operator(wrap_pad(iterate, 1), stencil)
    coarse_source = restrict_grid(wrap_pad(remainder, 1))
    correction = cycle_local(level_at + 1, jnp.zeros_like(coarse_source), coarse_source)
    iterate = iterate + prolong_grid(wrap_pad(correction, 1))
    for _ in range(POST):
        iterate = colour_sweep(iterate)
    return iterate


def reference(right_side, guess):
    solution = cycle_local(0, guess, right_side)
    height, breadth = right_side.shape
    row_ids = jnp.arange(height, dtype=jnp.int32)[:, None]
    stencil = coefficients(row_ids.astype(jnp.float32), 2.0 * math.pi / breadth)
    residual = right_side - apply_operator(wrap_pad(solution, 1), stencil)
    return solution, residual
```

```python
import math

import jax
import jax.numpy as jnp
from jax import lax
from jax.experimental import pallas as pl
from jax.experimental.pallas import tpu as pltpu
from jax.sharding import PartitionSpec as P

LEVELS = 8
PRE = 2
POST = 2
COARSE_SWEEPS = 8
F32 = jnp.float32
MESH = pl.DeviceIdType.MESH
HALO = 16


def one_hot(rows, cols, source):
    r = lax.broadcasted_iota(jnp.int32, (rows, cols), 0)
    c = lax.broadcasted_iota(jnp.int32, (rows, cols), 1)
    return jnp.where(r == source(c), 1.0, 0.0).astype(jnp.bfloat16)


def permute(x, table):
    hi = x.astype(jnp.bfloat16)
    rest = x - hi.astype(F32)
    mid = rest.astype(jnp.bfloat16)
    low = (rest - mid.astype(F32)).astype(jnp.bfloat16)
    n = x.shape[0]
    y = jnp.dot(jnp.concatenate([hi, mid, low], axis=0), table, preferred_element_type=F32)
    return (y[:n] + y[n:2 * n]) + y[2 * n:]


def wide(c, lanes):
    return jnp.concatenate([c] * (lanes // c.shape[1]), axis=1) if lanes > c.shape[1] else c


def roll(x, shift, axis):
    return pltpu.roll(x, shift % x.shape[axis], axis)


class Grid:
    def __init__(self, v, g, c, nr, nc, closed):
        self.v, self.g, self.c, self.nr, self.nc, self.closed = v, g, c, nr, nc, closed

    def rows_shift(self, x, d):
        y = roll(x, -d, 0)
        if self.closed:
            s = lax.broadcasted_iota(jnp.int32, x.shape, 0)
            y = jnp.where(s == (x.shape[0] - 1 if d > 0 else 0), 0.0, y)
        return y

    def up(self, a, gi, gj):
        return a[gi + 1, gj] if gi + 1 < self.nr else self.rows_shift(a[0, gj], 1)

    def down(self, a, gi, gj):
        return a[gi - 1, gj] if gi > 0 else self.rows_shift(a[self.nr - 1, gj], -1)

    def right(self, a, gi, gj):
        return a[gi, gj + 1] if gj + 1 < self.nc else roll(a[gi, 0], -1, 1)

    def left(self, a, gi, gj):
        return a[gi, gj - 1] if gj > 0 else roll(a[gi, self.nc - 1], 1, 1)

    def coef(self, k, gi):
        return wide(self.c[k, gi], self.v.shape[-1])

    def update(self, gi, gj):
        v = self.v
        return (self.coef(0, gi) * self.g[gi, gj] + self.coef(1, gi) * self.up(v, gi, gj)
                + self.coef(2, gi) * self.down(v, gi, gj)
                + self.coef(3, gi) * (self.right(v, gi, gj) + self.left(v, gi, gj)))

    def half(self, parity, first=False):
        for gi in range(self.nr):
            for gj in range(self.nc):
                if (gi + gj) % 2 == parity:
                    if first:
                        self.v[gi, gj] = self.coef(0, gi) * self.g[gi, gj]
                    else:
                        self.v[gi, gj] = self.update(gi, gj)

    def sweeps(self, count, zero):
        if zero:
            self.half(0, True)
            self.half(1)
            count -= 1

        def body(_, carry):
            self.half(0)
            self.half(1)
            return carry

        if count:
            lax.fori_loop(0, count, body, 0)

    def restrict(self, res, tmp, out):
        nr, nc = self.nr, self.nc
        for gi in range(nr):
            for gj in range(nc):
                if (gi + gj) % 2 == 0:
                    res[gi, gj] = self.coef(4, gi) * (self.update(gi, gj) - self.v[gi, gj])
        for big in range(nr // 2):
            for gj in range(nc):
                if gj % 2 == 0:
                    a, b = 3.0 * res[2 * big, gj], self.up(res, 2 * big + 1, gj)
                else:
                    a, b = 3.0 * res[2 * big + 1, gj], self.down(res, 2 * big, gj)
                tmp[big, gj] = (a + b) * 0.125
        for big in range(nr // 2):
            for col in range(nc // 2):
                inner = 3.0 * (tmp[big, 2 * col] + tmp[big, 2 * col + 1])
                outer = self.left(tmp, big, 2 * col) + self.right(tmp, big, 2 * col + 1)
                out(big, col, (inner + outer) * 0.5)

    def add_prolonged(self, coarse, tmp, mask, fit=lambda x: x):
        e = coarse.v
        for gi in range(self.nr):
            for col in range(coarse.nc):
                near = e[gi // 2, col]
                far = coarse.down(e, gi // 2, col) if gi % 2 == 0 else coarse.up(e, gi // 2, col)
                value = fit(0.75 * near + 0.25 * far)
                if mask:
                    value = value * self.coef(5, gi)
                tmp[gi, col] = value
        for gi in range(self.nr):
            for gj in range(self.nc):
                near = tmp[gi, gj // 2]
                far = coarse.left(tmp, gi, gj // 2) if gj % 2 == 0 else coarse.right(tmp, gi, gj // 2)
                self.v[gi, gj] = self.v[gi, gj] + (0.75 * near + 0.25 * far)


def fill_coefficients(c, nr, rows_per_group, start, total, spacing, wrap):
    for gi in range(nr):
        s = lax.broadcasted_iota(jnp.int32, (rows_per_group, 128), 0)
        if wrap:
            s = jnp.where(s >= wrap, s - rows_per_group, s)
        row = start + nr * s + gi
        inside = jnp.logical_and(row >= 0, row < total)
        radius = 1.0 + (jnp.where(inside, row, 0).astype(F32) + 0.5) * spacing
        ratio = 0.5 * spacing / radius
        angular = 1.0 / (radius * radius)
        centre = 2.0 + 2.0 * angular
        zero = jnp.zeros_like(radius)
        for k, value in enumerate((1.0 / centre, (1.0 + ratio) / centre, (1.0 - ratio) / centre,
                                   angular / centre, centre, jnp.ones_like(radius))):
            c[k, gi] = jnp.where(inside, value, zero)


def kernel(na, nrad, h, w, rs_in, gs_in, sol, resid, rs, gs, load_sem,
           rowbuf, pack, colbuf, s1, q1, t1, u1, stage, v0, g0, c0, v1, g1, c1, v2, g2, c2, v3, c3, wv, wg, tmp_res, tmp_mid,
           gat, rows3, nat3, a3, b3, d3, a4, b4, d4, a5, b5, d5, a6, b6, d6, a7, b7, d7, t3, u3,
           row_send, row_recv, col_send, col_recv, row1_send, row1_recv, col1_send, col1_recv, all_send, all_recv):
    a, r = lax.axis_index("ang"), lax.axis_index("rad")
    ar, al = lax.rem(a + 1, na), lax.rem(a + na - 1, na)
    lanes = w // 8
    ext = lanes + 128
    tiles = lanes // 128
    spacing = [2.0 * math.pi / (w * na >> l) for l in range(LEVELS)]
    lane = lambda shape: lax.broadcasted_iota(jnp.int32, shape, 1)

    loads = [pltpu.make_async_copy(src, dst, load_sem.at[k]) for k, (src, dst) in enumerate(((gs_in, gs), (rs_in, rs)))]
    for cp in loads:
        cp.start()
    blk = h // 8
    s0 = blk + 8
    total = na * nrad
    barrier = pltpu.get_barrier_semaphore()

    others = sorted(((da, dr) for da in range(na) for dr in range(nrad) if da or dr),
                    key=lambda d: -min(d[1], nrad - d[1]))
    for da, dr in others:
        pl.semaphore_signal(barrier, inc=1, device_id=(lax.rem(a + da, na), lax.rem(r + dr, nrad)), device_id_type=MESH)

    for l, c in ((0, c0), (1, c1), (2, c2)):
        fill_coefficients(c, 8 >> l, s0 if l == 0 else blk + 16, r * (h >> l), (h * nrad) >> l, spacing[l], blk + 4 if l == 0 else blk + 8)
    for l, d, n in ((3, d3, 16), (4, d4, 8), (5, d5, 4), (6, d6, 2), (7, d7, 1)):
        fill_coefficients(d, n, nrad, 0, (h * nrad) >> l, spacing[l], 0)

    for cp in loads:
        cp.wait()

    fold = h // 4
    place16 = lane((fold, 128)) // 16
    for p, (tile, base) in enumerate(((0, 0), (w - 128, 16))):
        folded = None
        for q in range(4):
            for k, x in enumerate((gs, rs)):
                piece = roll(x[q * fold:(q + 1) * fold, tile:tile + 128], 32 * q + 16 * k + base, 1)
                folded = piece if folded is None else jnp.where(place16 == 2 * q + k, piece, folded)
        pack[p] = folded

    def copy(src, dst, send, recv, to_a, to_r):
        return pltpu.make_async_remote_copy(src_ref=src, dst_ref=dst, send_sem=send, recv_sem=recv,
                                            device_id=(to_a, to_r), device_id_type=MESH)

    def row_copies(side):
        to_r = r - 1 if side == 0 else r + 1
        rows = pl.ds(0, HALO) if side == 0 else pl.ds(h - HALO, HALO)
        made = [copy(x.at[rows, :], rowbuf.at[k, side], row_send.at[k, side], row_recv.at[k, side], a, to_r)
                for k, x in enumerate((gs, rs))]
        for p, to_a in ((0, al), (1, ar)):
            made.append(copy(pack.at[p, pl.ds(side * (fold - HALO), HALO), :], colbuf.at[p, pl.ds(fold + side * HALO, HALO), :],
                             col_send.at[p, 1 + side], col_recv.at[p, 1 + side], to_a, to_r))
        return made

    pl.semaphore_wait(barrier, total - 1)
    ends = (r > 0, r < nrad - 1)
    for side in range(2):
        @pl.when(ends[side])
        def _():
            for cp in row_copies(side):
                cp.start()
    straight = [copy(pack.at[p], colbuf.at[p, pl.ds(0, fold), :], col_send.at[p, 0], col_recv.at[p, 0], to_a, r)
                for p, to_a in ((0, al), (1, ar))]
    for cp in straight:
        cp.start()

    spread = one_hot(256, 256, lambda c: 8 * (c % 32) + c // 32)
    halo_spread = [one_hot(128, 1024, lambda c, k=k: jnp.where(
        c % 128 < 2, 16 * k + 8 * (c % 128) + c // 128,
        jnp.where(c % 128 >= 126, 32 + 16 * k + 8 * (c % 128 - 126) + c // 128, -1))) for k in range(2)]

    def split_rows(x, count, put):
        ln = lane((count, 128)) // 32
        for t in range(tiles):
            parts = [permute(x(slice((4 * t + b) * 256, (4 * t + b) * 256 + 256)), spread) for b in range(4)]
            for gj in range(8):
                o = None
                for b in range(4):
                    half = parts[b][:, (gj // 4) * 128:(gj // 4) * 128 + 128]
                    piece = roll(half, 32 * (b - gj % 4), 1)
                    o = piece if o is None else jnp.where(ln == b, piece, o)
                put(gj, t, o)

    def put_own(k):
        def put(gj, t, value):
            stage[k, gj, t, pl.ds(0, h), :] = value
        return put

    for k, x in enumerate((gs, rs)):
        split_rows(lambda cols, x=x: x[:, cols], h, put_own(k))

    for side in range(2):
        @pl.when(ends[1 - side])
        def _():
            for cp in row_copies_in(side, rowbuf, colbuf, copy, row_send, row_recv, col_send, col_recv, gs, rs, pack, h, a, r):
                cp.wait_recv()
    for cp in straight:
        cp.wait_recv()
    at = (h, 8 * s0 - HALO)
    for k in range(2):
        for gj in range(8):
            for t in range(tiles + 1):
                stage[k, gj, t, pl.ds(h + HALO, 8 * s0 - h - 2 * HALO), :] = jnp.zeros((8 * s0 - h - 2 * HALO, 128), F32)
    def put_edges(gj, t, value):
        for k in range(2):
            for side in range(2):
                n = 2 * k + side
                stage[k, gj, t, pl.ds(at[side], HALO), :] = value[n * HALO:(n + 1) * HALO]

    split_rows(lambda cols: jnp.concatenate(
        [jnp.where(ends[1 - side], rowbuf[k, side, :, cols], 0.0) for k in range(2) for side in range(2)], axis=0),
        4 * HALO, put_edges)

    def beside(first, count, shift):
        right, left = colbuf[0, pl.ds(first, count), :], colbuf[1, pl.ds(first, count), :]
        return jnp.where(lane((count, 128)) < 32, roll(right, -shift, 1), roll(left, 32 - shift, 1))

    strips = [beside(0, fold, 32 * q) for q in range(4)]
    strips.append(jnp.where(ends[1], beside(fold, HALO, 0), 0.0))
    strips.append(jnp.where(ends[0], beside(fold + HALO, HALO, 96), 0.0))
    strips = jnp.concatenate(strips, axis=0)
    for k in range(2):
        y = permute(strips, halo_spread[k])
        for gj in range(8):
            cols = slice(gj * 128, gj * 128 + 128)
            stage[k, gj, tiles, pl.ds(0, h + HALO), :] = y[0:h + HALO, cols]
            stage[k, gj, tiles, pl.ds(at[1], HALO), :] = y[h + HALO:, cols]
    for k, dst in enumerate((v0, g0)):
        for gj in range(8):
            for gi in range(8):
                for t in range(tiles + 1):
                    dst[gi, gj, :, t * 128:t * 128 + 128] = stage[k, gj, t, pl.ds(gi, s0, stride=8), :]

    fine = Grid(v0, g0, c0, 8, 8, False)
    middle = Grid(v1, g1, c1, 4, 4, False)
    coarse = Grid(v2, g2, c2, 2, 2, False)
    window = Grid(v3, None, None, 1, 1, False)

    def into(ref):
        def put(gi, gj, value):
            ref[gi, gj] = value
        return put

    fine.sweeps(PRE, False)

    def put1(gi, gj, value):
        g1[gi, gj, 0:blk, 0:lanes] = value[0:blk, 0:lanes]
    fine.restrict(tmp_res, tmp_mid, put1)

    for side, first in ((0, blk), (1, blk + 8)):
        @pl.when(jnp.logical_not(ends[1 - side]))
        def _():
            g1[:, :, first:first + 8, 0:lanes] = jnp.zeros((4, 4, 8, lanes), F32)
    slot = lane((blk, 128)) // 8
    left_edge = right_edge = None
    for g in range(16):
        lo = roll(g1[g // 4, g % 4, 0:blk, 0:128], 8 * g, 1)
        hi = roll(g1[g // 4, g % 4, 0:blk, lanes - 128:lanes], 8 * g + 8, 1)
        left_edge = lo if g == 0 else jnp.where(slot == g, lo, left_edge)
        right_edge = hi if g == 0 else jnp.where(slot == g, hi, right_edge)
    s1[0] = left_edge
    s1[1] = right_edge

    def copies1(side, to_r):
        first = 0 if side == 0 else blk - 8
        made = [copy(g1.at[:, :, pl.ds(first, 8), pl.ds(0, lanes)], g1.at[:, :, pl.ds(blk + 8 * side, 8), pl.ds(0, lanes)],
                     row1_send.at[side], row1_recv.at[side], a, to_r)]
        for p, to_a in ((0, al), (1, ar)):
            made.append(copy(s1.at[p, pl.ds(first, 8), :], q1.at[p, pl.ds(blk + 8 * side, 8), :],
                             col1_send.at[p, 1 + side], col1_recv.at[p, 1 + side], to_a, to_r))
        return made

    straight1 = [copy(s1.at[p], q1.at[p, pl.ds(0, blk), :], col1_send.at[p, 0], col1_recv.at[p, 0], to_a, r)
                 for p, to_a in ((0, al), (1, ar))]
    for side in range(2):
        @pl.when(ends[side])
        def _():
            for cp in copies1(side, r - 1 if side == 0 else r + 1):
                cp.start()
    for cp in straight1:
        cp.start()
    for side in range(2):
        @pl.when(ends[1 - side])
        def _():
            for cp in copies1(side, r + 1 if side == 0 else r - 1):
                cp.wait_recv()
    for cp in straight1:
        cp.wait_recv()
    wl = lane((blk + 16, 128))
    sub = lax.broadcasted_iota(jnp.int32, (blk + 16, 128), 0)
    got = jnp.where(sub < blk, 1, jnp.where(sub < blk + 8, nrad - 1 - r, r)) > 0
    strip_r, strip_l = jnp.where(got, q1[0], 0.0), jnp.where(got, q1[1], 0.0)
    for g in range(16):
        g1[g // 4, g % 4, :, lanes:ext] = jnp.where(
            wl < 8, roll(strip_r, -8 * g, 1), jnp.where(wl >= 120, roll(strip_l, 120 - 8 * g, 1), 0.0))
    middle.sweeps(PRE, True)
    middle.restrict(t1, u1, into(g2))
    coarse.sweeps(PRE, True)

    def put3(gi, gj, value):
        wv[...] = value[0:blk, 0:lanes]
    coarse.restrict(t1, u1, put3)

    place = gat.at[a, pl.ds(pl.multiple_of(r * blk, 8), blk), :]
    gat[a, pl.ds(pl.multiple_of(r * blk, 8), blk), :] = wv[...]

    def hand(da, dr):
        step = da * nrad + dr
        return copy(wv, place, all_send.at[step], all_recv.at[step], lax.rem(a + da, na), lax.rem(r + dr, nrad))

    for d in others:
        hand(*d).start()
    for d in others:
        hand(*d).wait_recv()

    w3 = lanes * na
    q3 = w3 // 4
    for aa in range(na):
        for t in range(tiles):
            rows3[aa * tiles + t] = gat[aa, :, t * 128:t * 128 + 128]
    stacked = jnp.concatenate([jnp.concatenate(
        [rows3[t, pl.ds(gi, nrad, stride=16), :] for t in range(na * tiles)], axis=1) for gi in range(16)], axis=0)
    table3 = one_hot(w3, w3, lambda c: 4 * (c % q3) + c // q3)
    by_group = permute(stacked, table3)
    for gi in range(16):
        for gj in range(4):
            b3[gi, gj] = by_group[gi * nrad:(gi + 1) * nrad, gj * q3:(gj + 1) * q3]

    l3 = Grid(a3, b3, d3, 16, 4, True)
    l4 = Grid(a4, b4, d4, 8, 2, True)
    l5 = Grid(a5, b5, d5, 4, 4, True)
    l6 = Grid(a6, b6, d6, 2, 2, True)
    l3.sweeps(PRE, True)
    l3.restrict(t3, u3, into(b4))
    l4.sweeps(PRE, True)
    w5 = w3 // 4
    q5 = w5 // 4
    nat5 = {}

    def put5(gi, gj, value):
        nat5[gi] = value
    l4.restrict(t3, u3, put5)
    x5 = permute(jnp.concatenate([nat5[i] for i in range(4)], axis=0),
                 one_hot(w5, 512, lambda c: 4 * (c % q5) + c // 128))
    for gi in range(4):
        for gj in range(4):
            b5[gi, gj] = x5[gi * nrad:(gi + 1) * nrad, gj * 128:gj * 128 + 128]
    l5.sweeps(PRE, True)
    l5.restrict(tmp_small(t3), tmp_small(u3), into(b6))
    l6.sweeps(PRE, True)
    l6.restrict(tmp_small(t3), tmp_small(u3), into(b7))
    l7 = Grid(a7, b7, d7, 1, 1, True)
    red = (lax.broadcasted_iota(jnp.int32, (nrad, 128), 0) + lane((nrad, 128))) % 2 == 0
    a7[0, 0] = jnp.zeros((nrad, 128), F32)

    def coarsest(_, carry):
        a7[0, 0] = jnp.where(red, l7.update(0, 0), a7[0, 0])
        a7[0, 0] = jnp.where(red, a7[0, 0], l7.update(0, 0))
        return carry
    lax.fori_loop(0, COARSE_SWEEPS, coarsest, 0)

    l6.add_prolonged(l7, tmp_small(t3), False)
    l6.sweeps(POST, False)
    l5.add_prolonged(l6, tmp_small(t3), False)
    l5.sweeps(POST, False)
    y5 = None
    for gj in range(4):
        x = jnp.concatenate([a5[gi, gj] for gi in range(4)], axis=0)
        r0 = permute(x, one_hot(128, w5, lambda c, gj=gj: jnp.where(c % 4 == gj, c // 4, -1)))
        y5 = r0 if y5 is None else y5 + r0
    for gi in range(4):
        u3[gi, 0] = y5[gi * nrad:(gi + 1) * nrad]
    l4.add_prolonged(Grid(u3, None, None, 4, 1, True), t3, False)
    l4.sweeps(POST, False)
    l3.add_prolonged(l4, t3, False)
    l3.sweeps(POST, False)

    for gj in range(4):
        for t in range(q3 // 128):
            nat3[gj * (q3 // 128) + t, pl.ds(0, 8), :] = jnp.zeros((8, 128), F32)
            nat3[gj * (q3 // 128) + t, pl.ds(8 + 16 * nrad, 8), :] = jnp.zeros((8, 128), F32)
            for gi in range(16):
                nat3[gj * (q3 // 128) + t, pl.ds(8 + gi, nrad, stride=16), :] = a3[gi, gj, :, t * 128:t * 128 + 128]
    begin = pl.multiple_of(r * 16, 8)
    x3 = jnp.concatenate([nat3[t, pl.ds(begin, 32), :] for t in range(w3 // 128)], axis=1)
    x3 = jnp.concatenate([x3[8:24], x3[24:32], x3[0:8]], axis=0)
    y3 = permute(x3, one_hot(w3, w3, lambda c: (c % 4) * q3 + c // 4))
    for aa in range(na):
        wg[aa] = y3[:, aa * lanes:(aa + 1) * lanes]
    v3[0, 0, :, 0:lanes] = wg[a]
    v3[0, 0, :, lanes:ext] = jnp.where(lane((32, 128)) < 64, wg[ar, :, 0:128], wg[al, :, lanes - 128:lanes])

    coarse.add_prolonged(window, t1, True)
    coarse.sweeps(POST, False)
    middle.add_prolonged(coarse, t1, True)
    middle.sweeps(POST, False)
    near_end = lax.broadcasted_iota(jnp.int32, (8, ext), 0) < 4
    fine.add_prolonged(middle, tmp_res, True, lambda x: jnp.concatenate(
        [x[0:blk], jnp.where(near_end, x[blk:blk + 8], x[blk + 8:blk + 16])], axis=0))
    fine.sweeps(POST, False)

    for gi in range(8):
        centre = fine.coef(4, gi)
        out_c, in_c, ang_c = (fine.coef(k, gi) * centre for k in (1, 2, 3))
        for gj in range(8):
            full = (g0[gi, gj] + out_c * fine.up(v0, gi, gj) + in_c * fine.down(v0, gi, gj)
                    + ang_c * (fine.right(v0, gi, gj) + fine.left(v0, gi, gj)) - centre * v0[gi, gj])
            for t in range(tiles):
                cols = slice(t * 128, t * 128 + 128)
                sol[gj, t, pl.ds(gi, blk, stride=8), :] = v0[gi, gj, 0:blk, cols]
                resid[gj, t, pl.ds(gi, blk, stride=8), :] = full[0:blk, cols]
    for side in range(2):
        @pl.when(ends[side])
        def _():
            for cp in row_copies(side):
                cp.wait_send()
    for cp in straight:
        cp.wait_send()
    for side in range(2):
        @pl.when(ends[side])
        def _():
            for cp in copies1(side, r - 1 if side == 0 else r + 1):
                cp.wait_send()
    for cp in straight1:
        cp.wait_send()
    for d in others:
        hand(*d).wait_send()


def join_kernel(grouped_sol, grouped_res, sol, resid):
    tiles, h = grouped_sol.shape[1:3]
    join = one_hot(256, 256, lambda c: 32 * (c % 8) + c // 8)
    ln = lax.broadcasted_iota(jnp.int32, (h, 128), 1) // 32
    for x, out in ((grouped_sol, sol), (grouped_res, resid)):
        for t in range(tiles):
            for b in range(4):
                halves = []
                for hf in range(2):
                    o = None
                    for p in range(4):
                        piece = roll(x[hf * 4 + p, t], 32 * (p - b), 1)
                        o = piece if o is None else jnp.where(ln == p, piece, o)
                    halves.append(o)
                base = (4 * t + b) * 256
                out[:, base:base + 256] = permute(jnp.concatenate(halves, axis=1), join)


def row_copies_in(side, rowbuf, colbuf, copy, row_send, row_recv, col_send, col_recv, gs, rs, pack, h, a, r):
    rows = pl.ds(0, HALO)
    to_r = r + 1 if side == 0 else r - 1
    made = [copy(x.at[rows, :], rowbuf.at[k, side], row_send.at[k, side], row_recv.at[k, side], a, to_r)
            for k, x in enumerate((gs, rs))]
    for p in range(2):
        made.append(copy(pack.at[p, rows, :], colbuf.at[p, pl.ds(h // 4 + side * HALO, HALO), :],
                         col_send.at[p, 1 + side], col_recv.at[p, 1 + side], a, to_r))
    return made


def tmp_small(ref):
    return ref.at[:, :, :, 0:128]


def solution(mesh):
    na, nrad = mesh.shape["ang"], mesh.shape["rad"]

    def local(right_side, guess):
        h, w = right_side.shape
        lanes = w // 8
        ext, tiles = lanes + 128, lanes // 128
        blk = h // 8
        s0 = blk + 8
        w3, q3 = lanes * na, lanes * na // 4
        m = lambda *s: pltpu.VMEM(s, F32)
        scratch = [
            m(h, w), m(h, w), pltpu.SemaphoreType.DMA((2,)),
            m(2, 2, HALO, w), m(2, h // 4, 128), m(2, h // 4 + 2 * HALO, 128), m(2, blk, 128), m(2, blk + 16, 128), m(4, 4, 32, ext), m(4, 4, 32, ext),
            m(2, 8, tiles + 1, 8 * s0, 128),
            m(8, 8, s0, ext), m(8, 8, s0, ext), m(6, 8, s0, 128),
            m(4, 4, 32, ext), m(4, 4, 32, ext), m(6, 4, 32, 128),
            m(2, 2, 32, ext), m(2, 2, 32, ext), m(6, 2, 32, 128),
            m(1, 1, 32, ext), m(6, 1, 32, 128),
            m(h // 8, lanes), m(na, 32, lanes), m(8, 8, s0, ext), m(4, 8, s0, ext),
            m(na, nrad * 16, lanes), m(na * tiles, nrad * 16, 128), m(w3 // 128, nrad * 16 + 16, 128),
            m(16, 4, nrad, q3), m(16, 4, nrad, q3), m(6, 16, nrad, 128),
            m(8, 2, nrad, q3), m(8, 2, nrad, q3), m(6, 8, nrad, 128),
            m(4, 4, nrad, 128), m(4, 4, nrad, 128), m(6, 4, nrad, 128),
            m(2, 2, nrad, 128), m(2, 2, nrad, 128), m(6, 2, nrad, 128),
            m(1, 1, nrad, 128), m(1, 1, nrad, 128), m(6, 1, nrad, 128),
            m(16, 4, nrad, q3), m(8, 4, nrad, q3),
            pltpu.SemaphoreType.DMA((2, 2)), pltpu.SemaphoreType.DMA((2, 2)),
            pltpu.SemaphoreType.DMA((2, 3)), pltpu.SemaphoreType.DMA((2, 3)),
            pltpu.SemaphoreType.DMA((2,)), pltpu.SemaphoreType.DMA((2,)),
            pltpu.SemaphoreType.DMA((2, 3)), pltpu.SemaphoreType.DMA((2, 3)),
            pltpu.SemaphoreType.DMA((na * nrad,)), pltpu.SemaphoreType.DMA((na * nrad,)),
        ]
        grouped = pl.pallas_call(
            lambda *refs: kernel(na, nrad, h, w, *refs),
            out_shape=[jax.ShapeDtypeStruct((8, tiles, h, 128), F32)] * 2,
            in_specs=[pl.BlockSpec(memory_space=pl.ANY)] * 2,
            out_specs=[pl.BlockSpec(memory_space=pltpu.VMEM)] * 2,
            scratch_shapes=scratch,
            compiler_params=pltpu.CompilerParams(has_side_effects=True, collective_id=0, vmem_limit_bytes=60 * 1024 * 1024),
        )(right_side, guess)
        part = h // 2
        return pl.pallas_call(
            join_kernel,
            out_shape=[jax.ShapeDtypeStruct((h, w), F32)] * 2,
            grid=(2,),
            in_specs=[pl.BlockSpec((8, tiles, part, 128), lambda i: (0, 0, i, 0))] * 2,
            out_specs=[pl.BlockSpec((part, w), lambda i: (i, 0))] * 2,
        )(*grouped)

    placed = (P("rad", "ang"), P("rad", "ang"))
    return jax.shard_map(local, mesh=mesh, in_specs=placed, out_specs=placed, check_vma=False)
```

```python
import math

import jax
import jax.numpy as jnp
from jax import lax
from jax.experimental import pallas as pl
from jax.experimental.pallas import tpu as pltpu
from jax.sharding import PartitionSpec as P

LEVELS = 8
PRE = 2
POST = 2
COARSE_SWEEPS = 8
F32 = jnp.float32
MESH = pl.DeviceIdType.MESH
HALO = 16


def one_hot(rows, cols, source):
    r = lax.broadcasted_iota(jnp.int32, (rows, cols), 0)
    c = lax.broadcasted_iota(jnp.int32, (rows, cols), 1)
    return jnp.where(r == source(c), 1.0, 0.0).astype(jnp.bfloat16)


def permute(x, table):
    hi = x.astype(jnp.bfloat16)
    rest = x - hi.astype(F32)
    mid = rest.astype(jnp.bfloat16)
    low = (rest - mid.astype(F32)).astype(jnp.bfloat16)
    n = x.shape[0]
    y = jnp.dot(jnp.concatenate([hi, mid, low], axis=0), table, preferred_element_type=F32)
    return (y[:n] + y[n:2 * n]) + y[2 * n:]


def wide(c, lanes):
    return jnp.concatenate([c] * (lanes // c.shape[1]), axis=1) if lanes > c.shape[1] else c


def roll(x, shift, axis):
    return pltpu.roll(x, shift % x.shape[axis], axis)


class Grid:
    def __init__(self, v, g, c, nr, nc, closed):
        self.v, self.g, self.c, self.nr, self.nc, self.closed = v, g, c, nr, nc, closed

    def rows_shift(self, x, d):
        y = roll(x, -d, 0)
        if self.closed:
            s = lax.broadcasted_iota(jnp.int32, x.shape, 0)
            y = jnp.where(s == (x.shape[0] - 1 if d > 0 else 0), 0.0, y)
        return y

    def up(self, a, gi, gj):
        return a[gi + 1, gj] if gi + 1 < self.nr else self.rows_shift(a[0, gj], 1)

    def down(self, a, gi, gj):
        return a[gi - 1, gj] if gi > 0 else self.rows_shift(a[self.nr - 1, gj], -1)

    def right(self, a, gi, gj):
        return a[gi, gj + 1] if gj + 1 < self.nc else roll(a[gi, 0], -1, 1)

    def left(self, a, gi, gj):
        return a[gi, gj - 1] if gj > 0 else roll(a[gi, self.nc - 1], 1, 1)

    def coef(self, k, gi):
        return wide(self.c[k, gi], self.v.shape[-1])

    def update(self, gi, gj):
        v = self.v
        return (self.coef(0, gi) * self.g[gi, gj] + self.coef(1, gi) * self.up(v, gi, gj)
                + self.coef(2, gi) * self.down(v, gi, gj)
                + self.coef(3, gi) * (self.right(v, gi, gj) + self.left(v, gi, gj)))

    def half(self, parity, first=False):
        for gi in range(self.nr):
            for gj in range(self.nc):
                if (gi + gj) % 2 == parity:
                    if first:
                        self.v[gi, gj] = self.coef(0, gi) * self.g[gi, gj]
                    else:
                        self.v[gi, gj] = self.update(gi, gj)

    def sweeps(self, count, zero):
        if zero:
            self.half(0, True)
            self.half(1)
            count -= 1

        def body(_, carry):
            self.half(0)
            self.half(1)
            return carry

        if count:
            lax.fori_loop(0, count, body, 0)

    def restrict(self, res, tmp, out):
        nr, nc = self.nr, self.nc
        for gi in range(nr):
            for gj in range(nc):
                if (gi + gj) % 2 == 0:
                    res[gi, gj] = self.coef(4, gi) * (self.update(gi, gj) - self.v[gi, gj])
        for big in range(nr // 2):
            for gj in range(nc):
                if gj % 2 == 0:
                    a, b = 3.0 * res[2 * big, gj], self.up(res, 2 * big + 1, gj)
                else:
                    a, b = 3.0 * res[2 * big + 1, gj], self.down(res, 2 * big, gj)
                tmp[big, gj] = (a + b) * 0.125
        for big in range(nr // 2):
            for col in range(nc // 2):
                inner = 3.0 * (tmp[big, 2 * col] + tmp[big, 2 * col + 1])
                outer = self.left(tmp, big, 2 * col) + self.right(tmp, big, 2 * col + 1)
                out(big, col, (inner + outer) * 0.5)

    def add_prolonged(self, coarse, tmp, mask, fit=lambda x: x):
        e = coarse.v
        for gi in range(self.nr):
            for col in range(coarse.nc):
                near = e[gi // 2, col]
                far = coarse.down(e, gi // 2, col) if gi % 2 == 0 else coarse.up(e, gi // 2, col)
                value = fit(0.75 * near + 0.25 * far)
                if mask:
                    value = value * self.coef(5, gi)
                tmp[gi, col] = value
        for gi in range(self.nr):
            for gj in range(self.nc):
                near = tmp[gi, gj // 2]
                far = coarse.left(tmp, gi, gj // 2) if gj % 2 == 0 else coarse.right(tmp, gi, gj // 2)
                self.v[gi, gj] = self.v[gi, gj] + (0.75 * near + 0.25 * far)


def fill_coefficients(c, nr, rows_per_group, start, total, spacing, wrap):
    for gi in range(nr):
        s = lax.broadcasted_iota(jnp.int32, (rows_per_group, 128), 0)
        if wrap:
            s = jnp.where(s >= wrap, s - rows_per_group, s)
        row = start + nr * s + gi
        inside = jnp.logical_and(row >= 0, row < total)
        radius = 1.0 + (jnp.where(inside, row, 0).astype(F32) + 0.5) * spacing
        ratio = 0.5 * spacing / radius
        angular = 1.0 / (radius * radius)
        centre = 2.0 + 2.0 * angular
        zero = jnp.zeros_like(radius)
        for k, value in enumerate((1.0 / centre, (1.0 + ratio) / centre, (1.0 - ratio) / centre,
                                   angular / centre, centre, jnp.ones_like(radius))):
            c[k, gi] = jnp.where(inside, value, zero)


def kernel(na, nrad, h, w, rs_in, gs_in, sol, resid, rs, gs, load_sem,
           rowbuf, pack, colbuf, s1, q1, t1, u1, stage, v0, g0, c0, v1, g1, c1, v2, g2, c2, v3, c3, wv, wg, tmp_res, tmp_mid,
           gat, rows3, nat3, a3, b3, d3, a4, b4, d4, a5, b5, d5, a6, b6, d6, a7, b7, d7, t3, u3,
           row_send, row_recv, col_send, col_recv, row1_send, row1_recv, col1_send, col1_recv, all_send, all_recv, known):
    a, r = lax.axis_index("ang"), lax.axis_index("rad")
    ar, al = lax.rem(a + 1, na), lax.rem(a + na - 1, na)
    lanes = w // 8
    ext = lanes + 128
    tiles = lanes // 128
    spacing = [2.0 * math.pi / (w * na >> l) for l in range(LEVELS)]
    lane = lambda shape: lax.broadcasted_iota(jnp.int32, shape, 1)

    loads = [pltpu.make_async_copy(src, dst, load_sem.at[k]) for k, (src, dst) in enumerate(((gs_in, gs), (rs_in, rs)))]
    for cp in loads:
        cp.start()
    blk = h // 8
    s0 = blk + 8
    barrier = pltpu.get_barrier_semaphore()

    others = sorted(((da, dr) for da in range(na) for dr in range(nrad) if da or dr),
                    key=lambda d: -min(d[1], nrad - d[1]))
    ends = (r > 0, r < nrad - 1)

    def greet(to_r, first):
        for da in range(first, na):
            pl.semaphore_signal(barrier, inc=1, device_id=(lax.rem(a + da, na), to_r), device_id_type=MESH)

    for side in range(2):
        @pl.when(ends[side])
        def _():
            greet(r - 1 if side == 0 else r + 1, 0)
    greet(r, 1)
    reach = [2 << k for k in range(nrad.bit_length()) if 2 << k < nrad - 1]

    def announce(k):
        for side, there in ((0, r >= reach[k]), (1, r < nrad - reach[k])):
            @pl.when(there)
            def _():
                to_r = r - reach[k] if side == 0 else r + reach[k]
                pl.semaphore_signal(known.at[k, 1 - side], inc=1, device_id=(a, to_r), device_id_type=MESH)

    def learn(k):
        for side, there in ((0, r >= reach[k]), (1, r < nrad - reach[k])):
            @pl.when(there)
            def _():
                pl.semaphore_wait(known.at[k, side], 1)

    for l, c in ((0, c0), (1, c1), (2, c2)):
        fill_coefficients(c, 8 >> l, s0 if l == 0 else blk + 16, r * (h >> l), (h * nrad) >> l, spacing[l], blk + 4 if l == 0 else blk + 8)
    for l, d, n in ((3, d3, 16), (4, d4, 8), (5, d5, 4), (6, d6, 2), (7, d7, 1)):
        fill_coefficients(d, n, nrad, 0, (h * nrad) >> l, spacing[l], 0)

    for cp in loads:
        cp.wait()

    fold = h // 4
    place16 = lane((fold, 128)) // 16
    for p, (tile, base) in enumerate(((0, 0), (w - 128, 16))):
        folded = None
        for q in range(4):
            for k, x in enumerate((gs, rs)):
                piece = roll(x[q * fold:(q + 1) * fold, tile:tile + 128], 32 * q + 16 * k + base, 1)
                folded = piece if folded is None else jnp.where(place16 == 2 * q + k, piece, folded)
        pack[p] = folded

    def copy(src, dst, send, recv, to_a, to_r):
        return pltpu.make_async_remote_copy(src_ref=src, dst_ref=dst, send_sem=send, recv_sem=recv,
                                            device_id=(to_a, to_r), device_id_type=MESH)

    def row_copies(side):
        to_r = r - 1 if side == 0 else r + 1
        rows = pl.ds(0, HALO) if side == 0 else pl.ds(h - HALO, HALO)
        made = [copy(x.at[rows, :], rowbuf.at[k, side], row_send.at[k, side], row_recv.at[k, side], a, to_r)
                for k, x in enumerate((gs, rs))]
        for p, to_a in ((0, al), (1, ar)):
            made.append(copy(pack.at[p, pl.ds(side * (fold - HALO), HALO), :], colbuf.at[p, pl.ds(fold + side * HALO, HALO), :],
                             col_send.at[p, 1 + side], col_recv.at[p, 1 + side], to_a, to_r))
        return made

    pl.semaphore_wait(barrier, na * (1 + (r > 0).astype(jnp.int32) + (r < nrad - 1).astype(jnp.int32)) - 1)
    for side in range(2):
        @pl.when(ends[side])
        def _():
            for cp in row_copies(side):
                cp.start()
    straight = [copy(pack.at[p], colbuf.at[p, pl.ds(0, fold), :], col_send.at[p, 0], col_recv.at[p, 0], to_a, r)
                for p, to_a in ((0, al), (1, ar))]
    for cp in straight:
        cp.start()

    spread = one_hot(256, 256, lambda c: 8 * (c % 32) + c // 32)
    halo_spread = [one_hot(128, 1024, lambda c, k=k: jnp.where(
        c % 128 < 2, 16 * k + 8 * (c % 128) + c // 128,
        jnp.where(c % 128 >= 126, 32 + 16 * k + 8 * (c % 128 - 126) + c // 128, -1))) for k in range(2)]

    def split_rows(x, count, put):
        ln = lane((count, 128)) // 32
        for t in range(tiles):
            parts = [permute(x(slice((4 * t + b) * 256, (4 * t + b) * 256 + 256)), spread) for b in range(4)]
            for gj in range(8):
                o = None
                for b in range(4):
                    half = parts[b][:, (gj // 4) * 128:(gj // 4) * 128 + 128]
                    piece = roll(half, 32 * (b - gj % 4), 1)
                    o = piece if o is None else jnp.where(ln == b, piece, o)
                put(gj, t, o)

    def put_own(k):
        def put(gj, t, value):
            stage[k, gj, t, pl.ds(0, h), :] = value
        return put

    for k, x in enumerate((gs, rs)):
        split_rows(lambda cols, x=x: x[:, cols], h, put_own(k))

    for side in range(2):
        @pl.when(ends[1 - side])
        def _():
            for cp in row_copies_in(side, rowbuf, colbuf, copy, row_send, row_recv, col_send, col_recv, gs, rs, pack, h, a, r):
                cp.wait_recv()
    for cp in straight:
        cp.wait_recv()
    announce(0)
    at = (h, 8 * s0 - HALO)
    for k in range(2):
        for gj in range(8):
            for t in range(tiles + 1):
                stage[k, gj, t, pl.ds(h + HALO, 8 * s0 - h - 2 * HALO), :] = jnp.zeros((8 * s0 - h - 2 * HALO, 128), F32)
    def put_edges(gj, t, value):
        for k in range(2):
            for side in range(2):
                n = 2 * k + side
                stage[k, gj, t, pl.ds(at[side], HALO), :] = value[n * HALO:(n + 1) * HALO]

    split_rows(lambda cols: jnp.concatenate(
        [jnp.where(ends[1 - side], rowbuf[k, side, :, cols], 0.0) for k in range(2) for side in range(2)], axis=0),
        4 * HALO, put_edges)

    def beside(first, count, shift):
        right, left = colbuf[0, pl.ds(first, count), :], colbuf[1, pl.ds(first, count), :]
        return jnp.where(lane((count, 128)) < 32, roll(right, -shift, 1), roll(left, 32 - shift, 1))

    strips = [beside(0, fold, 32 * q) for q in range(4)]
    strips.append(jnp.where(ends[1], beside(fold, HALO, 0), 0.0))
    strips.append(jnp.where(ends[0], beside(fold + HALO, HALO, 96), 0.0))
    strips = jnp.concatenate(strips, axis=0)
    for k in range(2):
        y = permute(strips, halo_spread[k])
        for gj in range(8):
            cols = slice(gj * 128, gj * 128 + 128)
            stage[k, gj, tiles, pl.ds(0, h + HALO), :] = y[0:h + HALO, cols]
            stage[k, gj, tiles, pl.ds(at[1], HALO), :] = y[h + HALO:, cols]
    for k, dst in enumerate((v0, g0)):
        for gj in range(8):
            for gi in range(8):
                for t in range(tiles + 1):
                    dst[gi, gj, :, t * 128:t * 128 + 128] = stage[k, gj, t, pl.ds(gi, s0, stride=8), :]

    fine = Grid(v0, g0, c0, 8, 8, False)
    middle = Grid(v1, g1, c1, 4, 4, False)
    coarse = Grid(v2, g2, c2, 2, 2, False)
    window = Grid(v3, None, None, 1, 1, False)

    def into(ref):
        def put(gi, gj, value):
            ref[gi, gj] = value
        return put

    fine.sweeps(PRE, False)

    def put1(gi, gj, value):
        g1[gi, gj, 0:blk, 0:lanes] = value[0:blk, 0:lanes]
    fine.restrict(tmp_res, tmp_mid, put1)

    for side, first in ((0, blk), (1, blk + 8)):
        @pl.when(jnp.logical_not(ends[1 - side]))
        def _():
            g1[:, :, first:first + 8, 0:lanes] = jnp.zeros((4, 4, 8, lanes), F32)
    slot = lane((blk, 128)) // 8
    left_edge = right_edge = None
    for g in range(16):
        lo = roll(g1[g // 4, g % 4, 0:blk, 0:128], 8 * g, 1)
        hi = roll(g1[g // 4, g % 4, 0:blk, lanes - 128:lanes], 8 * g + 8, 1)
        left_edge = lo if g == 0 else jnp.where(slot == g, lo, left_edge)
        right_edge = hi if g == 0 else jnp.where(slot == g, hi, right_edge)
    s1[0] = left_edge
    s1[1] = right_edge

    def copies1(side, to_r):
        first = 0 if side == 0 else blk - 8
        made = [copy(g1.at[:, :, pl.ds(first, 8), pl.ds(0, lanes)], g1.at[:, :, pl.ds(blk + 8 * side, 8), pl.ds(0, lanes)],
                     row1_send.at[side], row1_recv.at[side], a, to_r)]
        for p, to_a in ((0, al), (1, ar)):
            made.append(copy(s1.at[p, pl.ds(first, 8), :], q1.at[p, pl.ds(blk + 8 * side, 8), :],
                             col1_send.at[p, 1 + side], col1_recv.at[p, 1 + side], to_a, to_r))
        return made

    straight1 = [copy(s1.at[p], q1.at[p, pl.ds(0, blk), :], col1_send.at[p, 0], col1_recv.at[p, 0], to_a, r)
                 for p, to_a in ((0, al), (1, ar))]
    for side in range(2):
        @pl.when(ends[side])
        def _():
            for cp in copies1(side, r - 1 if side == 0 else r + 1):
                cp.start()
    for cp in straight1:
        cp.start()
    learn(0)
    for k in range(1, len(reach)):
        announce(k)
        if k < len(reach) - 1:
            learn(k)
    for side in range(2):
        @pl.when(ends[1 - side])
        def _():
            for cp in copies1(side, r + 1 if side == 0 else r - 1):
                cp.wait_recv()
    for cp in straight1:
        cp.wait_recv()
    wl = lane((blk + 16, 128))
    sub = lax.broadcasted_iota(jnp.int32, (blk + 16, 128), 0)
    got = jnp.where(sub < blk, 1, jnp.where(sub < blk + 8, nrad - 1 - r, r)) > 0
    strip_r, strip_l = jnp.where(got, q1[0], 0.0), jnp.where(got, q1[1], 0.0)
    for g in range(16):
        g1[g // 4, g % 4, :, lanes:ext] = jnp.where(
            wl < 8, roll(strip_r, -8 * g, 1), jnp.where(wl >= 120, roll(strip_l, 120 - 8 * g, 1), 0.0))
    middle.sweeps(PRE, True)
    middle.restrict(t1, u1, into(g2))
    coarse.sweeps(PRE, True)

    def put3(gi, gj, value):
        wv[...] = value[0:blk, 0:lanes]
    coarse.restrict(t1, u1, put3)

    place = gat.at[a, pl.ds(pl.multiple_of(r * blk, 8), blk), :]
    gat[a, pl.ds(pl.multiple_of(r * blk, 8), blk), :] = wv[...]

    def hand(da, dr):
        step = da * nrad + dr
        return copy(wv, place, all_send.at[step], all_recv.at[step], lax.rem(a + da, na), lax.rem(r + dr, nrad))

    learn(len(reach) - 1)
    for d in others:
        hand(*d).start()
    for d in others:
        hand(*d).wait_recv()

    w3 = lanes * na
    q3 = w3 // 4
    for aa in range(na):
        for t in range(tiles):
            rows3[aa * tiles + t] = gat[aa, :, t * 128:t * 128 + 128]
    stacked = jnp.concatenate([jnp.concatenate(
        [rows3[t, pl.ds(gi, nrad, stride=16), :] for t in range(na * tiles)], axis=1) for gi in range(16)], axis=0)
    table3 = one_hot(w3, w3, lambda c: 4 * (c % q3) + c // q3)
    by_group = permute(stacked, table3)
    for gi in range(16):
        for gj in range(4):
            b3[gi, gj] = by_group[gi * nrad:(gi + 1) * nrad, gj * q3:(gj + 1) * q3]

    l3 = Grid(a3, b3, d3, 16, 4, True)
    l4 = Grid(a4, b4, d4, 8, 2, True)
    l5 = Grid(a5, b5, d5, 4, 4, True)
    l6 = Grid(a6, b6, d6, 2, 2, True)
    l3.sweeps(PRE, True)
    l3.restrict(t3, u3, into(b4))
    l4.sweeps(PRE, True)
    w5 = w3 // 4
    q5 = w5 // 4
    nat5 = {}

    def put5(gi, gj, value):
        nat5[gi] = value
    l4.restrict(t3, u3, put5)
    x5 = permute(jnp.concatenate([nat5[i] for i in range(4)], axis=0),
                 one_hot(w5, 512, lambda c: 4 * (c % q5) + c // 128))
    for gi in range(4):
        for gj in range(4):
            b5[gi, gj] = x5[gi * nrad:(gi + 1) * nrad, gj * 128:gj * 128 + 128]
    l5.sweeps(PRE, True)
    l5.restrict(tmp_small(t3), tmp_small(u3), into(b6))
    l6.sweeps(PRE, True)
    l6.restrict(tmp_small(t3), tmp_small(u3), into(b7))
    l7 = Grid(a7, b7, d7, 1, 1, True)
    red = (lax.broadcasted_iota(jnp.int32, (nrad, 128), 0) + lane((nrad, 128))) % 2 == 0
    a7[0, 0] = jnp.zeros((nrad, 128), F32)

    def coarsest(_, carry):
        a7[0, 0] = jnp.where(red, l7.update(0, 0), a7[0, 0])
        a7[0, 0] = jnp.where(red, a7[0, 0], l7.update(0, 0))
        return carry
    lax.fori_loop(0, COARSE_SWEEPS, coarsest, 0)

    l6.add_prolonged(l7, tmp_small(t3), False)
    l6.sweeps(POST, False)
    l5.add_prolonged(l6, tmp_small(t3), False)
    l5.sweeps(POST, False)
    y5 = None
    for gj in range(4):
        x = jnp.concatenate([a5[gi, gj] for gi in range(4)], axis=0)
        r0 = permute(x, one_hot(128, w5, lambda c, gj=gj: jnp.where(c % 4 == gj, c // 4, -1)))
        y5 = r0 if y5 is None else y5 + r0
    for gi in range(4):
        u3[gi, 0] = y5[gi * nrad:(gi + 1) * nrad]
    l4.add_prolonged(Grid(u3, None, None, 4, 1, True), t3, False)
    l4.sweeps(POST, False)
    l3.add_prolonged(l4, t3, False)
    l3.sweeps(POST, False)

    for gj in range(4):
        for t in range(q3 // 128):
            nat3[gj * (q3 // 128) + t, pl.ds(0, 8), :] = jnp.zeros((8, 128), F32)
            nat3[gj * (q3 // 128) + t, pl.ds(8 + 16 * nrad, 8), :] = jnp.zeros((8, 128), F32)
            for gi in range(16):
                nat3[gj * (q3 // 128) + t, pl.ds(8 + gi, nrad, stride=16), :] = a3[gi, gj, :, t * 128:t * 128 + 128]
    begin = pl.multiple_of(r * 16, 8)
    x3 = jnp.concatenate([nat3[t, pl.ds(begin, 32), :] for t in range(w3 // 128)], axis=1)
    x3 = jnp.concatenate([x3[8:24], x3[24:32], x3[0:8]], axis=0)
    y3 = permute(x3, one_hot(w3, w3, lambda c: (c % 4) * q3 + c // 4))
    for aa in range(na):
        wg[aa] = y3[:, aa * lanes:(aa + 1) * lanes]
    v3[0, 0, :, 0:lanes] = wg[a]
    v3[0, 0, :, lanes:ext] = jnp.where(lane((32, 128)) < 64, wg[ar, :, 0:128], wg[al, :, lanes - 128:lanes])

    coarse.add_prolonged(window, t1, True)
    coarse.sweeps(POST, False)
    middle.add_prolonged(coarse, t1, True)
    middle.sweeps(POST, False)
    near_end = lax.broadcasted_iota(jnp.int32, (8, ext), 0) < 4
    fine.add_prolonged(middle, tmp_res, True, lambda x: jnp.concatenate(
        [x[0:blk], jnp.where(near_end, x[blk:blk + 8], x[blk + 8:blk + 16])], axis=0))
    fine.sweeps(POST, False)

    for gi in range(8):
        centre = fine.coef(4, gi)
        out_c, in_c, ang_c = (fine.coef(k, gi) * centre for k in (1, 2, 3))
        for gj in range(8):
            full = (g0[gi, gj] + out_c * fine.up(v0, gi, gj) + in_c * fine.down(v0, gi, gj)
                    + ang_c * (fine.right(v0, gi, gj) + fine.left(v0, gi, gj)) - centre * v0[gi, gj])
            for t in range(tiles):
                cols = slice(t * 128, t * 128 + 128)
                sol[gj, t, pl.ds(gi, blk, stride=8), :] = v0[gi, gj, 0:blk, cols]
                resid[gj, t, pl.ds(gi, blk, stride=8), :] = full[0:blk, cols]
    for side in range(2):
        @pl.when(ends[side])
        def _():
            for cp in row_copies(side):
                cp.wait_send()
    for cp in straight:
        cp.wait_send()
    for side in range(2):
        @pl.when(ends[side])
        def _():
            for cp in copies1(side, r - 1 if side == 0 else r + 1):
                cp.wait_send()
    for cp in straight1:
        cp.wait_send()
    for d in others:
        hand(*d).wait_send()


def join_kernel(grouped_sol, grouped_res, sol, resid, whole, out_sem):
    tiles, h = grouped_sol.shape[1:3]
    join = one_hot(256, 256, lambda c: 32 * (c % 8) + c // 8)
    ln = lax.broadcasted_iota(jnp.int32, (h, 128), 1) // 32
    copies = []
    for k, (x, out) in enumerate(((grouped_sol, sol), (grouped_res, resid))):
        for t in range(tiles):
            for b in range(4):
                halves = []
                for hf in range(2):
                    o = None
                    for p in range(4):
                        piece = roll(x[hf * 4 + p, t], 32 * (p - b), 1)
                        o = piece if o is None else jnp.where(ln == p, piece, o)
                    halves.append(o)
                cols = pl.ds((4 * t + b) * 256, 256)
                whole[k, :, cols] = permute(jnp.concatenate(halves, axis=1), join)
                copies.append(pltpu.make_async_copy(whole.at[k, :, cols], out.at[:, cols], out_sem.at[k, 4 * t + b]))
                copies[-1].start()
    for cp in copies:
        cp.wait()


def row_copies_in(side, rowbuf, colbuf, copy, row_send, row_recv, col_send, col_recv, gs, rs, pack, h, a, r):
    rows = pl.ds(0, HALO)
    to_r = r + 1 if side == 0 else r - 1
    made = [copy(x.at[rows, :], rowbuf.at[k, side], row_send.at[k, side], row_recv.at[k, side], a, to_r)
            for k, x in enumerate((gs, rs))]
    for p in range(2):
        made.append(copy(pack.at[p, rows, :], colbuf.at[p, pl.ds(h // 4 + side * HALO, HALO), :],
                         col_send.at[p, 1 + side], col_recv.at[p, 1 + side], a, to_r))
    return made


def tmp_small(ref):
    return ref.at[:, :, :, 0:128]


def solution(mesh):
    na, nrad = mesh.shape["ang"], mesh.shape["rad"]

    def local(right_side, guess):
        h, w = right_side.shape
        lanes = w // 8
        ext, tiles = lanes + 128, lanes // 128
        blk = h // 8
        s0 = blk + 8
        w3, q3 = lanes * na, lanes * na // 4
        m = lambda *s: pltpu.VMEM(s, F32)
        scratch = [
            m(h, w), m(h, w), pltpu.SemaphoreType.DMA((2,)),
            m(2, 2, HALO, w), m(2, h // 4, 128), m(2, h // 4 + 2 * HALO, 128), m(2, blk, 128), m(2, blk + 16, 128), m(4, 4, 32, ext), m(4, 4, 32, ext),
            m(2, 8, tiles + 1, 8 * s0, 128),
            m(8, 8, s0, ext), m(8, 8, s0, ext), m(6, 8, s0, 128),
            m(4, 4, 32, ext), m(4, 4, 32, ext), m(6, 4, 32, 128),
            m(2, 2, 32, ext), m(2, 2, 32, ext), m(6, 2, 32, 128),
            m(1, 1, 32, ext), m(6, 1, 32, 128),
            m(h // 8, lanes), m(na, 32, lanes), m(8, 8, s0, ext), m(4, 8, s0, ext),
            m(na, nrad * 16, lanes), m(na * tiles, nrad * 16, 128), m(w3 // 128, nrad * 16 + 16, 128),
            m(16, 4, nrad, q3), m(16, 4, nrad, q3), m(6, 16, nrad, 128),
            m(8, 2, nrad, q3), m(8, 2, nrad, q3), m(6, 8, nrad, 128),
            m(4, 4, nrad, 128), m(4, 4, nrad, 128), m(6, 4, nrad, 128),
            m(2, 2, nrad, 128), m(2, 2, nrad, 128), m(6, 2, nrad, 128),
            m(1, 1, nrad, 128), m(1, 1, nrad, 128), m(6, 1, nrad, 128),
            m(16, 4, nrad, q3), m(8, 4, nrad, q3),
            pltpu.SemaphoreType.DMA((2, 2)), pltpu.SemaphoreType.DMA((2, 2)),
            pltpu.SemaphoreType.DMA((2, 3)), pltpu.SemaphoreType.DMA((2, 3)),
            pltpu.SemaphoreType.DMA((2,)), pltpu.SemaphoreType.DMA((2,)),
            pltpu.SemaphoreType.DMA((2, 3)), pltpu.SemaphoreType.DMA((2, 3)),
            pltpu.SemaphoreType.DMA((na * nrad,)), pltpu.SemaphoreType.DMA((na * nrad,)),
            pltpu.SemaphoreType.REGULAR((nrad.bit_length(), 2)),
        ]
        grouped = pl.pallas_call(
            lambda *refs: kernel(na, nrad, h, w, *refs),
            out_shape=[jax.ShapeDtypeStruct((8, tiles, h, 128), F32)] * 2,
            in_specs=[pl.BlockSpec(memory_space=pl.ANY)] * 2,
            out_specs=[pl.BlockSpec(memory_space=pltpu.VMEM)] * 2,
            scratch_shapes=scratch,
            compiler_params=pltpu.CompilerParams(has_side_effects=True, collective_id=0, vmem_limit_bytes=105 * 512 * 1024),
        )(right_side, guess)
        return pl.pallas_call(
            join_kernel,
            out_shape=[jax.ShapeDtypeStruct((h, w), F32)] * 2,
            in_specs=[pl.BlockSpec(memory_space=pltpu.VMEM)] * 2,
            out_specs=[pl.BlockSpec(memory_space=pl.ANY)] * 2,
            scratch_shapes=[m(2, h, w), pltpu.SemaphoreType.DMA((2, 4 * tiles))],
            compiler_params=pltpu.CompilerParams(vmem_limit_bytes=16 * 1024 * 1024),
        )(*grouped)

    placed = (P("rad", "ang"), P("rad", "ang"))
    return jax.shard_map(local, mesh=mesh, in_specs=placed, out_specs=placed, check_vma=False)
```

```python
import math

import jax
import jax.numpy as jnp
from jax import lax
from jax.experimental import pallas as pl
from jax.experimental.pallas import tpu as pltpu
from jax.sharding import PartitionSpec as P

LEVELS = 8
PRE = 2
POST = 2
COARSE_SWEEPS = 8
F32 = jnp.float32
MESH = pl.DeviceIdType.MESH
HALO = 16


def one_hot(rows, cols, source):
    r = lax.broadcasted_iota(jnp.int32, (rows, cols), 0)
    c = lax.broadcasted_iota(jnp.int32, (rows, cols), 1)
    return jnp.where(r == source(c), 1.0, 0.0).astype(jnp.bfloat16)


def permute(x, table):
    hi = x.astype(jnp.bfloat16)
    rest = x - hi.astype(F32)
    mid = rest.astype(jnp.bfloat16)
    low = (rest - mid.astype(F32)).astype(jnp.bfloat16)
    n = x.shape[0]
    y = jnp.dot(jnp.concatenate([hi, mid, low], axis=0), table, preferred_element_type=F32)
    return (y[:n] + y[n:2 * n]) + y[2 * n:]


def wide(c, lanes):
    return jnp.concatenate([c] * (lanes // c.shape[1]), axis=1) if lanes > c.shape[1] else c


def roll(x, shift, axis):
    return pltpu.roll(x, shift % x.shape[axis], axis)


class Grid:
    def __init__(self, v, g, c, nr, nc, closed):
        self.v, self.g, self.c, self.nr, self.nc, self.closed = v, g, c, nr, nc, closed

    def rows_shift(self, x, d):
        y = roll(x, -d, 0)
        if self.closed:
            s = lax.broadcasted_iota(jnp.int32, x.shape, 0)
            y = jnp.where(s == (x.shape[0] - 1 if d > 0 else 0), 0.0, y)
        return y

    def up(self, a, gi, gj):
        return a[gi + 1, gj] if gi + 1 < self.nr else self.rows_shift(a[0, gj], 1)

    def down(self, a, gi, gj):
        return a[gi - 1, gj] if gi > 0 else self.rows_shift(a[self.nr - 1, gj], -1)

    def right(self, a, gi, gj):
        return a[gi, gj + 1] if gj + 1 < self.nc else roll(a[gi, 0], -1, 1)

    def left(self, a, gi, gj):
        return a[gi, gj - 1] if gj > 0 else roll(a[gi, self.nc - 1], 1, 1)

    def coef(self, k, gi):
        return wide(self.c[k, gi], self.v.shape[-1])

    def update(self, gi, gj):
        v = self.v
        return (self.coef(0, gi) * self.g[gi, gj] + self.coef(1, gi) * self.up(v, gi, gj)
                + self.coef(2, gi) * self.down(v, gi, gj)
                + self.coef(3, gi) * (self.right(v, gi, gj) + self.left(v, gi, gj)))

    def half(self, parity, first=False):
        for gi in range(self.nr):
            for gj in range(self.nc):
                if (gi + gj) % 2 == parity:
                    if first:
                        self.v[gi, gj] = self.coef(0, gi) * self.g[gi, gj]
                    else:
                        self.v[gi, gj] = self.update(gi, gj)

    def sweeps(self, count, zero):
        if zero:
            self.half(0, True)
            self.half(1)
            count -= 1

        def body(_, carry):
            self.half(0)
            self.half(1)
            return carry

        if count:
            lax.fori_loop(0, count, body, 0)

    def restrict(self, res, tmp, out):
        nr, nc = self.nr, self.nc
        for gi in range(nr):
            for gj in range(nc):
                if (gi + gj) % 2 == 0:
                    res[gi, gj] = self.coef(4, gi) * (self.update(gi, gj) - self.v[gi, gj])
        for big in range(nr // 2):
            for gj in range(nc):
                if gj % 2 == 0:
                    a, b = 3.0 * res[2 * big, gj], self.up(res, 2 * big + 1, gj)
                else:
                    a, b = 3.0 * res[2 * big + 1, gj], self.down(res, 2 * big, gj)
                tmp[big, gj] = (a + b) * 0.125
        for big in range(nr // 2):
            for col in range(nc // 2):
                inner = 3.0 * (tmp[big, 2 * col] + tmp[big, 2 * col + 1])
                outer = self.left(tmp, big, 2 * col) + self.right(tmp, big, 2 * col + 1)
                out(big, col, (inner + outer) * 0.5)

    def add_prolonged(self, coarse, tmp, mask, fit=lambda x: x):
        e = coarse.v
        for gi in range(self.nr):
            for col in range(coarse.nc):
                near = e[gi // 2, col]
                far = coarse.down(e, gi // 2, col) if gi % 2 == 0 else coarse.up(e, gi // 2, col)
                value = fit(0.75 * near + 0.25 * far)
                if mask:
                    value = value * self.coef(5, gi)
                tmp[gi, col] = value
        for gi in range(self.nr):
            for gj in range(self.nc):
                near = tmp[gi, gj // 2]
                far = coarse.left(tmp, gi, gj // 2) if gj % 2 == 0 else coarse.right(tmp, gi, gj // 2)
                self.v[gi, gj] = self.v[gi, gj] + (0.75 * near + 0.25 * far)


def fill_coefficients(c, nr, rows_per_group, start, total, spacing, wrap):
    for gi in range(nr):
        s = lax.broadcasted_iota(jnp.int32, (rows_per_group, 128), 0)
        if wrap:
            s = jnp.where(s >= wrap, s - rows_per_group, s)
        row = start + nr * s + gi
        inside = jnp.logical_and(row >= 0, row < total)
        radius = 1.0 + (jnp.where(inside, row, 0).astype(F32) + 0.5) * spacing
        ratio = 0.5 * spacing / radius
        angular = 1.0 / (radius * radius)
        centre = 2.0 + 2.0 * angular
        zero = jnp.zeros_like(radius)
        for k, value in enumerate((1.0 / centre, (1.0 + ratio) / centre, (1.0 - ratio) / centre,
                                   angular / centre, centre, jnp.ones_like(radius))):
            c[k, gi] = jnp.where(inside, value, zero)


def kernel(na, nrad, h, w, rs_in, gs_in, sol, resid, rs, gs, load_sem,
           rowbuf, pack, colbuf, s1, q1, t1, u1, stage, v0, g0, c0, v1, g1, c1, v2, g2, c2, v3, c3, wv, wg, tmp_res, tmp_mid,
           gat, rows3, nat3, a3, b3, d3, a4, b4, d4, a5, b5, d5, a6, b6, d6, a7, b7, d7, t3, u3,
           row_send, row_recv, col_send, col_recv, row1_send, row1_recv, col1_send, col1_recv, all_send, all_recv, known):
    a, r = lax.axis_index("ang"), lax.axis_index("rad")
    ar, al = lax.rem(a + 1, na), lax.rem(a + na - 1, na)
    lanes = w // 8
    ext = lanes + 128
    tiles = lanes // 128
    spacing = [2.0 * math.pi / (w * na >> l) for l in range(LEVELS)]
    lane = lambda shape: lax.broadcasted_iota(jnp.int32, shape, 1)

    loads = [pltpu.make_async_copy(src, dst, load_sem.at[k]) for k, (src, dst) in enumerate(((gs_in, gs), (rs_in, rs)))]
    for cp in loads:
        cp.start()
    blk = h // 8
    s0 = blk + 8
    barrier = pltpu.get_barrier_semaphore()

    others = sorted(((da, dr) for da in range(na) for dr in range(0, nrad, 2) if da or dr),
                    key=lambda d: -min(d[1], nrad - d[1]))
    ends = (r > 0, r < nrad - 1)

    def greet(to_r, first):
        for da in range(first, na):
            pl.semaphore_signal(barrier, inc=1, device_id=(lax.rem(a + da, na), to_r), device_id_type=MESH)

    for side in range(2):
        @pl.when(ends[side])
        def _():
            greet(r - 1 if side == 0 else r + 1, 0)
    greet(r, 1)
    reach = [2 << k for k in range(nrad.bit_length()) if 2 << k < nrad - 1]

    def announce(k):
        for side, there in ((0, r >= reach[k]), (1, r < nrad - reach[k])):
            @pl.when(there)
            def _():
                to_r = r - reach[k] if side == 0 else r + reach[k]
                pl.semaphore_signal(known.at[k, 1 - side], inc=1, device_id=(a, to_r), device_id_type=MESH)

    def learn(k):
        for side, there in ((0, r >= reach[k]), (1, r < nrad - reach[k])):
            @pl.when(there)
            def _():
                pl.semaphore_wait(known.at[k, side], 1)

    for l, c in ((0, c0), (1, c1), (2, c2)):
        fill_coefficients(c, 8 >> l, s0 if l == 0 else blk + 16, r * (h >> l), (h * nrad) >> l, spacing[l], blk + 4 if l == 0 else blk + 8)
    for l, d, n in ((3, d3, 16), (4, d4, 8), (5, d5, 4), (6, d6, 2), (7, d7, 1)):
        fill_coefficients(d, n, nrad, 0, (h * nrad) >> l, spacing[l], 0)

    for cp in loads:
        cp.wait()

    fold = h // 4
    place16 = lane((fold, 128)) // 16
    for p, (tile, base) in enumerate(((0, 0), (w - 128, 16))):
        folded = None
        for q in range(4):
            for k, x in enumerate((gs, rs)):
                piece = roll(x[q * fold:(q + 1) * fold, tile:tile + 128], 32 * q + 16 * k + base, 1)
                folded = piece if folded is None else jnp.where(place16 == 2 * q + k, piece, folded)
        pack[p] = folded

    def copy(src, dst, send, recv, to_a, to_r):
        return pltpu.make_async_remote_copy(src_ref=src, dst_ref=dst, send_sem=send, recv_sem=recv,
                                            device_id=(to_a, to_r), device_id_type=MESH)

    def row_copies(side):
        to_r = r - 1 if side == 0 else r + 1
        rows = pl.ds(0, HALO) if side == 0 else pl.ds(h - HALO, HALO)
        made = [copy(x.at[rows, :], rowbuf.at[k, side], row_send.at[k, side], row_recv.at[k, side], a, to_r)
                for k, x in enumerate((gs, rs))]
        for p, to_a in ((0, al), (1, ar)):
            made.append(copy(pack.at[p, pl.ds(side * (fold - HALO), HALO), :], colbuf.at[p, pl.ds(fold + side * HALO, HALO), :],
                             col_send.at[p, 1 + side], col_recv.at[p, 1 + side], to_a, to_r))
        return made

    pl.semaphore_wait(barrier, na * (1 + (r > 0).astype(jnp.int32) + (r < nrad - 1).astype(jnp.int32)) - 1)
    for side in range(2):
        @pl.when(ends[side])
        def _():
            for cp in row_copies(side)[2:]:
                cp.start()
    straight = [copy(pack.at[p], colbuf.at[p, pl.ds(0, fold), :], col_send.at[p, 0], col_recv.at[p, 0], to_a, r)
                for p, to_a in ((0, al), (1, ar))]
    for cp in straight:
        cp.start()
    for side in range(2):
        @pl.when(ends[side])
        def _():
            for cp in row_copies(side)[:2]:
                cp.start()

    spread = one_hot(256, 256, lambda c: 8 * (c % 32) + c // 32)
    halo_spread = [one_hot(128, 1024, lambda c, k=k: jnp.where(
        c % 128 < 2, 16 * k + 8 * (c % 128) + c // 128,
        jnp.where(c % 128 >= 126, 32 + 16 * k + 8 * (c % 128 - 126) + c // 128, -1))) for k in range(2)]

    def split_rows(x, count, put):
        ln = lane((count, 128)) // 32
        for t in range(tiles):
            parts = [permute(x(slice((4 * t + b) * 256, (4 * t + b) * 256 + 256)), spread) for b in range(4)]
            for gj in range(8):
                o = None
                for b in range(4):
                    half = parts[b][:, (gj // 4) * 128:(gj // 4) * 128 + 128]
                    piece = roll(half, 32 * (b - gj % 4), 1)
                    o = piece if o is None else jnp.where(ln == b, piece, o)
                put(gj, t, o)

    def put_own(k):
        def put(gj, t, value):
            stage[k, gj, t, pl.ds(0, h), :] = value
        return put

    for k, x in enumerate((gs, rs)):
        split_rows(lambda cols, x=x: x[:, cols], h, put_own(k))

    for side in range(2):
        @pl.when(ends[1 - side])
        def _():
            for cp in row_copies_in(side, rowbuf, colbuf, copy, row_send, row_recv, col_send, col_recv, gs, rs, pack, h, a, r):
                cp.wait_recv()
    for cp in straight:
        cp.wait_recv()
    announce(0)
    at = (h, 8 * s0 - HALO)
    for k in range(2):
        for gj in range(8):
            for t in range(tiles + 1):
                stage[k, gj, t, pl.ds(h + HALO, 8 * s0 - h - 2 * HALO), :] = jnp.zeros((8 * s0 - h - 2 * HALO, 128), F32)
    def put_edges(gj, t, value):
        for k in range(2):
            for side in range(2):
                n = 2 * k + side
                stage[k, gj, t, pl.ds(at[side], HALO), :] = value[n * HALO:(n + 1) * HALO]

    split_rows(lambda cols: jnp.concatenate(
        [jnp.where(ends[1 - side], rowbuf[k, side, :, cols], 0.0) for k in range(2) for side in range(2)], axis=0),
        4 * HALO, put_edges)

    def beside(first, count, shift):
        right, left = colbuf[0, pl.ds(first, count), :], colbuf[1, pl.ds(first, count), :]
        return jnp.where(lane((count, 128)) < 32, roll(right, -shift, 1), roll(left, 32 - shift, 1))

    strips = [beside(0, fold, 32 * q) for q in range(4)]
    strips.append(jnp.where(ends[1], beside(fold, HALO, 0), 0.0))
    strips.append(jnp.where(ends[0], beside(fold + HALO, HALO, 96), 0.0))
    strips = jnp.concatenate(strips, axis=0)
    for k in range(2):
        y = permute(strips, halo_spread[k])
        for gj in range(8):
            cols = slice(gj * 128, gj * 128 + 128)
            stage[k, gj, tiles, pl.ds(0, h + HALO), :] = y[0:h + HALO, cols]
            stage[k, gj, tiles, pl.ds(at[1], HALO), :] = y[h + HALO:, cols]
    for k, dst in enumerate((v0, g0)):
        for gj in range(8):
            for gi in range(8):
                for t in range(tiles + 1):
                    dst[gi, gj, :, t * 128:t * 128 + 128] = stage[k, gj, t, pl.ds(gi, s0, stride=8), :]

    fine = Grid(v0, g0, c0, 8, 8, False)
    middle = Grid(v1, g1, c1, 4, 4, False)
    coarse = Grid(v2, g2, c2, 2, 2, False)
    window = Grid(v3, None, None, 1, 1, False)

    def into(ref):
        def put(gi, gj, value):
            ref[gi, gj] = value
        return put

    fine.sweeps(PRE, False)

    def put1(gi, gj, value):
        g1[gi, gj, 0:blk, 0:lanes] = value[0:blk, 0:lanes]
    fine.restrict(tmp_res, tmp_mid, put1)

    for side, first in ((0, blk), (1, blk + 8)):
        @pl.when(jnp.logical_not(ends[1 - side]))
        def _():
            g1[:, :, first:first + 8, 0:lanes] = jnp.zeros((4, 4, 8, lanes), F32)
    slot = lane((blk, 128)) // 8
    left_edge = right_edge = None
    for g in range(16):
        lo = roll(g1[g // 4, g % 4, 0:blk, 0:128], 8 * g, 1)
        hi = roll(g1[g // 4, g % 4, 0:blk, lanes - 128:lanes], 8 * g + 8, 1)
        left_edge = lo if g == 0 else jnp.where(slot == g, lo, left_edge)
        right_edge = hi if g == 0 else jnp.where(slot == g, hi, right_edge)
    s1[0] = left_edge
    s1[1] = right_edge

    def copies1(side, to_r):
        first = 0 if side == 0 else blk - 8
        made = [copy(g1.at[:, :, pl.ds(first, 8), pl.ds(0, lanes)], g1.at[:, :, pl.ds(blk + 8 * side, 8), pl.ds(0, lanes)],
                     row1_send.at[side], row1_recv.at[side], a, to_r)]
        for p, to_a in ((0, al), (1, ar)):
            made.append(copy(s1.at[p, pl.ds(first, 8), :], q1.at[p, pl.ds(blk + 8 * side, 8), :],
                             col1_send.at[p, 1 + side], col1_recv.at[p, 1 + side], to_a, to_r))
        return made

    straight1 = [copy(s1.at[p], q1.at[p, pl.ds(0, blk), :], col1_send.at[p, 0], col1_recv.at[p, 0], to_a, r)
                 for p, to_a in ((0, al), (1, ar))]
    for side in range(2):
        @pl.when(ends[side])
        def _():
            for cp in copies1(side, r - 1 if side == 0 else r + 1)[1:]:
                cp.start()
    for cp in straight1:
        cp.start()
    for side in range(2):
        @pl.when(ends[side])
        def _():
            copies1(side, r - 1 if side == 0 else r + 1)[0].start()
    learn(0)
    for k in range(1, len(reach)):
        announce(k)
        if k < len(reach) - 1:
            learn(k)
    for side in range(2):
        @pl.when(ends[1 - side])
        def _():
            for cp in copies1(side, r + 1 if side == 0 else r - 1):
                cp.wait_recv()
    for cp in straight1:
        cp.wait_recv()
    wl = lane((blk + 16, 128))
    sub = lax.broadcasted_iota(jnp.int32, (blk + 16, 128), 0)
    got = jnp.where(sub < blk, 1, jnp.where(sub < blk + 8, nrad - 1 - r, r)) > 0
    strip_r, strip_l = jnp.where(got, q1[0], 0.0), jnp.where(got, q1[1], 0.0)
    for g in range(16):
        g1[g // 4, g % 4, :, lanes:ext] = jnp.where(
            wl < 8, roll(strip_r, -8 * g, 1), jnp.where(wl >= 120, roll(strip_l, 120 - 8 * g, 1), 0.0))
    middle.sweeps(PRE, True)
    middle.restrict(t1, u1, into(g2))
    coarse.sweeps(PRE, True)

    def put3(gi, gj, value):
        wv[...] = value[0:blk, 0:lanes]
    coarse.restrict(t1, u1, put3)

    place = gat.at[a, pl.ds(pl.multiple_of(r * blk, 8), blk), :]
    gat[a, pl.ds(pl.multiple_of(r * blk, 8), blk), :] = wv[...]

    def hand(da, dr):
        step = da * nrad + dr
        return copy(wv, place, all_send.at[step], all_recv.at[step], lax.rem(a + da, na), lax.rem(r + dr, nrad))

    partner = r + 1 - 2 * lax.rem(r, 2)

    def relay(da, dr):
        step = da * nrad + dr + 1
        came = gat.at[lax.rem(a + na - da, na), pl.ds(pl.multiple_of(lax.rem(r + nrad - dr, nrad) * blk, 8), blk), :]
        return copy(came, came, all_send.at[step], all_recv.at[step], a, partner)

    own = copy(wv, place, all_send.at[0], all_recv.at[0], a, partner)
    learn(len(reach) - 1)
    for d in others:
        hand(*d).start()
    own.start()
    for d in reversed(others):
        hand(*d).wait_recv()
        relay(*d).start()
    own.wait_recv()
    for d in reversed(others):
        relay(*d).wait_recv()

    w3 = lanes * na
    q3 = w3 // 4
    for aa in range(na):
        for t in range(tiles):
            rows3[aa * tiles + t] = gat[aa, :, t * 128:t * 128 + 128]
    stacked = jnp.concatenate([jnp.concatenate(
        [rows3[t, pl.ds(gi, nrad, stride=16), :] for t in range(na * tiles)], axis=1) for gi in range(16)], axis=0)
    table3 = one_hot(w3, w3, lambda c: 4 * (c % q3) + c // q3)
    by_group = permute(stacked, table3)
    for gi in range(16):
        for gj in range(4):
            b3[gi, gj] = by_group[gi * nrad:(gi + 1) * nrad, gj * q3:(gj + 1) * q3]

    l3 = Grid(a3, b3, d3, 16, 4, True)
    l4 = Grid(a4, b4, d4, 8, 2, True)
    l5 = Grid(a5, b5, d5, 4, 4, True)
    l6 = Grid(a6, b6, d6, 2, 2, True)
    l3.sweeps(PRE, True)
    l3.restrict(t3, u3, into(b4))
    l4.sweeps(PRE, True)
    w5 = w3 // 4
    q5 = w5 // 4
    nat5 = {}

    def put5(gi, gj, value):
        nat5[gi] = value
    l4.restrict(t3, u3, put5)
    x5 = permute(jnp.concatenate([nat5[i] for i in range(4)], axis=0),
                 one_hot(w5, 512, lambda c: 4 * (c % q5) + c // 128))
    for gi in range(4):
        for gj in range(4):
            b5[gi, gj] = x5[gi * nrad:(gi + 1) * nrad, gj * 128:gj * 128 + 128]
    l5.sweeps(PRE, True)
    l5.restrict(tmp_small(t3), tmp_small(u3), into(b6))
    l6.sweeps(PRE, True)
    l6.restrict(tmp_small(t3), tmp_small(u3), into(b7))
    l7 = Grid(a7, b7, d7, 1, 1, True)
    red = (lax.broadcasted_iota(jnp.int32, (nrad, 128), 0) + lane((nrad, 128))) % 2 == 0
    a7[0, 0] = jnp.zeros((nrad, 128), F32)

    def coarsest(_, carry):
        a7[0, 0] = jnp.where(red, l7.update(0, 0), a7[0, 0])
        a7[0, 0] = jnp.where(red, a7[0, 0], l7.update(0, 0))
        return carry
    lax.fori_loop(0, COARSE_SWEEPS, coarsest, 0)

    l6.add_prolonged(l7, tmp_small(t3), False)
    l6.sweeps(POST, False)
    l5.add_prolonged(l6, tmp_small(t3), False)
    l5.sweeps(POST, False)
    y5 = None
    for gj in range(4):
        x = jnp.concatenate([a5[gi, gj] for gi in range(4)], axis=0)
        r0 = permute(x, one_hot(128, w5, lambda c, gj=gj: jnp.where(c % 4 == gj, c // 4, -1)))
        y5 = r0 if y5 is None else y5 + r0
    for gi in range(4):
        u3[gi, 0] = y5[gi * nrad:(gi + 1) * nrad]
    l4.add_prolonged(Grid(u3, None, None, 4, 1, True), t3, False)
    l4.sweeps(POST, False)
    l3.add_prolonged(l4, t3, False)
    l3.sweeps(POST, False)

    for gj in range(4):
        for t in range(q3 // 128):
            nat3[gj * (q3 // 128) + t, pl.ds(0, 8), :] = jnp.zeros((8, 128), F32)
            nat3[gj * (q3 // 128) + t, pl.ds(8 + 16 * nrad, 8), :] = jnp.zeros((8, 128), F32)
            for gi in range(16):
                nat3[gj * (q3 // 128) + t, pl.ds(8 + gi, nrad, stride=16), :] = a3[gi, gj, :, t * 128:t * 128 + 128]
    begin = pl.multiple_of(r * 16, 8)
    x3 = jnp.concatenate([nat3[t, pl.ds(begin, 32), :] for t in range(w3 // 128)], axis=1)
    x3 = jnp.concatenate([x3[8:24], x3[24:32], x3[0:8]], axis=0)
    y3 = permute(x3, one_hot(w3, w3, lambda c: (c % 4) * q3 + c // 4))
    for aa in range(na):
        wg[aa] = y3[:, aa * lanes:(aa + 1) * lanes]
    v3[0, 0, :, 0:lanes] = wg[a]
    v3[0, 0, :, lanes:ext] = jnp.where(lane((32, 128)) < 64, wg[ar, :, 0:128], wg[al, :, lanes - 128:lanes])

    coarse.add_prolonged(window, t1, True)
    coarse.sweeps(POST, False)
    middle.add_prolonged(coarse, t1, True)
    middle.sweeps(POST, False)
    near_end = lax.broadcasted_iota(jnp.int32, (8, ext), 0) < 4
    fine.add_prolonged(middle, tmp_res, True, lambda x: jnp.concatenate(
        [x[0:blk], jnp.where(near_end, x[blk:blk + 8], x[blk + 8:blk + 16])], axis=0))
    fine.sweeps(POST, False)

    for gi in range(8):
        centre = fine.coef(4, gi)
        out_c, in_c, ang_c = (fine.coef(k, gi) * centre for k in (1, 2, 3))
        for gj in range(8):
            full = (g0[gi, gj] + out_c * fine.up(v0, gi, gj) + in_c * fine.down(v0, gi, gj)
                    + ang_c * (fine.right(v0, gi, gj) + fine.left(v0, gi, gj)) - centre * v0[gi, gj])
            for t in range(tiles):
                cols = slice(t * 128, t * 128 + 128)
                sol[gj, t, pl.ds(gi, blk, stride=8), :] = v0[gi, gj, 0:blk, cols]
                resid[gj, t, pl.ds(gi, blk, stride=8), :] = full[0:blk, cols]
    for side in range(2):
        @pl.when(ends[side])
        def _():
            for cp in row_copies(side):
                cp.wait_send()
    for cp in straight:
        cp.wait_send()
    for side in range(2):
        @pl.when(ends[side])
        def _():
            for cp in copies1(side, r - 1 if side == 0 else r + 1):
                cp.wait_send()
    for cp in straight1:
        cp.wait_send()
    own.wait_send()
    for d in others:
        hand(*d).wait_send()
        relay(*d).wait_send()


def join_kernel(grouped_sol, grouped_res, sol, resid, whole, out_sem):
    tiles, h = grouped_sol.shape[1:3]
    join = one_hot(256, 256, lambda c: 32 * (c % 8) + c // 8)
    ln = lax.broadcasted_iota(jnp.int32, (h, 128), 1) // 32
    copies = []
    for k, (x, out) in enumerate(((grouped_sol, sol), (grouped_res, resid))):
        for t in range(tiles):
            for b in range(4):
                halves = []
                for hf in range(2):
                    o = None
                    for p in range(4):
                        piece = roll(x[hf * 4 + p, t], 32 * (p - b), 1)
                        o = piece if o is None else jnp.where(ln == p, piece, o)
                    halves.append(o)
                cols = pl.ds((4 * t + b) * 256, 256)
                whole[k, :, cols] = permute(jnp.concatenate(halves, axis=1), join)
                copies.append(pltpu.make_async_copy(whole.at[k, :, cols], out.at[:, cols], out_sem.at[k, 4 * t + b]))
                copies[-1].start()
    for cp in copies:
        cp.wait()


def row_copies_in(side, rowbuf, colbuf, copy, row_send, row_recv, col_send, col_recv, gs, rs, pack, h, a, r):
    rows = pl.ds(0, HALO)
    to_r = r + 1 if side == 0 else r - 1
    made = [copy(x.at[rows, :], rowbuf.at[k, side], row_send.at[k, side], row_recv.at[k, side], a, to_r)
            for k, x in enumerate((gs, rs))]
    for p in range(2):
        made.append(copy(pack.at[p, rows, :], colbuf.at[p, pl.ds(h // 4 + side * HALO, HALO), :],
                         col_send.at[p, 1 + side], col_recv.at[p, 1 + side], a, to_r))
    return made


def tmp_small(ref):
    return ref.at[:, :, :, 0:128]


def solution(mesh):
    na, nrad = mesh.shape["ang"], mesh.shape["rad"]

    def local(right_side, guess):
        h, w = right_side.shape
        lanes = w // 8
        ext, tiles = lanes + 128, lanes // 128
        blk = h // 8
        s0 = blk + 8
        w3, q3 = lanes * na, lanes * na // 4
        m = lambda *s: pltpu.VMEM(s, F32)
        scratch = [
            m(h, w), m(h, w), pltpu.SemaphoreType.DMA((2,)),
            m(2, 2, HALO, w), m(2, h // 4, 128), m(2, h // 4 + 2 * HALO, 128), m(2, blk, 128), m(2, blk + 16, 128), m(4, 4, 32, ext), m(4, 4, 32, ext),
            m(2, 8, tiles + 1, 8 * s0, 128),
            m(8, 8, s0, ext), m(8, 8, s0, ext), m(6, 8, s0, 128),
            m(4, 4, 32, ext), m(4, 4, 32, ext), m(6, 4, 32, 128),
            m(2, 2, 32, ext), m(2, 2, 32, ext), m(6, 2, 32, 128),
            m(1, 1, 32, ext), m(6, 1, 32, 128),
            m(h // 8, lanes), m(na, 32, lanes), m(8, 8, s0, ext), m(4, 8, s0, ext),
            m(na, nrad * 16, lanes), m(na * tiles, nrad * 16, 128), m(w3 // 128, nrad * 16 + 16, 128),
            m(16, 4, nrad, q3), m(16, 4, nrad, q3), m(6, 16, nrad, 128),
            m(8, 2, nrad, q3), m(8, 2, nrad, q3), m(6, 8, nrad, 128),
            m(4, 4, nrad, 128), m(4, 4, nrad, 128), m(6, 4, nrad, 128),
            m(2, 2, nrad, 128), m(2, 2, nrad, 128), m(6, 2, nrad, 128),
            m(1, 1, nrad, 128), m(1, 1, nrad, 128), m(6, 1, nrad, 128),
            m(16, 4, nrad, q3), m(8, 4, nrad, q3),
            pltpu.SemaphoreType.DMA((2, 2)), pltpu.SemaphoreType.DMA((2, 2)),
            pltpu.SemaphoreType.DMA((2, 3)), pltpu.SemaphoreType.DMA((2, 3)),
            pltpu.SemaphoreType.DMA((2,)), pltpu.SemaphoreType.DMA((2,)),
            pltpu.SemaphoreType.DMA((2, 3)), pltpu.SemaphoreType.DMA((2, 3)),
            pltpu.SemaphoreType.DMA((na * nrad,)), pltpu.SemaphoreType.DMA((na * nrad,)),
            pltpu.SemaphoreType.REGULAR((nrad.bit_length(), 2)),
        ]
        grouped = pl.pallas_call(
            lambda *refs: kernel(na, nrad, h, w, *refs),
            out_shape=[jax.ShapeDtypeStruct((8, tiles, h, 128), F32)] * 2,
            in_specs=[pl.BlockSpec(memory_space=pl.ANY)] * 2,
            out_specs=[pl.BlockSpec(memory_space=pltpu.VMEM)] * 2,
            scratch_shapes=scratch,
            compiler_params=pltpu.CompilerParams(has_side_effects=True, collective_id=0, vmem_limit_bytes=105 * 512 * 1024),
        )(right_side, guess)
        return pl.pallas_call(
            join_kernel,
            out_shape=[jax.ShapeDtypeStruct((h, w), F32)] * 2,
            in_specs=[pl.BlockSpec(memory_space=pltpu.VMEM)] * 2,
            out_specs=[pl.BlockSpec(memory_space=pl.ANY)] * 2,
            scratch_shapes=[m(2, h, w), pltpu.SemaphoreType.DMA((2, 4 * tiles))],
            compiler_params=pltpu.CompilerParams(vmem_limit_bytes=16 * 1024 * 1024),
        )(*grouped)

    placed = (P("rad", "ang"), P("rad", "ang"))
    return jax.shard_map(local, mesh=mesh, in_specs=placed, out_specs=placed, check_vma=False)
```

```python
import math

import jax
import jax.numpy as jnp
import numpy as np
from jax import lax
from jax.experimental import pallas as pl
from jax.experimental.pallas import tpu as pltpu
from jax.sharding import PartitionSpec as P

LEVELS = 8
PRE = 2
POST = 2
COARSE_SWEEPS = 8
F32 = jnp.float32
MESH = pl.DeviceIdType.MESH
HALO = 16


def one_hot(rows, cols, source):
    r = lax.broadcasted_iota(jnp.int32, (rows, cols), 0)
    c = lax.broadcasted_iota(jnp.int32, (rows, cols), 1)
    return jnp.where(r == source(c), 1.0, 0.0).astype(jnp.bfloat16)


def permute(x, table):
    hi = x.astype(jnp.bfloat16)
    rest = x - hi.astype(F32)
    mid = rest.astype(jnp.bfloat16)
    low = (rest - mid.astype(F32)).astype(jnp.bfloat16)
    n = x.shape[0]
    y = jnp.dot(jnp.concatenate([hi, mid, low], axis=0), table, preferred_element_type=F32)
    return (y[:n] + y[n:2 * n]) + y[2 * n:]


def wide(c, lanes):
    return jnp.concatenate([c] * (lanes // c.shape[1]), axis=1) if lanes > c.shape[1] else c


def roll(x, shift, axis):
    return pltpu.roll(x, shift % x.shape[axis], axis)


def coarsest_operator(rows, cols, spacing):
    radius = (1.0 + (np.arange(rows) + 0.5) * spacing)[:, None]
    outward, inward, angular = 1.0 + 0.5 * spacing / radius, 1.0 - 0.5 * spacing / radius, 1.0 / (radius * radius)
    colour = (np.arange(rows)[:, None] + np.arange(cols)[None, :]) % 2
    g = np.eye(rows * cols).reshape(-1, rows, cols)
    v = np.zeros_like(g)
    for step in range(2 * COARSE_SWEEPS):
        p = np.pad(v, ((0, 0), (1, 1), (0, 0)))
        new = (g + outward * p[:, 2:] + inward * p[:, :-2] + angular * (np.roll(v, -1, 2) + np.roll(v, 1, 2))) / (2.0 + 2.0 * angular)
        v = np.where(colour == step % 2, new, v)
    rest, parts = v.reshape(rows * cols, rows * cols), []
    for _ in range(3):
        parts.append(rest.astype(np.float32).astype(jnp.bfloat16))
        rest = rest - parts[-1].astype(np.float64)
    return np.concatenate(parts, axis=1)


def apply_operator(x, table, cols):
    rows, per = x.shape[0], 128 // cols
    tiles = table.shape[0] // 128
    s = lax.broadcasted_iota(jnp.int32, x.shape, 0)
    block = lax.broadcasted_iota(jnp.int32, x.shape, 1) // cols
    flat = jnp.concatenate([jnp.where(s == t * per + block, x, 0.0) for t in range(tiles)], axis=1)
    flat = jnp.broadcast_to(jnp.sum(flat, axis=0, keepdims=True), (rows, flat.shape[1]))
    hi = flat.astype(jnp.bfloat16).astype(F32)
    mid = (flat - hi).astype(jnp.bfloat16).astype(F32)
    low = flat - hi - mid
    lhs = [hi, mid, low] + [jnp.zeros_like(low)] * (3 * rows // 8 % 2)
    y = jnp.dot(jnp.concatenate(lhs, axis=0).astype(jnp.bfloat16), table, preferred_element_type=F32)
    out = None
    for t in range(tiles):
        piece = lambda k, m: y[k * rows:(k + 1) * rows, (m * tiles + t) * 128:(m * tiles + t) * 128 + 128]
        total = (piece(0, 2) + piece(1, 1) + piece(2, 0)) + (piece(0, 1) + piece(1, 0)) + piece(0, 0)
        out = total if out is None else jnp.where(s // per == t, total, out)
    turn = (block + per - s % per) % per
    spread = out
    for k in range(1, per):
        spread = jnp.where(turn == k, roll(out, cols * k, 1), spread)
    return spread


class Grid:
    def __init__(self, v, g, c, nr, nc, closed):
        self.v, self.g, self.c, self.nr, self.nc, self.closed = v, g, c, nr, nc, closed

    def rows_shift(self, x, d):
        y = roll(x, -d, 0)
        if self.closed:
            s = lax.broadcasted_iota(jnp.int32, x.shape, 0)
            y = jnp.where(s == (x.shape[0] - 1 if d > 0 else 0), 0.0, y)
        return y

    def up(self, a, gi, gj):
        return a[gi + 1, gj] if gi + 1 < self.nr else self.rows_shift(a[0, gj], 1)

    def down(self, a, gi, gj):
        return a[gi - 1, gj] if gi > 0 else self.rows_shift(a[self.nr - 1, gj], -1)

    def right(self, a, gi, gj):
        return a[gi, gj + 1] if gj + 1 < self.nc else roll(a[gi, 0], -1, 1)

    def left(self, a, gi, gj):
        return a[gi, gj - 1] if gj > 0 else roll(a[gi, self.nc - 1], 1, 1)

    def coef(self, k, gi):
        return wide(self.c[k, gi], self.v.shape[-1])

    def update(self, gi, gj):
        v = self.v
        return (self.coef(0, gi) * self.g[gi, gj] + self.coef(1, gi) * self.up(v, gi, gj)
                + self.coef(2, gi) * self.down(v, gi, gj)
                + self.coef(3, gi) * (self.right(v, gi, gj) + self.left(v, gi, gj)))

    def half(self, parity, first=False):
        for gi in range(self.nr):
            for gj in range(self.nc):
                if (gi + gj) % 2 == parity:
                    if first:
                        self.v[gi, gj] = self.coef(0, gi) * self.g[gi, gj]
                    else:
                        self.v[gi, gj] = self.update(gi, gj)

    def sweeps(self, count, zero):
        if zero:
            self.half(0, True)
            self.half(1)
            count -= 1

        def body(_, carry):
            self.half(0)
            self.half(1)
            return carry

        if count:
            lax.fori_loop(0, count, body, 0)

    def restrict(self, res, tmp, out):
        nr, nc = self.nr, self.nc
        for gi in range(nr):
            for gj in range(nc):
                if (gi + gj) % 2 == 0:
                    res[gi, gj] = self.coef(4, gi) * (self.update(gi, gj) - self.v[gi, gj])
        for big in range(nr // 2):
            for gj in range(nc):
                if gj % 2 == 0:
                    a, b = 3.0 * res[2 * big, gj], self.up(res, 2 * big + 1, gj)
                else:
                    a, b = 3.0 * res[2 * big + 1, gj], self.down(res, 2 * big, gj)
                tmp[big, gj] = (a + b) * 0.125
        for big in range(nr // 2):
            for col in range(nc // 2):
                inner = 3.0 * (tmp[big, 2 * col] + tmp[big, 2 * col + 1])
                outer = self.left(tmp, big, 2 * col) + self.right(tmp, big, 2 * col + 1)
                out(big, col, (inner + outer) * 0.5)

    def add_prolonged(self, coarse, tmp, mask, fit=lambda x: x):
        e = coarse.v
        for gi in range(self.nr):
            for col in range(coarse.nc):
                near = e[gi // 2, col]
                far = coarse.down(e, gi // 2, col) if gi % 2 == 0 else coarse.up(e, gi // 2, col)
                value = fit(0.75 * near + 0.25 * far)
                if mask:
                    value = value * self.coef(5, gi)
                tmp[gi, col] = value
        for gi in range(self.nr):
            for gj in range(self.nc):
                near = tmp[gi, gj // 2]
                far = coarse.left(tmp, gi, gj // 2) if gj % 2 == 0 else coarse.right(tmp, gi, gj // 2)
                self.v[gi, gj] = self.v[gi, gj] + (0.75 * near + 0.25 * far)


def fill_coefficients(c, nr, rows_per_group, start, total, spacing, wrap):
    for gi in range(nr):
        s = lax.broadcasted_iota(jnp.int32, (rows_per_group, 128), 0)
        if wrap:
            s = jnp.where(s >= wrap, s - rows_per_group, s)
        row = start + nr * s + gi
        inside = jnp.logical_and(row >= 0, row < total)
        radius = 1.0 + (jnp.where(inside, row, 0).astype(F32) + 0.5) * spacing
        ratio = 0.5 * spacing / radius
        angular = 1.0 / (radius * radius)
        centre = 2.0 + 2.0 * angular
        zero = jnp.zeros_like(radius)
        for k, value in enumerate((1.0 / centre, (1.0 + ratio) / centre, (1.0 - ratio) / centre,
                                   angular / centre, centre, jnp.ones_like(radius))):
            c[k, gi] = jnp.where(inside, value, zero)


def kernel(na, nrad, h, w, rs_in, gs_in, table_in, sol, resid, rs, gs, load_sem,
           rowbuf, pack, colbuf, s1, q1, t1, u1, stage, v0, g0, c0, v1, g1, c1, v2, g2, c2, v3, c3, wv, wg, tmp_res, tmp_mid,
           gat, rows3, nat3, a3, b3, d3, a4, b4, d4, a5, b5, d5, a6, b6, d6, a7, b7, t3, u3,
           row_send, row_recv, col_send, col_recv, row1_send, row1_recv, col1_send, col1_recv, all_send, all_recv, known, table7, table_sem):
    a, r = lax.axis_index("ang"), lax.axis_index("rad")
    ar, al = lax.rem(a + 1, na), lax.rem(a + na - 1, na)
    lanes = w // 8
    ext = lanes + 128
    tiles = lanes // 128
    spacing = [2.0 * math.pi / (w * na >> l) for l in range(LEVELS)]
    lane = lambda shape: lax.broadcasted_iota(jnp.int32, shape, 1)

    loads = [pltpu.make_async_copy(src, dst, load_sem.at[k]) for k, (src, dst) in enumerate(((gs_in, gs), (rs_in, rs)))]
    for cp in loads:
        cp.start()
    load_table = pltpu.make_async_copy(table_in.at[:, 0:table7.shape[1]], table7, table_sem)
    load_table.start()
    blk = h // 8
    s0 = blk + 8
    barrier = pltpu.get_barrier_semaphore()

    others = sorted(((da, dr) for da in range(na) for dr in range(0, nrad, 2) if da or dr),
                    key=lambda d: -min(d[1], nrad - d[1]))
    ends = (r > 0, r < nrad - 1)

    def greet(to_r, first):
        for da in range(first, na):
            pl.semaphore_signal(barrier, inc=1, device_id=(lax.rem(a + da, na), to_r), device_id_type=MESH)

    for side in range(2):
        @pl.when(ends[side])
        def _():
            greet(r - 1 if side == 0 else r + 1, 0)
    greet(r, 1)
    reach = [2 << k for k in range(nrad.bit_length()) if 2 << k < nrad - 1]

    def announce(k):
        for side, there in ((0, r >= reach[k]), (1, r < nrad - reach[k])):
            @pl.when(there)
            def _():
                to_r = r - reach[k] if side == 0 else r + reach[k]
                pl.semaphore_signal(known.at[k, 1 - side], inc=1, device_id=(a, to_r), device_id_type=MESH)

    def learn(k):
        for side, there in ((0, r >= reach[k]), (1, r < nrad - reach[k])):
            @pl.when(there)
            def _():
                pl.semaphore_wait(known.at[k, side], 1)

    for l, c in ((0, c0), (1, c1), (2, c2)):
        fill_coefficients(c, 8 >> l, s0 if l == 0 else blk + 16, r * (h >> l), (h * nrad) >> l, spacing[l], blk + 4 if l == 0 else blk + 8)
    for l, d, n in ((3, d3, 16), (4, d4, 8), (5, d5, 4), (6, d6, 2)):
        fill_coefficients(d, n, nrad, 0, (h * nrad) >> l, spacing[l], 0)

    for cp in loads:
        cp.wait()

    fold = h // 4
    place16 = lane((fold, 128)) // 16
    for p, (tile, base) in enumerate(((0, 0), (w - 128, 16))):
        folded = None
        for q in range(4):
            for k, x in enumerate((gs, rs)):
                piece = roll(x[q * fold:(q + 1) * fold, tile:tile + 128], 32 * q + 16 * k + base, 1)
                folded = piece if folded is None else jnp.where(place16 == 2 * q + k, piece, folded)
        pack[p] = folded

    def copy(src, dst, send, recv, to_a, to_r):
        return pltpu.make_async_remote_copy(src_ref=src, dst_ref=dst, send_sem=send, recv_sem=recv,
                                            device_id=(to_a, to_r), device_id_type=MESH)

    def row_copies(side):
        to_r = r - 1 if side == 0 else r + 1
        rows = pl.ds(0, HALO) if side == 0 else pl.ds(h - HALO, HALO)
        made = [copy(x.at[rows, :], rowbuf.at[k, side], row_send.at[k, side], row_recv.at[k, side], a, to_r)
                for k, x in enumerate((gs, rs))]
        for p, to_a in ((0, al), (1, ar)):
            made.append(copy(pack.at[p, pl.ds(side * (fold - HALO), HALO), :], colbuf.at[p, pl.ds(fold + side * HALO, HALO), :],
                             col_send.at[p, 1 + side], col_recv.at[p, 1 + side], to_a, to_r))
        return made

    pl.semaphore_wait(barrier, na * (1 + (r > 0).astype(jnp.int32) + (r < nrad - 1).astype(jnp.int32)) - 1)
    for side in range(2):
        @pl.when(ends[side])
        def _():
            for cp in row_copies(side)[2:]:
                cp.start()
    straight = [copy(pack.at[p], colbuf.at[p, pl.ds(0, fold), :], col_send.at[p, 0], col_recv.at[p, 0], to_a, r)
                for p, to_a in ((0, al), (1, ar))]
    for cp in straight:
        cp.start()
    for side in range(2):
        @pl.when(ends[side])
        def _():
            for cp in row_copies(side)[:2]:
                cp.start()

    spread = one_hot(256, 256, lambda c: 8 * (c % 32) + c // 32)
    halo_spread = [one_hot(128, 1024, lambda c, k=k: jnp.where(
        c % 128 < 2, 16 * k + 8 * (c % 128) + c // 128,
        jnp.where(c % 128 >= 126, 32 + 16 * k + 8 * (c % 128 - 126) + c // 128, -1))) for k in range(2)]

    def split_rows(x, count, put):
        ln = lane((count, 128)) // 32
        for t in range(tiles):
            parts = [permute(x(slice((4 * t + b) * 256, (4 * t + b) * 256 + 256)), spread) for b in range(4)]
            for gj in range(8):
                o = None
                for b in range(4):
                    half = parts[b][:, (gj // 4) * 128:(gj // 4) * 128 + 128]
                    piece = roll(half, 32 * (b - gj % 4), 1)
                    o = piece if o is None else jnp.where(ln == b, piece, o)
                put(gj, t, o)

    def put_own(k):
        def put(gj, t, value):
            stage[k, gj, t, pl.ds(0, h), :] = value
        return put

    for k, x in enumerate((gs, rs)):
        split_rows(lambda cols, x=x: x[:, cols], h, put_own(k))

    for side in range(2):
        @pl.when(ends[1 - side])
        def _():
            for cp in row_copies_in(side, rowbuf, colbuf, copy, row_send, row_recv, col_send, col_recv, gs, rs, pack, h, a, r):
                cp.wait_recv()
    for cp in straight:
        cp.wait_recv()
    announce(0)
    at = (h, 8 * s0 - HALO)
    for k in range(2):
        for gj in range(8):
            for t in range(tiles + 1):
                stage[k, gj, t, pl.ds(h + HALO, 8 * s0 - h - 2 * HALO), :] = jnp.zeros((8 * s0 - h - 2 * HALO, 128), F32)
    def put_edges(gj, t, value):
        for k in range(2):
            for side in range(2):
                n = 2 * k + side
                stage[k, gj, t, pl.ds(at[side], HALO), :] = value[n * HALO:(n + 1) * HALO]

    split_rows(lambda cols: jnp.concatenate(
        [jnp.where(ends[1 - side], rowbuf[k, side, :, cols], 0.0) for k in range(2) for side in range(2)], axis=0),
        4 * HALO, put_edges)

    def beside(first, count, shift):
        right, left = colbuf[0, pl.ds(first, count), :], colbuf[1, pl.ds(first, count), :]
        return jnp.where(lane((count, 128)) < 32, roll(right, -shift, 1), roll(left, 32 - shift, 1))

    strips = [beside(0, fold, 32 * q) for q in range(4)]
    strips.append(jnp.where(ends[1], beside(fold, HALO, 0), 0.0))
    strips.append(jnp.where(ends[0], beside(fold + HALO, HALO, 96), 0.0))
    strips = jnp.concatenate(strips, axis=0)
    for k in range(2):
        y = permute(strips, halo_spread[k])
        for gj in range(8):
            cols = slice(gj * 128, gj * 128 + 128)
            stage[k, gj, tiles, pl.ds(0, h + HALO), :] = y[0:h + HALO, cols]
            stage[k, gj, tiles, pl.ds(at[1], HALO), :] = y[h + HALO:, cols]
    for k, dst in enumerate((v0, g0)):
        for gj in range(8):
            for gi in range(8):
                for t in range(tiles + 1):
                    dst[gi, gj, :, t * 128:t * 128 + 128] = stage[k, gj, t, pl.ds(gi, s0, stride=8), :]

    fine = Grid(v0, g0, c0, 8, 8, False)
    middle = Grid(v1, g1, c1, 4, 4, False)
    coarse = Grid(v2, g2, c2, 2, 2, False)
    window = Grid(v3, None, None, 1, 1, False)

    def into(ref):
        def put(gi, gj, value):
            ref[gi, gj] = value
        return put

    fine.sweeps(PRE, False)

    def put1(gi, gj, value):
        g1[gi, gj, 0:blk, 0:lanes] = value[0:blk, 0:lanes]
    fine.restrict(tmp_res, tmp_mid, put1)

    for side, first in ((0, blk), (1, blk + 8)):
        @pl.when(jnp.logical_not(ends[1 - side]))
        def _():
            g1[:, :, first:first + 8, 0:lanes] = jnp.zeros((4, 4, 8, lanes), F32)
    slot = lane((blk, 128)) // 8
    left_edge = right_edge = None
    for g in range(16):
        lo = roll(g1[g // 4, g % 4, 0:blk, 0:128], 8 * g, 1)
        hi = roll(g1[g // 4, g % 4, 0:blk, lanes - 128:lanes], 8 * g + 8, 1)
        left_edge = lo if g == 0 else jnp.where(slot == g, lo, left_edge)
        right_edge = hi if g == 0 else jnp.where(slot == g, hi, right_edge)
    s1[0] = left_edge
    s1[1] = right_edge

    def copies1(side, to_r):
        first = 0 if side == 0 else blk - 8
        made = [copy(g1.at[:, :, pl.ds(first, 8), pl.ds(0, lanes)], g1.at[:, :, pl.ds(blk + 8 * side, 8), pl.ds(0, lanes)],
                     row1_send.at[side], row1_recv.at[side], a, to_r)]
        for p, to_a in ((0, al), (1, ar)):
            made.append(copy(s1.at[p, pl.ds(first, 8), :], q1.at[p, pl.ds(blk + 8 * side, 8), :],
                             col1_send.at[p, 1 + side], col1_recv.at[p, 1 + side], to_a, to_r))
        return made

    straight1 = [copy(s1.at[p], q1.at[p, pl.ds(0, blk), :], col1_send.at[p, 0], col1_recv.at[p, 0], to_a, r)
                 for p, to_a in ((0, al), (1, ar))]
    for side in range(2):
        @pl.when(ends[side])
        def _():
            for cp in copies1(side, r - 1 if side == 0 else r + 1)[1:]:
                cp.start()
    for cp in straight1:
        cp.start()
    for side in range(2):
        @pl.when(ends[side])
        def _():
            copies1(side, r - 1 if side == 0 else r + 1)[0].start()
    learn(0)
    for k in range(1, len(reach)):
        announce(k)
        if k < len(reach) - 1:
            learn(k)
    for side in range(2):
        @pl.when(ends[1 - side])
        def _():
            for cp in copies1(side, r + 1 if side == 0 else r - 1):
                cp.wait_recv()
    for cp in straight1:
        cp.wait_recv()
    wl = lane((blk + 16, 128))
    sub = lax.broadcasted_iota(jnp.int32, (blk + 16, 128), 0)
    got = jnp.where(sub < blk, 1, jnp.where(sub < blk + 8, nrad - 1 - r, r)) > 0
    strip_r, strip_l = jnp.where(got, q1[0], 0.0), jnp.where(got, q1[1], 0.0)
    for g in range(16):
        g1[g // 4, g % 4, :, lanes:ext] = jnp.where(
            wl < 8, roll(strip_r, -8 * g, 1), jnp.where(wl >= 120, roll(strip_l, 120 - 8 * g, 1), 0.0))
    middle.sweeps(PRE, True)
    middle.restrict(t1, u1, into(g2))
    coarse.sweeps(PRE, True)

    def put3(gi, gj, value):
        wv[...] = value[0:blk, 0:lanes]
    coarse.restrict(t1, u1, put3)

    place = gat.at[a, pl.ds(pl.multiple_of(r * blk, 8), blk), :]
    gat[a, pl.ds(pl.multiple_of(r * blk, 8), blk), :] = wv[...]

    def hand(da, dr):
        step = da * nrad + dr
        return copy(wv, place, all_send.at[step], all_recv.at[step], lax.rem(a + da, na), lax.rem(r + dr, nrad))

    partner = r + 1 - 2 * lax.rem(r, 2)

    def relay(da, dr):
        step = da * nrad + dr + 1
        came = gat.at[lax.rem(a + na - da, na), pl.ds(pl.multiple_of(lax.rem(r + nrad - dr, nrad) * blk, 8), blk), :]
        return copy(came, came, all_send.at[step], all_recv.at[step], a, partner)

    own = copy(wv, place, all_send.at[0], all_recv.at[0], a, partner)
    learn(len(reach) - 1)
    for d in others:
        hand(*d).start()
    own.start()
    load_table.wait()
    for d in reversed(others):
        hand(*d).wait_recv()
        relay(*d).start()
    own.wait_recv()
    for d in reversed(others):
        relay(*d).wait_recv()

    w3 = lanes * na
    q3 = w3 // 4
    for aa in range(na):
        for t in range(tiles):
            rows3[aa * tiles + t] = gat[aa, :, t * 128:t * 128 + 128]
    stacked = jnp.concatenate([jnp.concatenate(
        [rows3[t, pl.ds(gi, nrad, stride=16), :] for t in range(na * tiles)], axis=1) for gi in range(16)], axis=0)
    table3 = one_hot(w3, w3, lambda c: 4 * (c % q3) + c // q3)
    by_group = permute(stacked, table3)
    for gi in range(16):
        for gj in range(4):
            b3[gi, gj] = by_group[gi * nrad:(gi + 1) * nrad, gj * q3:(gj + 1) * q3]

    l3 = Grid(a3, b3, d3, 16, 4, True)
    l4 = Grid(a4, b4, d4, 8, 2, True)
    l5 = Grid(a5, b5, d5, 4, 4, True)
    l6 = Grid(a6, b6, d6, 2, 2, True)
    l3.sweeps(PRE, True)
    l3.restrict(t3, u3, into(b4))
    l4.sweeps(PRE, True)
    w5 = w3 // 4
    q5 = w5 // 4
    nat5 = {}

    def put5(gi, gj, value):
        nat5[gi] = value
    l4.restrict(t3, u3, put5)
    x5 = permute(jnp.concatenate([nat5[i] for i in range(4)], axis=0),
                 one_hot(w5, 512, lambda c: 4 * (c % q5) + c // 128))
    for gi in range(4):
        for gj in range(4):
            b5[gi, gj] = x5[gi * nrad:(gi + 1) * nrad, gj * 128:gj * 128 + 128]
    l5.sweeps(PRE, True)
    l5.restrict(tmp_small(t3), tmp_small(u3), into(b6))
    l6.sweeps(PRE, True)
    l6.restrict(tmp_small(t3), tmp_small(u3), into(b7))
    a7[0, 0] = apply_operator(b7[0, 0], table7[...], w * na >> 7)
    l7 = Grid(a7, None, None, 1, 1, True)

    l6.add_prolonged(l7, tmp_small(t3), False)
    l6.sweeps(POST, False)
    l5.add_prolonged(l6, tmp_small(t3), False)
    l5.sweeps(POST, False)
    y5 = None
    for gj in range(4):
        x = jnp.concatenate([a5[gi, gj] for gi in range(4)], axis=0)
        r0 = permute(x, one_hot(128, w5, lambda c, gj=gj: jnp.where(c % 4 == gj, c // 4, -1)))
        y5 = r0 if y5 is None else y5 + r0
    for gi in range(4):
        u3[gi, 0] = y5[gi * nrad:(gi + 1) * nrad]
    l4.add_prolonged(Grid(u3, None, None, 4, 1, True), t3, False)
    l4.sweeps(POST, False)
    l3.add_prolonged(l4, t3, False)
    l3.sweeps(POST, False)

    for gj in range(4):
        for t in range(q3 // 128):
            nat3[gj * (q3 // 128) + t, pl.ds(0, 8), :] = jnp.zeros((8, 128), F32)
            nat3[gj * (q3 // 128) + t, pl.ds(8 + 16 * nrad, 8), :] = jnp.zeros((8, 128), F32)
            for gi in range(16):
                nat3[gj * (q3 // 128) + t, pl.ds(8 + gi, nrad, stride=16), :] = a3[gi, gj, :, t * 128:t * 128 + 128]
    begin = pl.multiple_of(r * 16, 8)
    x3 = jnp.concatenate([nat3[t, pl.ds(begin, 32), :] for t in range(w3 // 128)], axis=1)
    x3 = jnp.concatenate([x3[8:24], x3[24:32], x3[0:8]], axis=0)
    y3 = permute(x3, one_hot(w3, w3, lambda c: (c % 4) * q3 + c // 4))
    for aa in range(na):
        wg[aa] = y3[:, aa * lanes:(aa + 1) * lanes]
    v3[0, 0, :, 0:lanes] = wg[a]
    v3[0, 0, :, lanes:ext] = jnp.where(lane((32, 128)) < 64, wg[ar, :, 0:128], wg[al, :, lanes - 128:lanes])

    coarse.add_prolonged(window, t1, True)
    coarse.sweeps(POST, False)
    middle.add_prolonged(coarse, t1, True)
    middle.sweeps(POST, False)
    near_end = lax.broadcasted_iota(jnp.int32, (8, ext), 0) < 4
    fine.add_prolonged(middle, tmp_res, True, lambda x: jnp.concatenate(
        [x[0:blk], jnp.where(near_end, x[blk:blk + 8], x[blk + 8:blk + 16])], axis=0))
    fine.sweeps(POST, False)

    for gi in range(8):
        centre = fine.coef(4, gi)
        out_c, in_c, ang_c = (fine.coef(k, gi) * centre for k in (1, 2, 3))
        for gj in range(8):
            full = (g0[gi, gj] + out_c * fine.up(v0, gi, gj) + in_c * fine.down(v0, gi, gj)
                    + ang_c * (fine.right(v0, gi, gj) + fine.left(v0, gi, gj)) - centre * v0[gi, gj])
            for t in range(tiles):
                cols = slice(t * 128, t * 128 + 128)
                sol[gj, t, pl.ds(gi, blk, stride=8), :] = v0[gi, gj, 0:blk, cols]
                resid[gj, t, pl.ds(gi, blk, stride=8), :] = full[0:blk, cols]
    for side in range(2):
        @pl.when(ends[side])
        def _():
            for cp in row_copies(side):
                cp.wait_send()
    for cp in straight:
        cp.wait_send()
    for side in range(2):
        @pl.when(ends[side])
        def _():
            for cp in copies1(side, r - 1 if side == 0 else r + 1):
                cp.wait_send()
    for cp in straight1:
        cp.wait_send()
    own.wait_send()
    for d in others:
        hand(*d).wait_send()
        relay(*d).wait_send()


def join_kernel(grouped_sol, grouped_res, sol, resid, whole, out_sem):
    tiles, h = grouped_sol.shape[1:3]
    join = one_hot(256, 256, lambda c: 32 * (c % 8) + c // 8)
    ln = lax.broadcasted_iota(jnp.int32, (h, 128), 1) // 32
    copies = []
    for k, (x, out) in enumerate(((grouped_sol, sol), (grouped_res, resid))):
        for t in range(tiles):
            for b in range(4):
                halves = []
                for hf in range(2):
                    o = None
                    for p in range(4):
                        piece = roll(x[hf * 4 + p, t], 32 * (p - b), 1)
                        o = piece if o is None else jnp.where(ln == p, piece, o)
                    halves.append(o)
                cols = pl.ds((4 * t + b) * 256, 256)
                whole[k, :, cols] = permute(jnp.concatenate(halves, axis=1), join)
                copies.append(pltpu.make_async_copy(whole.at[k, :, cols], out.at[:, cols], out_sem.at[k, 4 * t + b]))
                copies[-1].start()
    for cp in copies:
        cp.wait()


def row_copies_in(side, rowbuf, colbuf, copy, row_send, row_recv, col_send, col_recv, gs, rs, pack, h, a, r):
    rows = pl.ds(0, HALO)
    to_r = r + 1 if side == 0 else r - 1
    made = [copy(x.at[rows, :], rowbuf.at[k, side], row_send.at[k, side], row_recv.at[k, side], a, to_r)
            for k, x in enumerate((gs, rs))]
    for p in range(2):
        made.append(copy(pack.at[p, rows, :], colbuf.at[p, pl.ds(h // 4 + side * HALO, HALO), :],
                         col_send.at[p, 1 + side], col_recv.at[p, 1 + side], a, to_r))
    return made


def tmp_small(ref):
    return ref.at[:, :, :, 0:128]


def solution(mesh):
    na, nrad = mesh.shape["ang"], mesh.shape["rad"]

    def local(right_side, guess):
        h, w = right_side.shape
        lanes = w // 8
        ext, tiles = lanes + 128, lanes // 128
        blk = h // 8
        s0 = blk + 8
        w3, q3 = lanes * na, lanes * na // 4
        m = lambda *s: pltpu.VMEM(s, F32)
        last = LEVELS - 1
        table = coarsest_operator(h * nrad >> last, w * na >> last, 2.0 * math.pi / (w * na >> last))
        table7 = pltpu.VMEM(table.shape, jnp.bfloat16)
        table = jnp.asarray(np.pad(table, ((0, 0), (0, max(0, 5 * h * w // table.shape[0] - table.shape[1])))))
        scratch = [
            m(h, w), m(h, w), pltpu.SemaphoreType.DMA((2,)),
            m(2, 2, HALO, w), m(2, h // 4, 128), m(2, h // 4 + 2 * HALO, 128), m(2, blk, 128), m(2, blk + 16, 128), m(4, 4, 32, ext), m(4, 4, 32, ext),
            m(2, 8, tiles + 1, 8 * s0, 128),
            m(8, 8, s0, ext), m(8, 8, s0, ext), m(6, 8, s0, 128),
            m(4, 4, 32, ext), m(4, 4, 32, ext), m(6, 4, 32, 128),
            m(2, 2, 32, ext), m(2, 2, 32, ext), m(6, 2, 32, 128),
            m(1, 1, 32, ext), m(6, 1, 32, 128),
            m(h // 8, lanes), m(na, 32, lanes), m(8, 8, s0, ext), m(4, 8, s0, ext),
            m(na, nrad * 16, lanes), m(na * tiles, nrad * 16, 128), m(w3 // 128, nrad * 16 + 16, 128),
            m(16, 4, nrad, q3), m(16, 4, nrad, q3), m(6, 16, nrad, 128),
            m(8, 2, nrad, q3), m(8, 2, nrad, q3), m(6, 8, nrad, 128),
            m(4, 4, nrad, 128), m(4, 4, nrad, 128), m(6, 4, nrad, 128),
            m(2, 2, nrad, 128), m(2, 2, nrad, 128), m(6, 2, nrad, 128),
            m(1, 1, nrad, 128), m(1, 1, nrad, 128),
            m(16, 4, nrad, q3), m(8, 4, nrad, q3),
            pltpu.SemaphoreType.DMA((2, 2)), pltpu.SemaphoreType.DMA((2, 2)),
            pltpu.SemaphoreType.DMA((2, 3)), pltpu.SemaphoreType.DMA((2, 3)),
            pltpu.SemaphoreType.DMA((2,)), pltpu.SemaphoreType.DMA((2,)),
            pltpu.SemaphoreType.DMA((2, 3)), pltpu.SemaphoreType.DMA((2, 3)),
            pltpu.SemaphoreType.DMA((na * nrad,)), pltpu.SemaphoreType.DMA((na * nrad,)),
            pltpu.SemaphoreType.REGULAR((nrad.bit_length(), 2)),
            table7, pltpu.SemaphoreType.DMA,
        ]
        grouped = pl.pallas_call(
            lambda *refs: kernel(na, nrad, h, w, *refs),
            out_shape=[jax.ShapeDtypeStruct((8, tiles, h, 128), F32)] * 2,
            in_specs=[pl.BlockSpec(memory_space=pl.ANY)] * 3,
            out_specs=[pl.BlockSpec(memory_space=pltpu.VMEM)] * 2,
            scratch_shapes=scratch,
            compiler_params=pltpu.CompilerParams(has_side_effects=True, collective_id=0, vmem_limit_bytes=53760 * 1024),
        )(right_side, guess, table)
        return pl.pallas_call(
            join_kernel,
            out_shape=[jax.ShapeDtypeStruct((h, w), F32)] * 2,
            in_specs=[pl.BlockSpec(memory_space=pltpu.VMEM)] * 2,
            out_specs=[pl.BlockSpec(memory_space=pl.ANY)] * 2,
            scratch_shapes=[m(2, h, w), pltpu.SemaphoreType.DMA((2, 4 * tiles))],
            compiler_params=pltpu.CompilerParams(vmem_limit_bytes=16 * 1024 * 1024),
        )(*grouped)

    placed = (P("rad", "ang"), P("rad", "ang"))
    return jax.shard_map(local, mesh=mesh, in_specs=placed, out_specs=placed, check_vma=False)
```

```python
import math

import jax
import jax.numpy as jnp
import numpy as np
from jax import lax
from jax.experimental import pallas as pl
from jax.experimental.pallas import tpu as pltpu
from jax.sharding import PartitionSpec as P

LEVELS = 8
PRE = 2
POST = 2
COARSE_SWEEPS = 8
F32 = jnp.float32
MESH = pl.DeviceIdType.MESH
HALO = 16


def one_hot(rows, cols, source):
    r = lax.broadcasted_iota(jnp.int32, (rows, cols), 0)
    c = lax.broadcasted_iota(jnp.int32, (rows, cols), 1)
    return jnp.where(r == source(c), 1.0, 0.0).astype(jnp.bfloat16)


def permute(x, table, count=3):
    rest, parts = x, []
    for k in range(count):
        parts.append(rest.astype(jnp.bfloat16))
        if k < count - 1:
            rest = rest - parts[-1].astype(F32)
    n = x.shape[0]
    y = jnp.dot(jnp.concatenate(parts, axis=0), table, preferred_element_type=F32)
    total = y[:n] + y[n:2 * n]
    return total + y[2 * n:] if count == 3 else total


def wide(c, lanes):
    return jnp.concatenate([c] * (lanes // c.shape[1]), axis=1) if lanes > c.shape[1] else c


def roll(x, shift, axis):
    return pltpu.roll(x, shift % x.shape[axis], axis)


def coarsest_operator(rows, cols, spacing):
    radius = (1.0 + (np.arange(rows) + 0.5) * spacing)[:, None]
    outward, inward, angular = 1.0 + 0.5 * spacing / radius, 1.0 - 0.5 * spacing / radius, 1.0 / (radius * radius)
    colour = (np.arange(rows)[:, None] + np.arange(cols)[None, :]) % 2
    g = np.eye(rows * cols).reshape(-1, rows, cols)
    v = np.zeros_like(g)
    for step in range(2 * COARSE_SWEEPS):
        p = np.pad(v, ((0, 0), (1, 1), (0, 0)))
        new = (g + outward * p[:, 2:] + inward * p[:, :-2] + angular * (np.roll(v, -1, 2) + np.roll(v, 1, 2))) / (2.0 + 2.0 * angular)
        v = np.where(colour == step % 2, new, v)
    rest, parts = v.reshape(rows * cols, rows * cols), []
    for _ in range(3):
        parts.append(rest.astype(np.float32).astype(jnp.bfloat16))
        rest = rest - parts[-1].astype(np.float64)
    return np.concatenate(parts, axis=1)


def apply_operator(x, table, cols):
    rows, per = x.shape[0], 128 // cols
    tiles = table.shape[0] // 128
    s = lax.broadcasted_iota(jnp.int32, x.shape, 0)
    block = lax.broadcasted_iota(jnp.int32, x.shape, 1) // cols
    flat = jnp.concatenate([jnp.where(s == t * per + block, x, 0.0) for t in range(tiles)], axis=1)
    flat = jnp.broadcast_to(jnp.sum(flat, axis=0, keepdims=True), (rows, flat.shape[1]))
    hi = flat.astype(jnp.bfloat16).astype(F32)
    mid = (flat - hi).astype(jnp.bfloat16).astype(F32)
    low = flat - hi - mid
    lhs = [hi, mid, low] + [jnp.zeros_like(low)] * (3 * rows // 8 % 2)
    y = jnp.dot(jnp.concatenate(lhs, axis=0).astype(jnp.bfloat16), table, preferred_element_type=F32)
    out = None
    for t in range(tiles):
        piece = lambda k, m: y[k * rows:(k + 1) * rows, (m * tiles + t) * 128:(m * tiles + t) * 128 + 128]
        total = (piece(0, 2) + piece(1, 1) + piece(2, 0)) + (piece(0, 1) + piece(1, 0)) + piece(0, 0)
        out = total if out is None else jnp.where(s // per == t, total, out)
    turn = (block + per - s % per) % per
    spread = out
    for k in range(1, per):
        spread = jnp.where(turn == k, roll(out, cols * k, 1), spread)
    return spread


def transpose4(xs):
    ln = lax.broadcasted_iota(jnp.int32, xs[0].shape, 1) // 32

    def mix(pick):
        o = pick(0)
        for q in range(1, 4):
            o = jnp.where(ln == q, pick(q), o)
        return o

    turned = [roll(mix(lambda q: xs[(q + s) % 4]), 32 * s, 1) if s else mix(lambda q: xs[q]) for s in range(4)]
    return [mix(lambda p: turned[(p - b) % 4]) for b in range(4)]


class Grid:
    def __init__(self, v, g, c, nr, nc, closed):
        self.v, self.g, self.c, self.nr, self.nc, self.closed = v, g, c, nr, nc, closed

    def rows_shift(self, x, d):
        y = roll(x, -d, 0)
        if self.closed:
            s = lax.broadcasted_iota(jnp.int32, x.shape, 0)
            y = jnp.where(s == (x.shape[0] - 1 if d > 0 else 0), 0.0, y)
        return y

    def up(self, a, gi, gj):
        return a[gi + 1, gj] if gi + 1 < self.nr else self.rows_shift(a[0, gj], 1)

    def down(self, a, gi, gj):
        return a[gi - 1, gj] if gi > 0 else self.rows_shift(a[self.nr - 1, gj], -1)

    def right(self, a, gi, gj):
        return a[gi, gj + 1] if gj + 1 < self.nc else roll(a[gi, 0], -1, 1)

    def left(self, a, gi, gj):
        return a[gi, gj - 1] if gj > 0 else roll(a[gi, self.nc - 1], 1, 1)

    def coef(self, k, gi):
        return wide(self.c[k, gi], self.v.shape[-1])

    def update(self, gi, gj):
        v = self.v
        return (self.coef(0, gi) * self.g[gi, gj] + self.coef(1, gi) * self.up(v, gi, gj)
                + self.coef(2, gi) * self.down(v, gi, gj)
                + self.coef(3, gi) * (self.right(v, gi, gj) + self.left(v, gi, gj)))

    def half(self, parity, first=False):
        for gi in range(self.nr):
            for gj in range(self.nc):
                if (gi + gj) % 2 == parity:
                    if first:
                        self.v[gi, gj] = self.coef(0, gi) * self.g[gi, gj]
                    else:
                        self.v[gi, gj] = self.update(gi, gj)

    def sweeps(self, count, zero):
        if zero:
            self.half(0, True)
            self.half(1)
            count -= 1

        def body(_, carry):
            self.half(0)
            self.half(1)
            return carry

        if count:
            lax.fori_loop(0, count, body, 0)

    def restrict(self, res, tmp, out):
        nr, nc = self.nr, self.nc
        for gi in range(nr):
            for gj in range(nc):
                if (gi + gj) % 2 == 0:
                    res[gi, gj] = self.coef(4, gi) * (self.update(gi, gj) - self.v[gi, gj])
        for big in range(nr // 2):
            for gj in range(nc):
                if gj % 2 == 0:
                    a, b = 3.0 * res[2 * big, gj], self.up(res, 2 * big + 1, gj)
                else:
                    a, b = 3.0 * res[2 * big + 1, gj], self.down(res, 2 * big, gj)
                tmp[big, gj] = (a + b) * 0.125
        for big in range(nr // 2):
            for col in range(nc // 2):
                inner = 3.0 * (tmp[big, 2 * col] + tmp[big, 2 * col + 1])
                outer = self.left(tmp, big, 2 * col) + self.right(tmp, big, 2 * col + 1)
                out(big, col, (inner + outer) * 0.5)

    def add_prolonged(self, coarse, tmp, mask, fit=lambda x: x):
        e = coarse.v
        for gi in range(self.nr):
            for col in range(coarse.nc):
                near = e[gi // 2, col]
                far = coarse.down(e, gi // 2, col) if gi % 2 == 0 else coarse.up(e, gi // 2, col)
                value = fit(0.75 * near + 0.25 * far)
                if mask:
                    value = value * self.coef(5, gi)
                tmp[gi, col] = value
        for gi in range(self.nr):
            for gj in range(self.nc):
                near = tmp[gi, gj // 2]
                far = coarse.left(tmp, gi, gj // 2) if gj % 2 == 0 else coarse.right(tmp, gi, gj // 2)
                self.v[gi, gj] = self.v[gi, gj] + (0.75 * near + 0.25 * far)


def fill_coefficients(c, nr, rows_per_group, start, total, spacing, wrap):
    for gi in range(nr):
        s = lax.broadcasted_iota(jnp.int32, (rows_per_group, 128), 0)
        if wrap:
            s = jnp.where(s >= wrap, s - rows_per_group, s)
        row = start + nr * s + gi
        inside = jnp.logical_and(row >= 0, row < total)
        radius = 1.0 + (jnp.where(inside, row, 0).astype(F32) + 0.5) * spacing
        ratio = 0.5 * spacing / radius
        angular = 1.0 / (radius * radius)
        centre = 2.0 + 2.0 * angular
        zero = jnp.zeros_like(radius)
        for k, value in enumerate((1.0 / centre, (1.0 + ratio) / centre, (1.0 - ratio) / centre,
                                   angular / centre, centre, jnp.ones_like(radius))):
            c[k, gi] = jnp.where(inside, value, zero)


def kernel(na, nrad, h, w, rs_in, gs_in, table_in, sol, resid, rs, gs, load_sem,
           rowbuf, pack, colbuf, s1, q1, t1, u1, stage, v0, g0, c0, v1, g1, c1, v2, g2, c2, v3, c3, wv, wg, tmp_res, tmp_mid,
           gat, rows3, nat3, a3, b3, d3, a4, b4, d4, a5, b5, d5, a6, b6, d6, a7, b7, t3, u3,
           row_send, row_recv, col_send, col_recv, row1_send, row1_recv, col1_send, col1_recv, all_send, all_recv, relay_send, known, table7, table_sem):
    a, r = lax.axis_index("ang"), lax.axis_index("rad")
    ar, al = lax.rem(a + 1, na), lax.rem(a + na - 1, na)
    lanes = w // 8
    ext = lanes + 128
    tiles = lanes // 128
    spacing = [2.0 * math.pi / (w * na >> l) for l in range(LEVELS)]
    lane = lambda shape: lax.broadcasted_iota(jnp.int32, shape, 1)

    spans = (pl.ds(0, 128), pl.ds(w - 128, 128), pl.ds(128, w - 256))
    loads = [[pltpu.make_async_copy(src.at[:, cols], dst.at[:, cols], load_sem.at[k, n])
              for k, (src, dst) in enumerate(((gs_in, gs), (rs_in, rs)))] for n, cols in enumerate(spans)]
    for cp in sum(loads, []):
        cp.start()
    load_table = pltpu.make_async_copy(table_in.at[:, 0:table7.shape[1]], table7, table_sem)
    load_table.start()
    blk = h // 8
    s0 = blk + 8
    barrier = pltpu.get_barrier_semaphore()

    ends = (r > 0, r < nrad - 1)

    def greet(to_r, first):
        for da in range(first, na):
            pl.semaphore_signal(barrier, inc=1, device_id=(lax.rem(a + da, na), to_r), device_id_type=MESH)

    for side in range(2):
        @pl.when(ends[side])
        def _():
            greet(r - 1 if side == 0 else r + 1, 0)
    greet(r, 1)
    reach = [2 << k for k in range(nrad.bit_length()) if 2 << k < nrad - 1]

    def announce(k):
        for side, there in ((0, r >= reach[k]), (1, r < nrad - reach[k])):
            @pl.when(there)
            def _():
                to_r = r - reach[k] if side == 0 else r + reach[k]
                pl.semaphore_signal(known.at[k, 1 - side], inc=1, device_id=(a, to_r), device_id_type=MESH)

    def learn(k):
        for side, there in ((0, r >= reach[k]), (1, r < nrad - reach[k])):
            @pl.when(there)
            def _():
                pl.semaphore_wait(known.at[k, side], 1)

    for l, c in ((0, c0), (1, c1), (2, c2)):
        fill_coefficients(c, 8 >> l, s0 if l == 0 else blk + 16, r * (h >> l), (h * nrad) >> l, spacing[l], blk + 4 if l == 0 else blk + 8)
    for l, d, n in ((3, d3, 16), (4, d4, 8), (5, d5, 4), (6, d6, 2)):
        fill_coefficients(d, n, nrad, 0, (h * nrad) >> l, spacing[l], 0)

    for cp in loads[0] + loads[1]:
        cp.wait()

    fold = h // 4
    place16 = lane((fold, 128)) // 16
    for p, (tile, base) in enumerate(((0, 0), (w - 128, 16))):
        folded = None
        for q in range(4):
            for k, x in enumerate((gs, rs)):
                piece = roll(x[q * fold:(q + 1) * fold, tile:tile + 128], 32 * q + 16 * k + base, 1)
                folded = piece if folded is None else jnp.where(place16 == 2 * q + k, piece, folded)
        pack[p] = folded

    def copy(src, dst, send, recv, to_a, to_r):
        return pltpu.make_async_remote_copy(src_ref=src, dst_ref=dst, send_sem=send, recv_sem=recv,
                                            device_id=(to_a, to_r), device_id_type=MESH)

    def row_copies(side):
        to_r = r - 1 if side == 0 else r + 1
        made = [copy(x.at[pl.ds(side * (h - n), n), :], rowbuf.at[k, side, pl.ds(side * (HALO - n), n), :],
                     row_send.at[side], row_recv.at[side], a, to_r) for k, (x, n) in enumerate(((gs, HALO), (rs, HALO // 2)))]
        for p, to_a in ((0, al), (1, ar)):
            made.append(copy(pack.at[p, pl.ds(side * (fold - HALO), HALO), :], colbuf.at[p, pl.ds(fold + side * HALO, HALO), :],
                             col_send.at[1 + side], col_recv.at[1 + side], to_a, to_r))
        return made

    def side_totals(side, to_r):
        rows, corners = gs.at[pl.ds(0, HALO + HALO // 2), :], colbuf.at[0, pl.ds(0, 2 * HALO), :]
        return [copy(rows, rows, row_send.at[side], row_recv.at[side], a, to_r),
                copy(corners, corners, col_send.at[1 + side], col_recv.at[1 + side], a, to_r)]

    pl.semaphore_wait(barrier, na * (1 + (r > 0).astype(jnp.int32) + (r < nrad - 1).astype(jnp.int32)) - 1)
    for side in range(2):
        @pl.when(ends[side])
        def _():
            for cp in row_copies(side)[2:]:
                cp.start()
    straight = [copy(pack.at[p], colbuf.at[p, pl.ds(0, fold), :], col_send.at[0], col_recv.at[0], to_a, r)
                for p, to_a in ((0, al), (1, ar))]
    straight_total = copy(pack, pack, col_send.at[0], col_recv.at[0], al, r)
    for cp in straight:
        cp.start()
    for cp in loads[2]:
        cp.wait()
    for side in range(2):
        @pl.when(ends[side])
        def _():
            for cp in row_copies(side)[:2]:
                cp.start()

    spread = one_hot(256, 256, lambda c: 8 * (c % 32) + c // 32)
    halo_spread = one_hot(128, 256, lambda c: jnp.where(
        (c + 2) % 16 < 8, -1, jnp.where((c + 2) % 16 >= 12, -1,
                                        (c // 128) * 16 + (c % 128) // 16 + jnp.where(c % 16 >= 8, 8 * (c % 16 - 8), 8 * (c % 16 - 6) + 32))))

    def split_rows(x, count, put):
        for t in range(tiles):
            parts = [permute(x(slice((4 * t + b) * 256, (4 * t + b) * 256 + 256)), spread) for b in range(4)]
            for half in range(2):
                for g, o in enumerate(transpose4([p[:, half * 128:half * 128 + 128] for p in parts])):
                    put(4 * half + g, t, o)

    def put_own(k):
        def put(gj, t, value):
            stage[k, gj, t, pl.ds(0, h), :] = value
        return put

    for k, x in enumerate((gs, rs)):
        split_rows(lambda cols, x=x: x[:, cols], h, put_own(k))
    for k, dst in enumerate((v0, g0)):
        for gj in range(8):
            for gi in range(8):
                for t in range(tiles):
                    dst[gi, gj, 0:blk, t * 128:t * 128 + 128] = stage[k, gj, t, pl.ds(gi, blk, stride=8), :]
    for k in range(2):
        for gj in range(8):
            for t in range(tiles + 1):
                stage[k, gj, t, pl.ds(h + HALO, 8 * s0 - h - 2 * HALO), :] = jnp.zeros((8 * s0 - h - 2 * HALO, 128), F32)

    for side in range(2):
        @pl.when(ends[1 - side])
        def _():
            for cp in side_totals(side, r + 1 if side == 0 else r - 1):
                cp.wait_recv()
    straight_total.wait_recv()
    announce(0)
    at = (h, 8 * s0 - HALO)
    def put_edges(gj, t, value):
        for k in range(2):
            for side in range(2):
                n = 2 * k + side
                stage[k, gj, t, pl.ds(at[side], HALO), :] = value[n * HALO:(n + 1) * HALO]

    def edge(k, side, cols):
        if k == 0:
            return [jnp.where(ends[1 - side], rowbuf[k, side, :, cols], 0.0)]
        half = HALO // 2
        x = jnp.where(ends[1 - side], rowbuf[k, side, side * half:side * half + half, cols], 0.0)
        return [jnp.zeros_like(x), x] if side else [x, jnp.zeros_like(x)]

    split_rows(lambda cols: jnp.concatenate(sum((edge(k, side, cols) for k in range(2) for side in range(2)), []), axis=0),
               4 * HALO, put_edges)

    def beside(first, count, shift):
        right, left = colbuf[0, pl.ds(first, count), :], colbuf[1, pl.ds(first, count), :]
        return jnp.where(lane((count, 128)) < 32, roll(right, -shift, 1), roll(left, 32 - shift, 1))

    strips = [beside(0, fold, 32 * q) for q in range(4)]
    strips.append(jnp.where(ends[1], beside(fold, HALO, 0), 0.0))
    strips.append(jnp.where(ends[0], beside(fold + HALO, HALO, 96), 0.0))
    strips = jnp.concatenate(strips, axis=0)
    y = permute(strips, halo_spread)
    for k in range(2):
        for gj in range(8):
            piece = roll(y[:, k * 128:k * 128 + 128], -16 * gj - 8, 1)
            stage[k, gj, tiles, pl.ds(0, h + HALO), :] = piece[0:h + HALO]
            stage[k, gj, tiles, pl.ds(at[1], HALO), :] = piece[h + HALO:]
    for k, dst in enumerate((v0, g0)):
        for gj in range(8):
            for gi in range(8):
                for t in range(tiles):
                    dst[gi, gj, blk:s0, t * 128:t * 128 + 128] = stage[k, gj, t, pl.ds(h + gi, s0 - blk, stride=8), :]
                dst[gi, gj, :, lanes:ext] = stage[k, gj, tiles, pl.ds(gi, s0, stride=8), :]

    fine = Grid(v0, g0, c0, 8, 8, False)
    middle = Grid(v1, g1, c1, 4, 4, False)
    coarse = Grid(v2, g2, c2, 2, 2, False)
    window = Grid(v3, None, None, 1, 1, False)

    def into(ref):
        def put(gi, gj, value):
            ref[gi, gj] = value
        return put

    fine.sweeps(PRE, False)

    def put1(gi, gj, value):
        g1[gi, gj, 0:blk, 0:lanes] = value[0:blk, 0:lanes]
    fine.restrict(tmp_res, tmp_mid, put1)

    for side, first in ((0, blk), (1, blk + 8)):
        @pl.when(jnp.logical_not(ends[1 - side]))
        def _():
            g1[:, :, first:first + 8, 0:lanes] = jnp.zeros((4, 4, 8, lanes), F32)
    slot = lane((blk, 128)) // 8
    left_edge = right_edge = None
    for g in range(16):
        lo = roll(g1[g // 4, g % 4, 0:blk, 0:128], 8 * g, 1)
        hi = roll(g1[g // 4, g % 4, 0:blk, lanes - 128:lanes], 8 * g + 8, 1)
        left_edge = lo if g == 0 else jnp.where(slot == g, lo, left_edge)
        right_edge = hi if g == 0 else jnp.where(slot == g, hi, right_edge)
    s1[0] = left_edge
    s1[1] = right_edge

    def copies1(side, to_r):
        first = 0 if side == 0 else blk - 8
        made = [copy(g1.at[:, :, pl.ds(first, 8), pl.ds(0, lanes)], g1.at[:, :, pl.ds(blk + 8 * side, 8), pl.ds(0, lanes)],
                     row1_send.at[side], row1_recv.at[side], a, to_r)]
        for p, to_a in ((0, al), (1, ar)):
            made.append(copy(s1.at[p, pl.ds(first, 8), :], q1.at[p, pl.ds(blk + 8 * side, 8), :],
                             col1_send.at[1 + side], col1_recv.at[1 + side], to_a, to_r))
        return made

    def totals1(side, to_r):
        corners = q1.at[0, pl.ds(0, 16), :]
        return [copies1(side, to_r)[0], copy(corners, corners, col1_send.at[1 + side], col1_recv.at[1 + side], a, to_r)]

    straight1 = [copy(s1.at[p], q1.at[p, pl.ds(0, blk), :], col1_send.at[0], col1_recv.at[0], to_a, r)
                 for p, to_a in ((0, al), (1, ar))]
    straight1_total = copy(s1, s1, col1_send.at[0], col1_recv.at[0], al, r)
    for side in range(2):
        @pl.when(ends[side])
        def _():
            for cp in copies1(side, r - 1 if side == 0 else r + 1)[1:]:
                cp.start()
    for cp in straight1:
        cp.start()
    for side in range(2):
        @pl.when(ends[side])
        def _():
            copies1(side, r - 1 if side == 0 else r + 1)[0].start()
    learn(0)
    for k in range(1, len(reach)):
        announce(k)
        if k < len(reach) - 1:
            learn(k)
    for side in range(2):
        @pl.when(ends[1 - side])
        def _():
            for cp in totals1(side, r + 1 if side == 0 else r - 1):
                cp.wait_recv()
    straight1_total.wait_recv()
    wl = lane((blk + 16, 128))
    sub = lax.broadcasted_iota(jnp.int32, (blk + 16, 128), 0)
    got = jnp.where(sub < blk, 1, jnp.where(sub < blk + 8, nrad - 1 - r, r)) > 0
    strip_r, strip_l = jnp.where(got, q1[0], 0.0), jnp.where(got, q1[1], 0.0)
    for g in range(16):
        g1[g // 4, g % 4, :, lanes:ext] = jnp.where(
            wl < 8, roll(strip_r, -8 * g, 1), jnp.where(wl >= 120, roll(strip_l, 120 - 8 * g, 1), 0.0))
    middle.sweeps(PRE, True)
    middle.restrict(t1, u1, into(g2))
    coarse.sweeps(PRE, True)

    def put3(gi, gj, value):
        wv[...] = value[0:blk, 0:lanes]
    coarse.restrict(t1, u1, put3)

    place = gat.at[a, pl.ds(pl.multiple_of(r * blk, 8), blk), :]
    gat[a, pl.ds(pl.multiple_of(r * blk, 8), blk), :] = wv[...]

    z, core, nz = lax.div(r, 2), lax.rem(r, 2), nrad // 2

    def hand(da, zt):
        to_a = lax.rem(a + da, na)
        return copy(wv, place, all_send, all_recv.at[a, z], to_a, 2 * zt + 1)

    def relay(da, zs):
        from_a = lax.rem(a + na - da, na)
        came = gat.at[from_a, pl.ds(pl.multiple_of(2 * zs * blk, 8), 2 * blk), :]
        return copy(came, came, relay_send.at[1 if da else 0], all_recv.at[from_a, zs], a, r + 1 - 2 * core)

    own = copy(wv, place, all_send, all_recv.at[a, z], a, r + 1 - 2 * core)

    def sent(ref, send):
        copy(ref, ref, send, all_recv.at[0, 0], a, r + 1 - 2 * core).wait_send()

    def each_chip(near_first, do):
        for k in reversed(range(nz)) if near_first else range(nz):
            zt = jnp.where(z < nz // 2, nz - 1 - k, k)
            for da in reversed(range(na)):
                if da:
                    do(da, zt)
                else:
                    pl.when(zt != z)(lambda: do(0, zt))

    def pass_on(da, zs):
        relay(da, zs).wait_recv()
        relay(da, zs).start()

    learn(len(reach) - 1)
    own.start()
    each_chip(False, lambda da, zt: hand(da, zt).start())
    load_table.wait()

    pl.when(core == 1)(lambda: each_chip(True, pass_on))
    pl.when(core == 0)(lambda: each_chip(True, lambda da, zs: relay(da, zs).wait_recv()))
    own.wait_recv()

    w3 = lanes * na
    q3 = w3 // 4
    for aa in range(na):
        for t in range(tiles):
            rows3[aa * tiles + t] = gat[aa, :, t * 128:t * 128 + 128]
    stacked = jnp.concatenate([jnp.concatenate(
        [rows3[t, pl.ds(gi, nrad, stride=16), :] for t in range(na * tiles)], axis=1) for gi in range(16)], axis=0)
    table3 = one_hot(w3, w3, lambda c: 4 * (c % q3) + c // q3)
    by_group = permute(stacked, table3, 2)
    for gi in range(16):
        for gj in range(4):
            b3[gi, gj] = by_group[gi * nrad:(gi + 1) * nrad, gj * q3:(gj + 1) * q3]

    l3 = Grid(a3, b3, d3, 16, 4, True)
    l4 = Grid(a4, b4, d4, 8, 2, True)
    l5 = Grid(a5, b5, d5, 4, 4, True)
    l6 = Grid(a6, b6, d6, 2, 2, True)
    l3.sweeps(PRE, True)
    l3.restrict(t3, u3, into(b4))
    l4.sweeps(PRE, True)
    w5 = w3 // 4
    q5 = w5 // 4
    nat5 = {}

    def put5(gi, gj, value):
        nat5[gi] = value
    l4.restrict(t3, u3, put5)
    x5 = permute(jnp.concatenate([nat5[i] for i in range(4)], axis=0),
                 one_hot(w5, 512, lambda c: 4 * (c % q5) + c // 128), 2)
    for gi in range(4):
        for gj in range(4):
            b5[gi, gj] = x5[gi * nrad:(gi + 1) * nrad, gj * 128:gj * 128 + 128]
    l5.sweeps(PRE, True)
    l5.restrict(tmp_small(t3), tmp_small(u3), into(b6))
    l6.sweeps(PRE, True)
    l6.restrict(tmp_small(t3), tmp_small(u3), into(b7))
    a7[0, 0] = apply_operator(b7[0, 0], table7[...], w * na >> 7)
    l7 = Grid(a7, None, None, 1, 1, True)

    l6.add_prolonged(l7, tmp_small(t3), False)
    l6.sweeps(POST, False)
    l5.add_prolonged(l6, tmp_small(t3), False)
    l5.sweeps(POST, False)
    y5 = None
    for gj in range(4):
        x = jnp.concatenate([a5[gi, gj] for gi in range(4)], axis=0)
        r0 = permute(x, one_hot(128, w5, lambda c, gj=gj: jnp.where(c % 4 == gj, c // 4, -1)))
        y5 = r0 if y5 is None else y5 + r0
    for gi in range(4):
        u3[gi, 0] = y5[gi * nrad:(gi + 1) * nrad]
    l4.add_prolonged(Grid(u3, None, None, 4, 1, True), t3, False)
    l4.sweeps(POST, False)
    l3.add_prolonged(l4, t3, False)
    l3.sweeps(POST, False)

    for gj in range(4):
        for t in range(q3 // 128):
            nat3[gj * (q3 // 128) + t, pl.ds(0, 8), :] = jnp.zeros((8, 128), F32)
            nat3[gj * (q3 // 128) + t, pl.ds(8 + 16 * nrad, 8), :] = jnp.zeros((8, 128), F32)
            for gi in range(16):
                nat3[gj * (q3 // 128) + t, pl.ds(8 + gi, nrad, stride=16), :] = a3[gi, gj, :, t * 128:t * 128 + 128]
    begin = pl.multiple_of(r * 16, 8)
    x3 = jnp.concatenate([nat3[t, pl.ds(begin, 32), :] for t in range(w3 // 128)], axis=1)
    x3 = jnp.concatenate([x3[8:24], x3[24:32], x3[0:8]], axis=0)
    y3 = permute(x3, one_hot(w3, w3, lambda c: (c % 4) * q3 + c // 4))
    for aa in range(na):
        wg[aa] = y3[:, aa * lanes:(aa + 1) * lanes]
    v3[0, 0, :, 0:lanes] = wg[a]
    v3[0, 0, :, lanes:ext] = jnp.where(lane((32, 128)) < 64, wg[ar, :, 0:128], wg[al, :, lanes - 128:lanes])

    coarse.add_prolonged(window, t1, True)
    coarse.sweeps(POST, False)
    middle.add_prolonged(coarse, t1, True)
    middle.sweeps(POST, False)
    near_end = lax.broadcasted_iota(jnp.int32, (8, ext), 0) < 4
    fine.add_prolonged(middle, tmp_res, True, lambda x: jnp.concatenate(
        [x[0:blk], jnp.where(near_end, x[blk:blk + 8], x[blk + 8:blk + 16])], axis=0))
    fine.sweeps(POST, False)

    for gi in range(8):
        centre = fine.coef(4, gi)
        out_c, in_c, ang_c = (fine.coef(k, gi) * centre for k in (1, 2, 3))
        for gj in range(8):
            full = (g0[gi, gj] + out_c * fine.up(v0, gi, gj) + in_c * fine.down(v0, gi, gj)
                    + ang_c * (fine.right(v0, gi, gj) + fine.left(v0, gi, gj)) - centre * v0[gi, gj])
            for t in range(tiles):
                cols = slice(t * 128, t * 128 + 128)
                sol[gj, t, pl.ds(gi, blk, stride=8), :] = v0[gi, gj, 0:blk, cols]
                resid[gj, t, pl.ds(gi, blk, stride=8), :] = full[0:blk, cols]
    for side in range(2):
        @pl.when(ends[side])
        def _():
            for cp in side_totals(side, r - 1 if side == 0 else r + 1):
                cp.wait_send()
    straight_total.wait_send()
    for side in range(2):
        @pl.when(ends[side])
        def _():
            for cp in totals1(side, r - 1 if side == 0 else r + 1):
                cp.wait_send()
    straight1_total.wait_send()
    sent(gat.at[:, pl.ds(0, nz * blk), :], all_send)

    @pl.when(core == 1)
    def _():
        sent(gat.at[pl.ds(0, na - 1)], relay_send.at[1])
        sent(gat.at[0, pl.ds(0, (nz - 1) * 2 * blk), :], relay_send.at[0])


def join_kernel(grouped_sol, grouped_res, sol, resid, whole, out_sem):
    tiles, h = grouped_sol.shape[1:3]
    join = one_hot(256, 256, lambda c: 32 * (c % 8) + c // 8)
    copies = []
    for k, (x, out) in enumerate(((grouped_sol, sol), (grouped_res, resid))):
        for t in range(tiles):
            halves = [transpose4([x[hf * 4 + p, t] for p in range(4)]) for hf in range(2)]
            for b in range(4):
                cols = pl.ds((4 * t + b) * 256, 256)
                whole[k, :, cols] = permute(jnp.concatenate([halves[0][b], halves[1][b]], axis=1), join, 2)
                copies.append(pltpu.make_async_copy(whole.at[k, :, cols], out.at[:, cols], out_sem.at[k, 4 * t + b]))
                copies[-1].start()
    for cp in copies:
        cp.wait()


def tmp_small(ref):
    return ref.at[:, :, :, 0:128]


def solution(mesh):
    na, nrad = mesh.shape["ang"], mesh.shape["rad"]

    def local(right_side, guess):
        h, w = right_side.shape
        lanes = w // 8
        ext, tiles = lanes + 128, lanes // 128
        blk = h // 8
        s0 = blk + 8
        w3, q3 = lanes * na, lanes * na // 4
        m = lambda *s: pltpu.VMEM(s, F32)
        last = LEVELS - 1
        table = coarsest_operator(h * nrad >> last, w * na >> last, 2.0 * math.pi / (w * na >> last))
        table7 = pltpu.VMEM(table.shape, jnp.bfloat16)
        table = jnp.asarray(np.pad(table, ((0, 0), (0, max(0, 5 * h * w // table.shape[0] - table.shape[1])))))
        scratch = [
            m(h, w), m(h, w), pltpu.SemaphoreType.DMA((2, 3)),
            m(2, 2, HALO, w), m(2, h // 4, 128), m(2, h // 4 + 2 * HALO, 128), m(2, blk, 128), m(2, blk + 16, 128), m(4, 4, 32, ext), m(4, 4, 32, ext),
            m(2, 8, tiles + 1, 8 * s0, 128),
            m(8, 8, s0, ext), m(8, 8, s0, ext), m(6, 8, s0, 128),
            m(4, 4, 32, ext), m(4, 4, 32, ext), m(6, 4, 32, 128),
            m(2, 2, 32, ext), m(2, 2, 32, ext), m(6, 2, 32, 128),
            m(1, 1, 32, ext), m(6, 1, 32, 128),
            m(h // 8, lanes), m(na, 32, lanes), m(8, 8, s0, ext), m(4, 8, s0, ext),
            m(na, nrad * 16, lanes), m(na * tiles, nrad * 16, 128), m(w3 // 128, nrad * 16 + 16, 128),
            m(16, 4, nrad, q3), m(16, 4, nrad, q3), m(6, 16, nrad, 128),
            m(8, 2, nrad, q3), m(8, 2, nrad, q3), m(6, 8, nrad, 128),
            m(4, 4, nrad, 128), m(4, 4, nrad, 128), m(6, 4, nrad, 128),
            m(2, 2, nrad, 128), m(2, 2, nrad, 128), m(6, 2, nrad, 128),
            m(1, 1, nrad, 128), m(1, 1, nrad, 128),
            m(16, 4, nrad, q3), m(8, 4, nrad, q3),
            *[pltpu.SemaphoreType.DMA((n,)) for n in (2, 2, 3, 3, 2, 2, 3, 3)],
            pltpu.SemaphoreType.DMA, pltpu.SemaphoreType.DMA((na, nrad // 2)), pltpu.SemaphoreType.DMA((2,)),
            pltpu.SemaphoreType.REGULAR((max(1, len([k for k in range(nrad.bit_length()) if 2 << k < nrad - 1])), 2)),
            table7, pltpu.SemaphoreType.DMA,
        ]
        grouped = pl.pallas_call(
            lambda *refs: kernel(na, nrad, h, w, *refs),
            out_shape=[jax.ShapeDtypeStruct((8, tiles, h, 128), F32)] * 2,
            in_specs=[pl.BlockSpec(memory_space=pl.ANY)] * 3,
            out_specs=[pl.BlockSpec(memory_space=pltpu.VMEM)] * 2,
            scratch_shapes=scratch,
            compiler_params=pltpu.CompilerParams(has_side_effects=True, collective_id=0, vmem_limit_bytes=53760 * 1024),
        )(right_side, guess, table)
        return pl.pallas_call(
            join_kernel,
            out_shape=[jax.ShapeDtypeStruct((h, w), F32)] * 2,
            in_specs=[pl.BlockSpec(memory_space=pltpu.VMEM)] * 2,
            out_specs=[pl.BlockSpec(memory_space=pl.ANY)] * 2,
            scratch_shapes=[m(2, h, w), pltpu.SemaphoreType.DMA((2, 4 * tiles))],
            compiler_params=pltpu.CompilerParams(vmem_limit_bytes=16 * 1024 * 1024),
        )(*grouped)

    placed = (P("rad", "ang"), P("rad", "ang"))
    return jax.shard_map(local, mesh=mesh, in_specs=placed, out_specs=placed, check_vma=False)
```

```python
import math

import jax
import jax.numpy as jnp
import numpy as np
from jax import lax
from jax.experimental import pallas as pl
from jax.experimental.pallas import tpu as pltpu
from jax.sharding import PartitionSpec as P

LEVELS = 8
PRE = 2
POST = 2
COARSE_SWEEPS = 8
F32 = jnp.float32
MESH = pl.DeviceIdType.MESH
HALO = 16


def one_hot(rows, cols, source):
    r = lax.broadcasted_iota(jnp.int32, (rows, cols), 0)
    c = lax.broadcasted_iota(jnp.int32, (rows, cols), 1)
    return jnp.where(r == source(c), 1.0, 0.0).astype(jnp.bfloat16)


def permute(x, table, count=3):
    rest, parts = x, []
    for k in range(count):
        parts.append(rest.astype(jnp.bfloat16))
        if k < count - 1:
            rest = rest - parts[-1].astype(F32)
    n = x.shape[0]
    y = jnp.dot(jnp.concatenate(parts, axis=0), table, preferred_element_type=F32)
    total = y[:n] + y[n:2 * n]
    return total + y[2 * n:] if count == 3 else total


def wide(c, lanes):
    return jnp.concatenate([c] * (lanes // c.shape[1]), axis=1) if lanes > c.shape[1] else c


def roll(x, shift, axis):
    return pltpu.roll(x, shift % x.shape[axis], axis)


def coarsest_operator(rows, cols, spacing):
    radius = (1.0 + (np.arange(rows) + 0.5) * spacing)[:, None]
    outward, inward, angular = 1.0 + 0.5 * spacing / radius, 1.0 - 0.5 * spacing / radius, 1.0 / (radius * radius)
    colour = (np.arange(rows)[:, None] + np.arange(cols)[None, :]) % 2
    g = np.eye(rows * cols).reshape(-1, rows, cols)
    v = np.zeros_like(g)
    for step in range(2 * COARSE_SWEEPS):
        p = np.pad(v, ((0, 0), (1, 1), (0, 0)))
        new = (g + outward * p[:, 2:] + inward * p[:, :-2] + angular * (np.roll(v, -1, 2) + np.roll(v, 1, 2))) / (2.0 + 2.0 * angular)
        v = np.where(colour == step % 2, new, v)
    rest, parts = v.reshape(rows * cols, rows * cols), []
    for _ in range(3):
        parts.append(rest.astype(np.float32).astype(jnp.bfloat16))
        rest = rest - parts[-1].astype(np.float64)
    return np.concatenate(parts, axis=1)


def apply_operator(x, table, cols):
    rows, per = x.shape[0], 128 // cols
    tiles = table.shape[0] // 128
    s = lax.broadcasted_iota(jnp.int32, x.shape, 0)
    block = lax.broadcasted_iota(jnp.int32, x.shape, 1) // cols
    flat = jnp.concatenate([jnp.where(s == t * per + block, x, 0.0) for t in range(tiles)], axis=1)
    flat = jnp.broadcast_to(jnp.sum(flat, axis=0, keepdims=True), (rows, flat.shape[1]))
    hi = flat.astype(jnp.bfloat16).astype(F32)
    mid = (flat - hi).astype(jnp.bfloat16).astype(F32)
    low = flat - hi - mid
    lhs = [hi, mid, low] + [jnp.zeros_like(low)] * (3 * rows // 8 % 2)
    y = jnp.dot(jnp.concatenate(lhs, axis=0).astype(jnp.bfloat16), table, preferred_element_type=F32)
    out = None
    for t in range(tiles):
        piece = lambda k, m: y[k * rows:(k + 1) * rows, (m * tiles + t) * 128:(m * tiles + t) * 128 + 128]
        total = (piece(0, 2) + piece(1, 1) + piece(2, 0)) + (piece(0, 1) + piece(1, 0)) + piece(0, 0)
        out = total if out is None else jnp.where(s // per == t, total, out)
    turn = (block + per - s % per) % per
    spread = out
    for k in range(1, per):
        spread = jnp.where(turn == k, roll(out, cols * k, 1), spread)
    return spread


def transpose4(xs):
    ln = lax.broadcasted_iota(jnp.int32, xs[0].shape, 1) // 32

    def mix(pick):
        o = pick(0)
        for q in range(1, 4):
            o = jnp.where(ln == q, pick(q), o)
        return o

    turned = [roll(mix(lambda q: xs[(q + s) % 4]), 32 * s, 1) if s else mix(lambda q: xs[q]) for s in range(4)]
    return [mix(lambda p: turned[(p - b) % 4]) for b in range(4)]


class Grid:
    def __init__(self, v, g, c, nr, nc, closed):
        self.v, self.g, self.c, self.nr, self.nc, self.closed = v, g, c, nr, nc, closed

    def rows_shift(self, x, d):
        y = roll(x, -d, 0)
        if self.closed:
            s = lax.broadcasted_iota(jnp.int32, x.shape, 0)
            y = jnp.where(s == (x.shape[0] - 1 if d > 0 else 0), 0.0, y)
        return y

    def up(self, a, gi, gj):
        return a[gi + 1, gj] if gi + 1 < self.nr else self.rows_shift(a[0, gj], 1)

    def down(self, a, gi, gj):
        return a[gi - 1, gj] if gi > 0 else self.rows_shift(a[self.nr - 1, gj], -1)

    def right(self, a, gi, gj):
        return a[gi, gj + 1] if gj + 1 < self.nc else roll(a[gi, 0], -1, 1)

    def left(self, a, gi, gj):
        return a[gi, gj - 1] if gj > 0 else roll(a[gi, self.nc - 1], 1, 1)

    def coef(self, k, gi):
        return wide(self.c[k, gi], self.v.shape[-1])

    def set_source(self, gi, gj, value):
        self.g[gi, gj] = self.coef(0, gi) * value

    def update(self, gi, gj):
        v = self.v
        return (self.g[gi, gj] + self.coef(1, gi) * self.up(v, gi, gj)
                + self.coef(2, gi) * self.down(v, gi, gj)
                + self.coef(3, gi) * (self.right(v, gi, gj) + self.left(v, gi, gj)))

    def extent(self, gi, gj, depth, rows, cols):
        near = lambda i, n: i < depth or i >= n - depth
        return (self.v.shape[2] if near(gi, self.nr) else rows), (self.v.shape[3] if near(gj, self.nc) else cols)

    def half_near(self, parity, depth, rows, cols):
        for gi in range(self.nr):
            for gj in range(self.nc):
                if (gi + gj) % 2 == parity:
                    m, n = self.extent(gi, gj, depth, rows, cols)
                    self.v[gi, gj, 0:m, 0:n] = self.update(gi, gj)[0:m, 0:n]

    def half_far(self, parity, depth, rows, cols):
        full_m, full_n = self.v.shape[2:]
        for gi in range(self.nr):
            for gj in range(self.nc):
                m, n = self.extent(gi, gj, depth, rows, cols)
                if (gi + gj) % 2 == parity and (m < full_m or n < full_n):
                    value = self.update(gi, gj)
                    if m < full_m:
                        self.v[gi, gj, m:full_m, :] = value[m:full_m]
                    if n < full_n:
                        self.v[gi, gj, 0:m, n:full_n] = value[0:m, n:full_n]

    def half(self, parity, first=False):
        for gi in range(self.nr):
            for gj in range(self.nc):
                if (gi + gj) % 2 == parity:
                    if first:
                        self.v[gi, gj] = self.g[gi, gj]
                    else:
                        self.v[gi, gj] = self.update(gi, gj)

    def sweeps(self, count, zero):
        if zero:
            self.half(0, True)
            self.half(1)
            count -= 1

        for _ in range(count):
            self.half(0)
            self.half(1)

    def restrict(self, res, tmp, out, own=None):
        nr, nc = self.nr, self.nc
        size = lambda gi, gj: self.extent(gi, gj, 1, *own) if own else self.v.shape[2:]
        for gi in range(nr):
            for gj in range(nc):
                if (gi + gj) % 2 == 0:
                    m, n = size(gi, gj)
                    res[gi, gj, 0:m, 0:n] = (self.coef(4, gi) * (self.update(gi, gj) - self.v[gi, gj]))[0:m, 0:n]
        for big in range(nr // 2):
            for gj in range(nc):
                if gj % 2 == 0:
                    a, b = 3.0 * res[2 * big, gj], self.up(res, 2 * big + 1, gj)
                else:
                    a, b = 3.0 * res[2 * big + 1, gj], self.down(res, 2 * big, gj)
                m, n = own[0] if own else self.v.shape[2], size(0, gj)[1]
                tmp[big, gj, 0:m, 0:n] = ((a + b) * 0.125)[0:m, 0:n]
        for big in range(nr // 2):
            for col in range(nc // 2):
                inner = 3.0 * (tmp[big, 2 * col] + tmp[big, 2 * col + 1])
                outer = self.left(tmp, big, 2 * col) + self.right(tmp, big, 2 * col + 1)
                out(big, col, (inner + outer) * 0.5)

    def add_prolonged(self, coarse, tmp, mask, fit=lambda x: x):
        e = coarse.v
        for gi in range(self.nr):
            for col in range(coarse.nc):
                near = e[gi // 2, col]
                far = coarse.down(e, gi // 2, col) if gi % 2 == 0 else coarse.up(e, gi // 2, col)
                value = fit(0.75 * near + 0.25 * far)
                if mask:
                    value = value * self.coef(5, gi)
                tmp[gi, col] = value
        for gi in range(self.nr):
            for gj in range(self.nc):
                if (gi + gj) % 2 == 0:
                    continue
                near = tmp[gi, gj // 2]
                far = coarse.left(tmp, gi, gj // 2) if gj % 2 == 0 else coarse.right(tmp, gi, gj // 2)
                self.v[gi, gj] = self.v[gi, gj] + (0.75 * near + 0.25 * far)


def fill_coefficients(c, nr, rows_per_group, start, total, spacing, wrap):
    for gi in range(nr):
        s = lax.broadcasted_iota(jnp.int32, (rows_per_group, 128), 0)
        if wrap:
            s = jnp.where(s >= wrap, s - rows_per_group, s)
        row = start + nr * s + gi
        inside = jnp.logical_and(row >= 0, row < total)
        radius = 1.0 + (jnp.where(inside, row, 0).astype(F32) + 0.5) * spacing
        ratio = 0.5 * spacing / radius
        angular = 1.0 / (radius * radius)
        centre = 2.0 + 2.0 * angular
        zero = jnp.zeros_like(radius)
        for k, value in enumerate((1.0 / centre, (1.0 + ratio) / centre, (1.0 - ratio) / centre,
                                   angular / centre, centre, jnp.ones_like(radius))):
            c[k, gi] = jnp.where(inside, value, zero)


def kernel(na, nrad, h, w, rs_in, gs_in, table_in, sol, resid, rs, gs, load_sem,
           rowbuf, pack, colbuf, s1, q1, t1, u1, stage, v0, g0, c0, v1, g1, c1, v2, g2, c2, v3, c3, wv, wg, tmp_res, tmp_mid,
           gat, rows3, nat3, a3, b3, d3, a4, b4, d4, a5, b5, d5, a6, b6, d6, a7, b7, t3, u3,
           row_send, row_recv, col_send, col_recv, row1_send, row1_recv, col1_send, col1_recv, all_send, all_recv, relay_send, known, table7, table_sem):
    a, r = lax.axis_index("ang"), lax.axis_index("rad")
    ar, al = lax.rem(a + 1, na), lax.rem(a + na - 1, na)
    lanes = w // 8
    ext = lanes + 128
    tiles = lanes // 128
    spacing = [2.0 * math.pi / (w * na >> l) for l in range(LEVELS)]
    lane = lambda shape: lax.broadcasted_iota(jnp.int32, shape, 1)

    spans = (pl.ds(0, 128), pl.ds(w - 128, 128), pl.ds(128, w - 256))
    loads = [[pltpu.make_async_copy(src.at[:, cols], dst.at[:, cols], load_sem.at[k, n])
              for k, (src, dst) in enumerate(((gs_in, gs), (rs_in, rs)))] for n, cols in enumerate(spans)]
    for cp in sum(loads, []):
        cp.start()
    load_table = pltpu.make_async_copy(table_in.at[:, 0:table7.shape[1]], table7, table_sem)
    load_table.start()
    blk = h // 8
    s0 = blk + 8
    barrier = pltpu.get_barrier_semaphore()

    ends = (r > 0, r < nrad - 1)

    def greet(to_r, first):
        for da in range(first, na):
            pl.semaphore_signal(barrier, inc=1, device_id=(lax.rem(a + da, na), to_r), device_id_type=MESH)

    for side in range(2):
        @pl.when(ends[side])
        def _():
            greet(r - 1 if side == 0 else r + 1, 0)
    greet(r, 1)
    reach = [2 << k for k in range(nrad.bit_length()) if 2 << k < nrad - 1]

    def announce(k):
        for side, there in ((0, r >= reach[k]), (1, r < nrad - reach[k])):
            @pl.when(there)
            def _():
                to_r = r - reach[k] if side == 0 else r + reach[k]
                pl.semaphore_signal(known.at[k, 1 - side], inc=1, device_id=(a, to_r), device_id_type=MESH)

    def learn(k):
        for side, there in ((0, r >= reach[k]), (1, r < nrad - reach[k])):
            @pl.when(there)
            def _():
                pl.semaphore_wait(known.at[k, side], 1)

    for l, c in ((0, c0), (1, c1), (2, c2)):
        fill_coefficients(c, 8 >> l, s0 if l == 0 else blk + 16, r * (h >> l), (h * nrad) >> l, spacing[l], blk + 4 if l == 0 else blk + 8)
    for l, d, n in ((3, d3, 16), (4, d4, 8), (5, d5, 4), (6, d6, 2)):
        fill_coefficients(d, n, nrad, 0, (h * nrad) >> l, spacing[l], 0)

    for cp in loads[0] + loads[1]:
        cp.wait()

    fold = h // 4
    place16 = lane((fold, 128)) // 16
    for p, (tile, base) in enumerate(((0, 0), (w - 128, 16))):
        folded = None
        for q in range(4):
            for k, x in enumerate((gs, rs)):
                piece = roll(x[q * fold:(q + 1) * fold, tile:tile + 128], 32 * q + 16 * k + base, 1)
                folded = piece if folded is None else jnp.where(place16 == 2 * q + k, piece, folded)
        pack[p] = folded

    def copy(src, dst, send, recv, to_a, to_r):
        return pltpu.make_async_remote_copy(src_ref=src, dst_ref=dst, send_sem=send, recv_sem=recv,
                                            device_id=(to_a, to_r), device_id_type=MESH)

    def row_copies(side):
        to_r = r - 1 if side == 0 else r + 1
        made = [copy(x.at[pl.ds(side * (h - n), n), :], rowbuf.at[k, side, pl.ds(side * (HALO - n), n), :],
                     row_send.at[side], row_recv.at[side], a, to_r) for k, (x, n) in enumerate(((gs, HALO), (rs, HALO // 2)))]
        for p, to_a in ((0, al), (1, ar)):
            made.append(copy(pack.at[p, pl.ds(side * (fold - HALO), HALO), :], colbuf.at[p, pl.ds(fold + side * HALO, HALO), :],
                             col_send.at[1 + side], col_recv.at[1 + side], to_a, to_r))
        return made

    def side_totals(side, to_r):
        rows, corners = gs.at[pl.ds(0, HALO + HALO // 2), :], colbuf.at[0, pl.ds(0, 2 * HALO), :]
        return [copy(rows, rows, row_send.at[side], row_recv.at[side], a, to_r),
                copy(corners, corners, col_send.at[1 + side], col_recv.at[1 + side], a, to_r)]

    pl.semaphore_wait(barrier, na * (1 + (r > 0).astype(jnp.int32) + (r < nrad - 1).astype(jnp.int32)) - 1)
    for side in range(2):
        @pl.when(ends[side])
        def _():
            for cp in row_copies(side)[2:]:
                cp.start()
    straight = [copy(pack.at[p], colbuf.at[p, pl.ds(0, fold), :], col_send.at[0], col_recv.at[0], to_a, r)
                for p, to_a in ((0, al), (1, ar))]
    straight_total = copy(pack, pack, col_send.at[0], col_recv.at[0], al, r)
    for cp in straight:
        cp.start()
    for cp in loads[2]:
        cp.wait()
    for side in range(2):
        @pl.when(ends[side])
        def _():
            for cp in row_copies(side)[:2]:
                cp.start()

    spread = one_hot(256, 256, lambda c: 8 * (c % 32) + c // 32)
    halo_spread = one_hot(128, 256, lambda c: jnp.where(
        (c + 2) % 16 < 8, -1, jnp.where((c + 2) % 16 >= 12, -1,
                                        (c // 128) * 16 + (c % 128) // 16 + jnp.where(c % 16 >= 8, 8 * (c % 16 - 8), 8 * (c % 16 - 6) + 32))))

    def split_rows(x, count, put):
        for t in range(tiles):
            parts = [permute(x(slice((4 * t + b) * 256, (4 * t + b) * 256 + 256)), spread) for b in range(4)]
            for half in range(2):
                for g, o in enumerate(transpose4([p[:, half * 128:half * 128 + 128] for p in parts])):
                    put(4 * half + g, t, o)

    def scaled(k, gi, first, last, x):
        return c0[0, gi, first:last] * x if k else x

    def put_own(k):
        def put(gj, t, value):
            stage[k, gj, t, pl.ds(0, h), :] = value
        return put

    for k, x in enumerate((gs, rs)):
        split_rows(lambda cols, x=x: x[:, cols], h, put_own(k))
    for k, dst in enumerate((v0, g0)):
        for gj in range(8):
            for gi in range(8):
                for t in range(tiles):
                    dst[gi, gj, 0:blk, t * 128:t * 128 + 128] = scaled(k, gi, 0, blk, stage[k, gj, t, pl.ds(gi, blk, stride=8), :])
    for k in range(2):
        for gj in range(8):
            for t in range(tiles + 1):
                stage[k, gj, t, pl.ds(h + HALO, 8 * s0 - h - 2 * HALO), :] = jnp.zeros((8 * s0 - h - 2 * HALO, 128), F32)

    for side in range(2):
        @pl.when(ends[1 - side])
        def _():
            for cp in side_totals(side, r + 1 if side == 0 else r - 1):
                cp.wait_recv()
    straight_total.wait_recv()
    announce(0)
    at = (h, 8 * s0 - HALO)
    def put_edges(gj, t, value):
        for k in range(2):
            for side in range(2):
                n = 2 * k + side
                stage[k, gj, t, pl.ds(at[side], HALO), :] = value[n * HALO:(n + 1) * HALO]

    def edge(k, side, cols):
        if k == 0:
            return [jnp.where(ends[1 - side], rowbuf[k, side, :, cols], 0.0)]
        half = HALO // 2
        x = jnp.where(ends[1 - side], rowbuf[k, side, side * half:side * half + half, cols], 0.0)
        return [jnp.zeros_like(x), x] if side else [x, jnp.zeros_like(x)]

    split_rows(lambda cols: jnp.concatenate(sum((edge(k, side, cols) for k in range(2) for side in range(2)), []), axis=0),
               4 * HALO, put_edges)

    def beside(first, count, shift):
        right, left = colbuf[0, pl.ds(first, count), :], colbuf[1, pl.ds(first, count), :]
        return jnp.where(lane((count, 128)) < 32, roll(right, -shift, 1), roll(left, 32 - shift, 1))

    strips = [beside(0, fold, 32 * q) for q in range(4)]
    strips.append(jnp.where(ends[1], beside(fold, HALO, 0), 0.0))
    strips.append(jnp.where(ends[0], beside(fold + HALO, HALO, 96), 0.0))
    strips = jnp.concatenate(strips, axis=0)
    y = permute(strips, halo_spread)
    for k in range(2):
        for gj in range(8):
            piece = roll(y[:, k * 128:k * 128 + 128], -16 * gj - 8, 1)
            stage[k, gj, tiles, pl.ds(0, h + HALO), :] = piece[0:h + HALO]
            stage[k, gj, tiles, pl.ds(at[1], HALO), :] = piece[h + HALO:]
    for k, dst in enumerate((v0, g0)):
        for gj in range(8):
            for gi in range(8):
                for t in range(tiles):
                    dst[gi, gj, blk:s0, t * 128:t * 128 + 128] = scaled(k, gi, blk, s0, stage[k, gj, t, pl.ds(h + gi, s0 - blk, stride=8), :])
                dst[gi, gj, :, lanes:ext] = scaled(k, gi, 0, s0, stage[k, gj, tiles, pl.ds(gi, s0, stride=8), :])

    fine = Grid(v0, g0, c0, 8, 8, False)
    middle = Grid(v1, g1, c1, 4, 4, False)
    coarse = Grid(v2, g2, c2, 2, 2, False)
    window = Grid(v3, None, None, 1, 1, False)

    def into(ref):
        def put(gi, gj, value):
            ref[gi, gj] = value
        return put

    for step in range(2 * PRE):
        fine.half_near(step % 2, 2 * PRE + 1 - step, blk, lanes)

    def put1(gi, gj, value):
        g1[gi, gj, 0:blk, 0:lanes] = wide(c1[0, gi, 0:blk], lanes) * value[0:blk, 0:lanes]
    fine.restrict(tmp_res, tmp_mid, put1, (blk, lanes))

    for side, first in ((0, blk), (1, blk + 8)):
        @pl.when(jnp.logical_not(ends[1 - side]))
        def _():
            g1[:, :, first:first + 8, 0:lanes] = jnp.zeros((4, 4, 8, lanes), F32)
    slot = lane((blk, 128)) // 8
    left_edge = right_edge = None
    for g in range(16):
        lo = roll(g1[g // 4, g % 4, 0:blk, 0:128], 8 * g, 1)
        hi = roll(g1[g // 4, g % 4, 0:blk, lanes - 128:lanes], 8 * g + 8, 1)
        left_edge = lo if g == 0 else jnp.where(slot == g, lo, left_edge)
        right_edge = hi if g == 0 else jnp.where(slot == g, hi, right_edge)
    s1[0] = left_edge
    s1[1] = right_edge

    def copies1(side, to_r):
        first = 0 if side == 0 else blk - 8
        made = [copy(g1.at[:, :, pl.ds(first, 8), pl.ds(0, lanes)], g1.at[:, :, pl.ds(blk + 8 * side, 8), pl.ds(0, lanes)],
                     row1_send.at[side], row1_recv.at[side], a, to_r)]
        for p, to_a in ((0, al), (1, ar)):
            made.append(copy(s1.at[p, pl.ds(first, 8), :], q1.at[p, pl.ds(blk + 8 * side, 8), :],
                             col1_send.at[1 + side], col1_recv.at[1 + side], to_a, to_r))
        return made

    def totals1(side, to_r):
        corners = q1.at[0, pl.ds(0, 16), :]
        return [copies1(side, to_r)[0], copy(corners, corners, col1_send.at[1 + side], col1_recv.at[1 + side], a, to_r)]

    straight1 = [copy(s1.at[p], q1.at[p, pl.ds(0, blk), :], col1_send.at[0], col1_recv.at[0], to_a, r)
                 for p, to_a in ((0, al), (1, ar))]
    straight1_total = copy(s1, s1, col1_send.at[0], col1_recv.at[0], al, r)
    for side in range(2):
        @pl.when(ends[side])
        def _():
            for cp in copies1(side, r - 1 if side == 0 else r + 1)[1:]:
                cp.start()
    for cp in straight1:
        cp.start()
    for side in range(2):
        @pl.when(ends[side])
        def _():
            copies1(side, r - 1 if side == 0 else r + 1)[0].start()
    learn(0)
    for k in range(1, len(reach)):
        announce(k)
        if k < len(reach) - 1:
            learn(k)
    for side in range(2):
        @pl.when(ends[1 - side])
        def _():
            for cp in totals1(side, r + 1 if side == 0 else r - 1):
                cp.wait_recv()
    straight1_total.wait_recv()
    wl = lane((blk + 16, 128))
    sub = lax.broadcasted_iota(jnp.int32, (blk + 16, 128), 0)
    got = jnp.where(sub < blk, 1, jnp.where(sub < blk + 8, nrad - 1 - r, r)) > 0
    strip_r, strip_l = jnp.where(got, q1[0], 0.0), jnp.where(got, q1[1], 0.0)
    for g in range(16):
        g1[g // 4, g % 4, :, lanes:ext] = jnp.where(
            wl < 8, roll(strip_r, -8 * g, 1), jnp.where(wl >= 120, roll(strip_l, 120 - 8 * g, 1), 0.0))
    middle.sweeps(PRE, True)
    middle.restrict(t1, u1, coarse.set_source)
    coarse.sweeps(PRE, True)

    def put3(gi, gj, value):
        wv[...] = value[0:blk, 0:lanes]
    coarse.restrict(t1, u1, put3)

    place = gat.at[a, pl.ds(pl.multiple_of(r * blk, 8), blk), :]
    gat[a, pl.ds(pl.multiple_of(r * blk, 8), blk), :] = wv[...]

    z, core, nz = lax.div(r, 2), lax.rem(r, 2), nrad // 2

    def hand(da, zt):
        to_a = lax.rem(a + da, na)
        return copy(wv, place, all_send, all_recv.at[a, z], to_a, 2 * zt + 1)

    def relay(da, zs):
        from_a = lax.rem(a + na - da, na)
        came = gat.at[from_a, pl.ds(pl.multiple_of(2 * zs * blk, 8), 2 * blk), :]
        return copy(came, came, relay_send.at[1 if da else 0], all_recv.at[from_a, zs], a, r + 1 - 2 * core)

    own = copy(wv, place, all_send, all_recv.at[a, z], a, r + 1 - 2 * core)

    def sent(ref, send):
        copy(ref, ref, send, all_recv.at[0, 0], a, r + 1 - 2 * core).wait_send()

    def each_chip(near_first, do):
        for k in reversed(range(nz)) if near_first else range(nz):
            zt = jnp.where(z < nz // 2, nz - 1 - k, k)
            for da in reversed(range(na)):
                if da:
                    do(da, zt)
                else:
                    pl.when(zt != z)(lambda: do(0, zt))

    def pass_on(da, zs):
        relay(da, zs).wait_recv()
        relay(da, zs).start()

    learn(len(reach) - 1)
    own.start()
    each_chip(False, lambda da, zt: hand(da, zt).start())
    load_table.wait()
    for step in range(2 * PRE):
        fine.half_far(step % 2, 2 * PRE + 1 - step, blk, lanes)

    pl.when(core == 1)(lambda: each_chip(True, pass_on))
    pl.when(core == 0)(lambda: each_chip(True, lambda da, zs: relay(da, zs).wait_recv()))
    own.wait_recv()

    w3 = lanes * na
    q3 = w3 // 4
    for aa in range(na):
        for t in range(tiles):
            rows3[aa * tiles + t] = gat[aa, :, t * 128:t * 128 + 128]
    stacked = jnp.concatenate([jnp.concatenate(
        [rows3[t, pl.ds(gi, nrad, stride=16), :] for t in range(na * tiles)], axis=1) for gi in range(16)], axis=0)
    table3 = one_hot(w3, w3, lambda c: 4 * (c % q3) + c // q3)
    by_group = permute(stacked, table3, 2)
    for gi in range(16):
        for gj in range(4):
            b3[gi, gj] = wide(d3[0, gi], q3) * by_group[gi * nrad:(gi + 1) * nrad, gj * q3:(gj + 1) * q3]

    l3 = Grid(a3, b3, d3, 16, 4, True)
    l4 = Grid(a4, b4, d4, 8, 2, True)
    l5 = Grid(a5, b5, d5, 4, 4, True)
    l6 = Grid(a6, b6, d6, 2, 2, True)
    l3.sweeps(PRE, True)
    l3.restrict(t3, u3, l4.set_source)
    l4.sweeps(PRE, True)
    w5 = w3 // 4
    q5 = w5 // 4
    nat5 = {}

    def put5(gi, gj, value):
        nat5[gi] = value
    l4.restrict(t3, u3, put5)
    x5 = permute(jnp.concatenate([nat5[i] for i in range(4)], axis=0),
                 one_hot(w5, 512, lambda c: 4 * (c % q5) + c // 128), 2)
    for gi in range(4):
        for gj in range(4):
            b5[gi, gj] = d5[0, gi] * x5[gi * nrad:(gi + 1) * nrad, gj * 128:gj * 128 + 128]
    l5.sweeps(PRE, True)
    l5.restrict(tmp_small(t3), tmp_small(u3), l6.set_source)
    l6.sweeps(PRE, True)
    l6.restrict(tmp_small(t3), tmp_small(u3), into(b7))
    a7[0, 0] = apply_operator(b7[0, 0], table7[...], w * na >> 7)
    l7 = Grid(a7, None, None, 1, 1, True)

    l6.add_prolonged(l7, tmp_small(t3), False)
    l6.sweeps(POST, False)
    l5.add_prolonged(l6, tmp_small(t3), False)
    l5.sweeps(POST, False)
    y5 = None
    for gj in range(4):
        x = jnp.concatenate([a5[gi, gj] for gi in range(4)], axis=0)
        r0 = permute(x, one_hot(128, w5, lambda c, gj=gj: jnp.where(c % 4 == gj, c // 4, -1)))
        y5 = r0 if y5 is None else y5 + r0
    for gi in range(4):
        u3[gi, 0] = y5[gi * nrad:(gi + 1) * nrad]
    l4.add_prolonged(Grid(u3, None, None, 4, 1, True), t3, False)
    l4.sweeps(POST, False)
    l3.add_prolonged(l4, t3, False)
    l3.sweeps(POST, False)

    for gj in range(4):
        for t in range(q3 // 128):
            nat3[gj * (q3 // 128) + t, pl.ds(0, 8), :] = jnp.zeros((8, 128), F32)
            nat3[gj * (q3 // 128) + t, pl.ds(8 + 16 * nrad, 8), :] = jnp.zeros((8, 128), F32)
            for gi in range(16):
                nat3[gj * (q3 // 128) + t, pl.ds(8 + gi, nrad, stride=16), :] = a3[gi, gj, :, t * 128:t * 128 + 128]
    begin = pl.multiple_of(r * 16, 8)
    x3 = jnp.concatenate([nat3[t, pl.ds(begin, 32), :] for t in range(w3 // 128)], axis=1)
    x3 = jnp.concatenate([x3[8:24], x3[24:32], x3[0:8]], axis=0)
    y3 = permute(x3, one_hot(w3, w3, lambda c: (c % 4) * q3 + c // 4))
    for aa in range(na):
        wg[aa] = y3[:, aa * lanes:(aa + 1) * lanes]
    v3[0, 0, :, 0:lanes] = wg[a]
    v3[0, 0, :, lanes:ext] = jnp.where(lane((32, 128)) < 64, wg[ar, :, 0:128], wg[al, :, lanes - 128:lanes])

    coarse.add_prolonged(window, t1, True)
    coarse.sweeps(POST, False)
    middle.add_prolonged(coarse, t1, True)
    middle.sweeps(POST, False)
    near_end = lax.broadcasted_iota(jnp.int32, (8, ext), 0) < 4
    fine.add_prolonged(middle, tmp_res, True, lambda x: jnp.concatenate(
        [x[0:blk], jnp.where(near_end, x[blk:blk + 8], x[blk + 8:blk + 16])], axis=0))
    for step in range(2 * POST):
        fine.half_near(step % 2, 2 * POST - step, blk, lanes)

    for gi in range(8):
        for gj in range(8):
            full = fine.coef(4, gi) * (fine.update(gi, gj) - v0[gi, gj])
            for t in range(tiles):
                cols = slice(t * 128, t * 128 + 128)
                sol[gj, t, pl.ds(gi, blk, stride=8), :] = v0[gi, gj, 0:blk, cols]
                resid[gj, t, pl.ds(gi, blk, stride=8), :] = full[0:blk, cols]
    for side in range(2):
        @pl.when(ends[side])
        def _():
            for cp in side_totals(side, r - 1 if side == 0 else r + 1):
                cp.wait_send()
    straight_total.wait_send()
    for side in range(2):
        @pl.when(ends[side])
        def _():
            for cp in totals1(side, r - 1 if side == 0 else r + 1):
                cp.wait_send()
    straight1_total.wait_send()
    sent(gat.at[:, pl.ds(0, nz * blk), :], all_send)

    @pl.when(core == 1)
    def _():
        sent(gat.at[pl.ds(0, na - 1)], relay_send.at[1])
        sent(gat.at[0, pl.ds(0, (nz - 1) * 2 * blk), :], relay_send.at[0])


def join_kernel(grouped_sol, grouped_res, sol, resid, whole, out_sem):
    tiles, h = grouped_sol.shape[1:3]
    join = one_hot(256, 256, lambda c: 32 * (c % 8) + c // 8)
    copies = []
    for k, (x, out) in enumerate(((grouped_sol, sol), (grouped_res, resid))):
        for t in range(tiles):
            halves = [transpose4([x[hf * 4 + p, t] for p in range(4)]) for hf in range(2)]
            for b in range(4):
                cols = pl.ds((4 * t + b) * 256, 256)
                whole[k, :, cols] = permute(jnp.concatenate([halves[0][b], halves[1][b]], axis=1), join, 2)
                copies.append(pltpu.make_async_copy(whole.at[k, :, cols], out.at[:, cols], out_sem.at[k, 4 * t + b]))
                copies[-1].start()
    for cp in copies:
        cp.wait()


def tmp_small(ref):
    return ref.at[:, :, :, 0:128]


def solution(mesh):
    na, nrad = mesh.shape["ang"], mesh.shape["rad"]

    def local(right_side, guess):
        h, w = right_side.shape
        lanes = w // 8
        ext, tiles = lanes + 128, lanes // 128
        blk = h // 8
        s0 = blk + 8
        w3, q3 = lanes * na, lanes * na // 4
        m = lambda *s: pltpu.VMEM(s, F32)
        last = LEVELS - 1
        table = coarsest_operator(h * nrad >> last, w * na >> last, 2.0 * math.pi / (w * na >> last))
        table7 = pltpu.VMEM(table.shape, jnp.bfloat16)
        table = jnp.asarray(np.pad(table, ((0, 0), (0, max(0, 5 * h * w // table.shape[0] - table.shape[1])))))
        scratch = [
            m(h, w), m(h, w), pltpu.SemaphoreType.DMA((2, 3)),
            m(2, 2, HALO, w), m(2, h // 4, 128), m(2, h // 4 + 2 * HALO, 128), m(2, blk, 128), m(2, blk + 16, 128), m(4, 4, 32, ext), m(4, 4, 32, ext),
            m(2, 8, tiles + 1, 8 * s0, 128),
            m(8, 8, s0, ext), m(8, 8, s0, ext), m(6, 8, s0, 128),
            m(4, 4, 32, ext), m(4, 4, 32, ext), m(6, 4, 32, 128),
            m(2, 2, 32, ext), m(2, 2, 32, ext), m(6, 2, 32, 128),
            m(1, 1, 32, ext), m(6, 1, 32, 128),
            m(h // 8, lanes), m(na, 32, lanes), m(8, 8, s0, ext), m(4, 8, s0, ext),
            m(na, nrad * 16, lanes), m(na * tiles, nrad * 16, 128), m(w3 // 128, nrad * 16 + 16, 128),
            m(16, 4, nrad, q3), m(16, 4, nrad, q3), m(6, 16, nrad, 128),
            m(8, 2, nrad, q3), m(8, 2, nrad, q3), m(6, 8, nrad, 128),
            m(4, 4, nrad, 128), m(4, 4, nrad, 128), m(6, 4, nrad, 128),
            m(2, 2, nrad, 128), m(2, 2, nrad, 128), m(6, 2, nrad, 128),
            m(1, 1, nrad, 128), m(1, 1, nrad, 128),
            m(16, 4, nrad, q3), m(8, 4, nrad, q3),
            *[pltpu.SemaphoreType.DMA((n,)) for n in (2, 2, 3, 3, 2, 2, 3, 3)],
            pltpu.SemaphoreType.DMA, pltpu.SemaphoreType.DMA((na, nrad // 2)), pltpu.SemaphoreType.DMA((2,)),
            pltpu.SemaphoreType.REGULAR((max(1, len([k for k in range(nrad.bit_length()) if 2 << k < nrad - 1])), 2)),
            table7, pltpu.SemaphoreType.DMA,
        ]
        grouped = pl.pallas_call(
            lambda *refs: kernel(na, nrad, h, w, *refs),
            out_shape=[jax.ShapeDtypeStruct((8, tiles, h, 128), F32)] * 2,
            in_specs=[pl.BlockSpec(memory_space=pl.ANY)] * 3,
            out_specs=[pl.BlockSpec(memory_space=pltpu.VMEM)] * 2,
            scratch_shapes=scratch,
            compiler_params=pltpu.CompilerParams(has_side_effects=True, collective_id=0, vmem_limit_bytes=53760 * 1024),
        )(right_side, guess, table)
        return pl.pallas_call(
            join_kernel,
            out_shape=[jax.ShapeDtypeStruct((h, w), F32)] * 2,
            in_specs=[pl.BlockSpec(memory_space=pltpu.VMEM)] * 2,
            out_specs=[pl.BlockSpec(memory_space=pl.ANY)] * 2,
            scratch_shapes=[m(2, h, w), pltpu.SemaphoreType.DMA((2, 4 * tiles))],
            compiler_params=pltpu.CompilerParams(vmem_limit_bytes=16 * 1024 * 1024),
        )(*grouped)

    placed = (P("rad", "ang"), P("rad", "ang"))
    return jax.shard_map(local, mesh=mesh, in_specs=placed, out_specs=placed, check_vma=False)
```

```python
import math

import jax
import jax.numpy as jnp
import numpy as np
from jax import lax
from jax.experimental import pallas as pl
from jax.experimental.pallas import tpu as pltpu
from jax.sharding import PartitionSpec as P

LEVELS = 8
PRE = 2
POST = 2
COARSE_SWEEPS = 8
F32 = jnp.float32
MESH = pl.DeviceIdType.MESH
HALO = 16


def one_hot(rows, cols, source):
    r = lax.broadcasted_iota(jnp.int32, (rows, cols), 0)
    c = lax.broadcasted_iota(jnp.int32, (rows, cols), 1)
    return jnp.where(r == source(c), 1.0, 0.0).astype(jnp.bfloat16)


def permute(x, table, count=3):
    rest, parts = x, []
    for k in range(count):
        parts.append(rest.astype(jnp.bfloat16))
        if k < count - 1:
            rest = rest - parts[-1].astype(F32)
    n = x.shape[0]
    y = jnp.dot(jnp.concatenate(parts, axis=0), table, preferred_element_type=F32)
    total = y[:n] + y[n:2 * n]
    return total + y[2 * n:] if count == 3 else total


def wide(c, lanes):
    return jnp.concatenate([c] * (lanes // c.shape[1]), axis=1) if lanes > c.shape[1] else c


def roll(x, shift, axis):
    return pltpu.roll(x, shift % x.shape[axis], axis)


def coarsest_operator(rows, cols, spacing):
    radius = (1.0 + (np.arange(rows) + 0.5) * spacing)[:, None]
    outward, inward, angular = 1.0 + 0.5 * spacing / radius, 1.0 - 0.5 * spacing / radius, 1.0 / (radius * radius)
    colour = (np.arange(rows)[:, None] + np.arange(cols)[None, :]) % 2
    g = np.eye(rows * cols).reshape(-1, rows, cols)
    v = np.zeros_like(g)
    for step in range(2 * COARSE_SWEEPS):
        p = np.pad(v, ((0, 0), (1, 1), (0, 0)))
        new = (g + outward * p[:, 2:] + inward * p[:, :-2] + angular * (np.roll(v, -1, 2) + np.roll(v, 1, 2))) / (2.0 + 2.0 * angular)
        v = np.where(colour == step % 2, new, v)
    rest, parts = v.reshape(rows * cols, rows * cols), []
    for _ in range(3):
        parts.append(rest.astype(np.float32).astype(jnp.bfloat16))
        rest = rest - parts[-1].astype(np.float64)
    return np.concatenate(parts, axis=1)


def apply_operator(x, table, cols):
    rows, per = x.shape[0], 128 // cols
    tiles = table.shape[0] // 128
    s = lax.broadcasted_iota(jnp.int32, x.shape, 0)
    block = lax.broadcasted_iota(jnp.int32, x.shape, 1) // cols
    flat = jnp.concatenate([jnp.where(s == t * per + block, x, 0.0) for t in range(tiles)], axis=1)
    flat = jnp.broadcast_to(jnp.sum(flat, axis=0, keepdims=True), (rows, flat.shape[1]))
    hi = flat.astype(jnp.bfloat16).astype(F32)
    mid = (flat - hi).astype(jnp.bfloat16).astype(F32)
    low = flat - hi - mid
    lhs = [hi, mid, low] + [jnp.zeros_like(low)] * (3 * rows // 8 % 2)
    y = jnp.dot(jnp.concatenate(lhs, axis=0).astype(jnp.bfloat16), table, preferred_element_type=F32)
    out = None
    for t in range(tiles):
        piece = lambda k, m: y[k * rows:(k + 1) * rows, (m * tiles + t) * 128:(m * tiles + t) * 128 + 128]
        total = (piece(0, 2) + piece(1, 1) + piece(2, 0)) + (piece(0, 1) + piece(1, 0)) + piece(0, 0)
        out = total if out is None else jnp.where(s // per == t, total, out)
    turn = (block + per - s % per) % per
    spread = out
    for k in range(1, per):
        spread = jnp.where(turn == k, roll(out, cols * k, 1), spread)
    return spread


def transpose4(xs):
    ln = lax.broadcasted_iota(jnp.int32, xs[0].shape, 1) // 32

    def mix(pick):
        o = pick(0)
        for q in range(1, 4):
            o = jnp.where(ln == q, pick(q), o)
        return o

    turned = [roll(mix(lambda q: xs[(q + s) % 4]), 32 * s, 1) if s else mix(lambda q: xs[q]) for s in range(4)]
    return [mix(lambda p: turned[(p - b) % 4]) for b in range(4)]


class Grid:
    def __init__(self, v, g, c, nr, nc, closed):
        self.v, self.g, self.c, self.nr, self.nc, self.closed = v, g, c, nr, nc, closed

    def rows_shift(self, x, d):
        y = roll(x, -d, 0)
        if self.closed:
            s = lax.broadcasted_iota(jnp.int32, x.shape, 0)
            y = jnp.where(s == (x.shape[0] - 1 if d > 0 else 0), 0.0, y)
        return y

    def up(self, a, gi, gj):
        return a[gi + 1, gj] if gi + 1 < self.nr else self.rows_shift(a[0, gj], 1)

    def down(self, a, gi, gj):
        return a[gi - 1, gj] if gi > 0 else self.rows_shift(a[self.nr - 1, gj], -1)

    def right(self, a, gi, gj):
        return a[gi, gj + 1] if gj + 1 < self.nc else roll(a[gi, 0], -1, 1)

    def left(self, a, gi, gj):
        return a[gi, gj - 1] if gj > 0 else roll(a[gi, self.nc - 1], 1, 1)

    def coef(self, k, gi):
        return wide(self.c[k, gi], self.v.shape[-1])

    def set_source(self, gi, gj, value):
        self.g[gi, gj] = self.coef(0, gi) * value

    def update(self, gi, gj):
        v = self.v
        return (self.g[gi, gj] + self.coef(1, gi) * self.up(v, gi, gj)
                + self.coef(2, gi) * self.down(v, gi, gj)
                + self.coef(3, gi) * (self.right(v, gi, gj) + self.left(v, gi, gj)))

    def extent(self, gi, gj, depth, rows, cols):
        near = lambda i, n: i < depth or i >= n - depth
        return (self.v.shape[2] if near(gi, self.nr) else rows), (self.v.shape[3] if near(gj, self.nc) else cols)

    def half_near(self, parity, depth, rows, cols):
        for gi in range(self.nr):
            for gj in range(self.nc):
                if (gi + gj) % 2 == parity:
                    m, n = self.extent(gi, gj, depth, rows, cols)
                    self.v[gi, gj, 0:m, 0:n] = self.update(gi, gj)[0:m, 0:n]

    def half_far(self, parity, depth, rows, cols):
        full_m, full_n = self.v.shape[2:]
        for gi in range(self.nr):
            for gj in range(self.nc):
                m, n = self.extent(gi, gj, depth, rows, cols)
                if (gi + gj) % 2 == parity and (m < full_m or n < full_n):
                    value = self.update(gi, gj)
                    if m < full_m:
                        self.v[gi, gj, m:full_m, :] = value[m:full_m]
                    if n < full_n:
                        self.v[gi, gj, 0:m, n:full_n] = value[0:m, n:full_n]

    def half(self, parity, first=False):
        for gi in range(self.nr):
            for gj in range(self.nc):
                if (gi + gj) % 2 == parity:
                    if first:
                        self.v[gi, gj] = self.g[gi, gj]
                    else:
                        self.v[gi, gj] = self.update(gi, gj)

    def sweeps(self, count, zero):
        if zero:
            self.half(0, True)
            self.half(1)
            count -= 1

        for _ in range(count):
            self.half(0)
            self.half(1)

    def restrict(self, res, tmp, out, own=None):
        nr, nc = self.nr, self.nc
        size = lambda gi, gj: self.extent(gi, gj, 1, *own) if own else self.v.shape[2:]
        for gi in range(nr):
            for gj in range(nc):
                if (gi + gj) % 2 == 0:
                    m, n = size(gi, gj)
                    res[gi, gj, 0:m, 0:n] = (self.coef(4, gi) * (self.update(gi, gj) - self.v[gi, gj]))[0:m, 0:n]
        for big in range(nr // 2):
            for gj in range(nc):
                if gj % 2 == 0:
                    a, b = 3.0 * res[2 * big, gj], self.up(res, 2 * big + 1, gj)
                else:
                    a, b = 3.0 * res[2 * big + 1, gj], self.down(res, 2 * big, gj)
                m, n = own[0] if own else self.v.shape[2], size(0, gj)[1]
                tmp[big, gj, 0:m, 0:n] = ((a + b) * 0.125)[0:m, 0:n]
        for big in range(nr // 2):
            for col in range(nc // 2):
                inner = 3.0 * (tmp[big, 2 * col] + tmp[big, 2 * col + 1])
                outer = self.left(tmp, big, 2 * col) + self.right(tmp, big, 2 * col + 1)
                out(big, col, (inner + outer) * 0.5)

    def add_prolonged(self, coarse, tmp, mask, fit=lambda x: x):
        e = coarse.v
        for gi in range(self.nr):
            for col in range(coarse.nc):
                near = e[gi // 2, col]
                far = coarse.down(e, gi // 2, col) if gi % 2 == 0 else coarse.up(e, gi // 2, col)
                value = fit(0.75 * near + 0.25 * far)
                if mask:
                    value = value * self.coef(5, gi)
                tmp[gi, col] = value
        for gi in range(self.nr):
            for gj in range(self.nc):
                if (gi + gj) % 2 == 0:
                    continue
                near = tmp[gi, gj // 2]
                far = coarse.left(tmp, gi, gj // 2) if gj % 2 == 0 else coarse.right(tmp, gi, gj // 2)
                self.v[gi, gj] = self.v[gi, gj] + (0.75 * near + 0.25 * far)


def fill_coefficients(c, nr, rows_per_group, start, total, spacing, wrap):
    for gi in range(nr):
        s = lax.broadcasted_iota(jnp.int32, (rows_per_group, 128), 0)
        if wrap:
            s = jnp.where(s >= wrap, s - rows_per_group, s)
        row = start + nr * s + gi
        inside = jnp.logical_and(row >= 0, row < total)
        radius = 1.0 + (jnp.where(inside, row, 0).astype(F32) + 0.5) * spacing
        ratio = 0.5 * spacing / radius
        angular = 1.0 / (radius * radius)
        centre = 2.0 + 2.0 * angular
        zero = jnp.zeros_like(radius)
        for k, value in enumerate((1.0 / centre, (1.0 + ratio) / centre, (1.0 - ratio) / centre,
                                   angular / centre, centre, jnp.ones_like(radius))):
            c[k, gi] = jnp.where(inside, value, zero)


def kernel(na, nrad, h, w, rs_in, gs_in, table_in, sol, resid, rs, gs, load_sem,
           rowbuf, pack, colbuf, s1, q1, t1, u1, stage, v0, g0, c0, v1, g1, c1, v2, g2, c2, v3, c3, wv, wg, tmp_res, tmp_mid,
           gat, rows3, nat3, a3, b3, d3, a4, b4, d4, a5, b5, d5, a6, b6, d6, a7, b7, t3, u3,
           row_send, row_recv, col_send, col_recv, row1_send, row1_recv, col1_send, col1_recv, all_send, all_recv, relay_send, known, table7, table_sem,
           spread, halo_spread, split3, join3, split5, join5):
    a, r = lax.axis_index("ang"), lax.axis_index("rad")
    ar, al = lax.rem(a + 1, na), lax.rem(a + na - 1, na)
    lanes = w // 8
    ext = lanes + 128
    tiles = lanes // 128
    spacing = [2.0 * math.pi / (w * na >> l) for l in range(LEVELS)]
    lane = lambda shape: lax.broadcasted_iota(jnp.int32, shape, 1)

    spans = (pl.ds(0, 128), pl.ds(w - 128, 128), pl.ds(128, w - 256))
    loads = [[pltpu.make_async_copy(src.at[:, cols], dst.at[:, cols], load_sem.at[k, n])
              for k, (src, dst) in enumerate(((gs_in, gs), (rs_in, rs)))] for n, cols in enumerate(spans)]
    for cp in sum(loads, []):
        cp.start()
    load_table = pltpu.make_async_copy(table_in.at[:, 0:table7.shape[1]], table7, table_sem)
    load_table.start()
    blk = h // 8
    s0 = blk + 8
    barrier = pltpu.get_barrier_semaphore()

    ends = (r > 0, r < nrad - 1)

    def greet(to_r, first):
        for da in range(first, na):
            pl.semaphore_signal(barrier, inc=1, device_id=(lax.rem(a + da, na), to_r), device_id_type=MESH)

    for side in range(2):
        @pl.when(ends[side])
        def _():
            greet(r - 1 if side == 0 else r + 1, 0)
    greet(r, 1)
    reach = [2 << k for k in range(nrad.bit_length()) if 2 << k < nrad - 1]

    def announce(k):
        for side, there in ((0, r >= reach[k]), (1, r < nrad - reach[k])):
            @pl.when(there)
            def _():
                to_r = r - reach[k] if side == 0 else r + reach[k]
                pl.semaphore_signal(known.at[k, 1 - side], inc=1, device_id=(a, to_r), device_id_type=MESH)

    def learn(k):
        for side, there in ((0, r >= reach[k]), (1, r < nrad - reach[k])):
            @pl.when(there)
            def _():
                pl.semaphore_wait(known.at[k, side], 1)

    for l, c in ((0, c0), (1, c1), (2, c2)):
        fill_coefficients(c, 8 >> l, s0 if l == 0 else blk + 16, r * (h >> l), (h * nrad) >> l, spacing[l], blk + 4 if l == 0 else blk + 8)
    for l, d, n in ((3, d3, 16), (4, d4, 8), (5, d5, 4), (6, d6, 2)):
        fill_coefficients(d, n, nrad, 0, (h * nrad) >> l, spacing[l], 0)

    for cp in loads[0] + loads[1]:
        cp.wait()

    fold = h // 4
    place16 = lane((fold, 128)) // 16
    for p, (tile, base) in enumerate(((0, 0), (w - 128, 16))):
        folded = None
        for q in range(4):
            for k, x in enumerate((gs, rs)):
                piece = roll(x[q * fold:(q + 1) * fold, tile:tile + 128], 32 * q + 16 * k + base, 1)
                folded = piece if folded is None else jnp.where(place16 == 2 * q + k, piece, folded)
        pack[p] = folded

    def copy(src, dst, send, recv, to_a, to_r):
        return pltpu.make_async_remote_copy(src_ref=src, dst_ref=dst, send_sem=send, recv_sem=recv,
                                            device_id=(to_a, to_r), device_id_type=MESH)

    def row_copies(side):
        to_r = r - 1 if side == 0 else r + 1
        made = [copy(x.at[pl.ds(side * (h - n), n), :], rowbuf.at[k, side, pl.ds(side * (HALO - n), n), :],
                     row_send.at[side], row_recv.at[side], a, to_r) for k, (x, n) in enumerate(((gs, HALO), (rs, HALO // 2)))]
        for p, to_a in ((0, al), (1, ar)):
            made.append(copy(pack.at[p, pl.ds(side * (fold - HALO), HALO), :], colbuf.at[p, pl.ds(fold + side * HALO, HALO), :],
                             col_send.at[1 + side], col_recv.at[1 + side], to_a, to_r))
        return made

    def side_totals(side, to_r):
        rows, corners = gs.at[pl.ds(0, HALO + HALO // 2), :], colbuf.at[0, pl.ds(0, 2 * HALO), :]
        return [copy(rows, rows, row_send.at[side], row_recv.at[side], a, to_r),
                copy(corners, corners, col_send.at[1 + side], col_recv.at[1 + side], a, to_r)]

    pl.semaphore_wait(barrier, na * (1 + (r > 0).astype(jnp.int32) + (r < nrad - 1).astype(jnp.int32)) - 1)
    for side in range(2):
        @pl.when(ends[side])
        def _():
            for cp in row_copies(side)[2:]:
                cp.start()
    straight = [copy(pack.at[p], colbuf.at[p, pl.ds(0, fold), :], col_send.at[0], col_recv.at[0], to_a, r)
                for p, to_a in ((0, al), (1, ar))]
    straight_total = copy(pack, pack, col_send.at[0], col_recv.at[0], al, r)
    for cp in straight:
        cp.start()
    for cp in loads[2]:
        cp.wait()
    for side in range(2):
        @pl.when(ends[side])
        def _():
            for cp in row_copies(side)[:2]:
                cp.start()

    spread[...] = one_hot(256, 256, lambda c: 8 * (c % 32) + c // 32)
    halo_spread[...] = one_hot(128, 256, lambda c: jnp.where(
        (c + 2) % 16 < 8, -1, jnp.where((c + 2) % 16 >= 12, -1,
                                        (c // 128) * 16 + (c % 128) // 16 + jnp.where(c % 16 >= 8, 8 * (c % 16 - 8), 8 * (c % 16 - 6) + 32))))

    def split_rows(x, count, put):
        for t in range(tiles):
            y = permute(jnp.concatenate([x(slice((4 * t + b) * 256, (4 * t + b) * 256 + 256)) for b in range(4)], axis=0), spread[...])
            parts = [y[b * count:(b + 1) * count] for b in range(4)]
            for half in range(2):
                for g, o in enumerate(transpose4([p[:, half * 128:half * 128 + 128] for p in parts])):
                    put(4 * half + g, t, o)

    def scaled(k, gi, first, last, x):
        return c0[0, gi, first:last] * x if k else x

    def put_own(k):
        def put(gj, t, value):
            stage[k, gj, t, pl.ds(0, h), :] = value
        return put

    for k, x in enumerate((gs, rs)):
        split_rows(lambda cols, x=x: x[:, cols], h, put_own(k))
    for k, dst in enumerate((v0, g0)):
        for gj in range(8):
            for gi in range(8):
                for t in range(tiles):
                    dst[gi, gj, 0:blk, t * 128:t * 128 + 128] = scaled(k, gi, 0, blk, stage[k, gj, t, pl.ds(gi, blk, stride=8), :])
    for k in range(2):
        for gj in range(8):
            for t in range(tiles + 1):
                stage[k, gj, t, pl.ds(h + HALO, 8 * s0 - h - 2 * HALO), :] = jnp.zeros((8 * s0 - h - 2 * HALO, 128), F32)

    for side in range(2):
        @pl.when(ends[1 - side])
        def _():
            for cp in side_totals(side, r + 1 if side == 0 else r - 1):
                cp.wait_recv()
    straight_total.wait_recv()
    announce(0)
    at = (h, 8 * s0 - HALO)
    def put_edges(gj, t, value):
        for k in range(2):
            for side in range(2):
                n = 2 * k + side
                stage[k, gj, t, pl.ds(at[side], HALO), :] = value[n * HALO:(n + 1) * HALO]

    def edge(k, side, cols):
        if k == 0:
            return [jnp.where(ends[1 - side], rowbuf[k, side, :, cols], 0.0)]
        half = HALO // 2
        x = jnp.where(ends[1 - side], rowbuf[k, side, side * half:side * half + half, cols], 0.0)
        return [jnp.zeros_like(x), x] if side else [x, jnp.zeros_like(x)]

    split_rows(lambda cols: jnp.concatenate(sum((edge(k, side, cols) for k in range(2) for side in range(2)), []), axis=0),
               4 * HALO, put_edges)

    def beside(first, count, shift):
        right, left = colbuf[0, pl.ds(first, count), :], colbuf[1, pl.ds(first, count), :]
        return jnp.where(lane((count, 128)) < 32, roll(right, -shift, 1), roll(left, 32 - shift, 1))

    strips = [beside(0, fold, 32 * q) for q in range(4)]
    strips.append(jnp.where(ends[1], beside(fold, HALO, 0), 0.0))
    strips.append(jnp.where(ends[0], beside(fold + HALO, HALO, 96), 0.0))
    strips = jnp.concatenate(strips, axis=0)
    y = permute(strips, halo_spread[...])
    for k in range(2):
        for gj in range(8):
            piece = roll(y[:, k * 128:k * 128 + 128], -16 * gj - 8, 1)
            stage[k, gj, tiles, pl.ds(0, h + HALO), :] = piece[0:h + HALO]
            stage[k, gj, tiles, pl.ds(at[1], HALO), :] = piece[h + HALO:]
    for k, dst in enumerate((v0, g0)):
        for gj in range(8):
            for gi in range(8):
                for t in range(tiles):
                    dst[gi, gj, blk:s0, t * 128:t * 128 + 128] = scaled(k, gi, blk, s0, stage[k, gj, t, pl.ds(h + gi, s0 - blk, stride=8), :])
                dst[gi, gj, :, lanes:ext] = scaled(k, gi, 0, s0, stage[k, gj, tiles, pl.ds(gi, s0, stride=8), :])

    fine = Grid(v0, g0, c0, 8, 8, False)
    middle = Grid(v1, g1, c1, 4, 4, False)
    coarse = Grid(v2, g2, c2, 2, 2, False)
    window = Grid(v3, None, None, 1, 1, False)

    def into(ref):
        def put(gi, gj, value):
            ref[gi, gj] = value
        return put

    for step in range(2 * PRE):
        fine.half_near(step % 2, 2 * PRE + 1 - step, blk, lanes)

    def put1(gi, gj, value):
        g1[gi, gj, 0:blk, 0:lanes] = wide(c1[0, gi, 0:blk], lanes) * value[0:blk, 0:lanes]
    fine.restrict(tmp_res, tmp_mid, put1, (blk, lanes))

    for side, first in ((0, blk), (1, blk + 8)):
        @pl.when(jnp.logical_not(ends[1 - side]))
        def _():
            g1[:, :, first:first + 8, 0:lanes] = jnp.zeros((4, 4, 8, lanes), F32)
    slot = lane((blk, 128)) // 8
    left_edge = right_edge = None
    for g in range(16):
        lo = roll(g1[g // 4, g % 4, 0:blk, 0:128], 8 * g, 1)
        hi = roll(g1[g // 4, g % 4, 0:blk, lanes - 128:lanes], 8 * g + 8, 1)
        left_edge = lo if g == 0 else jnp.where(slot == g, lo, left_edge)
        right_edge = hi if g == 0 else jnp.where(slot == g, hi, right_edge)
    s1[0] = left_edge
    s1[1] = right_edge

    def copies1(side, to_r):
        first = 0 if side == 0 else blk - 8
        made = [copy(g1.at[:, :, pl.ds(first, 8), pl.ds(0, lanes)], g1.at[:, :, pl.ds(blk + 8 * side, 8), pl.ds(0, lanes)],
                     row1_send.at[side], row1_recv.at[side], a, to_r)]
        for p, to_a in ((0, al), (1, ar)):
            made.append(copy(s1.at[p, pl.ds(first, 8), :], q1.at[p, pl.ds(blk + 8 * side, 8), :],
                             col1_send.at[1 + side], col1_recv.at[1 + side], to_a, to_r))
        return made

    def totals1(side, to_r):
        corners = q1.at[0, pl.ds(0, 16), :]
        return [copies1(side, to_r)[0], copy(corners, corners, col1_send.at[1 + side], col1_recv.at[1 + side], a, to_r)]

    straight1 = [copy(s1.at[p], q1.at[p, pl.ds(0, blk), :], col1_send.at[0], col1_recv.at[0], to_a, r)
                 for p, to_a in ((0, al), (1, ar))]
    straight1_total = copy(s1, s1, col1_send.at[0], col1_recv.at[0], al, r)
    for side in range(2):
        @pl.when(ends[side])
        def _():
            for cp in copies1(side, r - 1 if side == 0 else r + 1)[1:]:
                cp.start()
    for cp in straight1:
        cp.start()
    for side in range(2):
        @pl.when(ends[side])
        def _():
            copies1(side, r - 1 if side == 0 else r + 1)[0].start()
    w3 = lanes * na
    q3, w5 = w3 // 4, w3 // 4
    q5 = w5 // 4
    split3[...] = one_hot(w3, w3, lambda c: 4 * (c % q3) + c // q3)
    join3[...] = one_hot(w3, w3, lambda c: (c % 4) * q3 + c // 4)
    split5[...] = one_hot(w5, 512, lambda c: 4 * (c % q5) + c // 128)
    for gj in range(4):
        join5[gj] = one_hot(128, w5, lambda c, gj=gj: jnp.where(c % 4 == gj, c // 4, -1))
    learn(0)
    for k in range(1, len(reach)):
        announce(k)
        if k < len(reach) - 1:
            learn(k)
    for side in range(2):
        @pl.when(ends[1 - side])
        def _():
            for cp in totals1(side, r + 1 if side == 0 else r - 1):
                cp.wait_recv()
    straight1_total.wait_recv()
    wl = lane((blk + 16, 128))
    sub = lax.broadcasted_iota(jnp.int32, (blk + 16, 128), 0)
    got = jnp.where(sub < blk, 1, jnp.where(sub < blk + 8, nrad - 1 - r, r)) > 0
    strip_r, strip_l = jnp.where(got, q1[0], 0.0), jnp.where(got, q1[1], 0.0)
    for g in range(16):
        g1[g // 4, g % 4, :, lanes:ext] = jnp.where(
            wl < 8, roll(strip_r, -8 * g, 1), jnp.where(wl >= 120, roll(strip_l, 120 - 8 * g, 1), 0.0))
    middle.sweeps(PRE, True)
    middle.restrict(t1, u1, coarse.set_source)
    coarse.sweeps(PRE, True)

    def put3(gi, gj, value):
        wv[...] = value[0:blk, 0:lanes]
    coarse.restrict(t1, u1, put3)

    place = gat.at[a, pl.ds(pl.multiple_of(r * blk, 8), blk), :]
    gat[a, pl.ds(pl.multiple_of(r * blk, 8), blk), :] = wv[...]

    z, core, nz = lax.div(r, 2), lax.rem(r, 2), nrad // 2

    def hand(da, zt):
        to_a = lax.rem(a + da, na)
        return copy(wv, place, all_send, all_recv.at[a, z], to_a, 2 * zt + 1)

    def relay(da, zs):
        from_a = lax.rem(a + na - da, na)
        came = gat.at[from_a, pl.ds(pl.multiple_of(2 * zs * blk, 8), 2 * blk), :]
        return copy(came, came, relay_send.at[1 if da else 0], all_recv.at[from_a, zs], a, r + 1 - 2 * core)

    own = copy(wv, place, all_send, all_recv.at[a, z], a, r + 1 - 2 * core)

    def sent(ref, send):
        copy(ref, ref, send, all_recv.at[0, 0], a, r + 1 - 2 * core).wait_send()

    def each_chip(near_first, do):
        for k in reversed(range(nz)) if near_first else range(nz):
            zt = jnp.where(z < nz // 2, nz - 1 - k, k)
            for da in reversed(range(na)):
                if da:
                    do(da, zt)
                else:
                    pl.when(zt != z)(lambda: do(0, zt))

    def pass_on(da, zs):
        relay(da, zs).wait_recv()
        relay(da, zs).start()

    learn(len(reach) - 1)
    own.start()
    each_chip(False, lambda da, zt: hand(da, zt).start())
    load_table.wait()
    for step in range(2 * PRE):
        fine.half_far(step % 2, 2 * PRE + 1 - step, blk, lanes)

    pl.when(core == 1)(lambda: each_chip(True, pass_on))
    pl.when(core == 0)(lambda: each_chip(True, lambda da, zs: relay(da, zs).wait_recv()))
    own.wait_recv()

    for aa in range(na):
        for t in range(tiles):
            rows3[aa * tiles + t] = gat[aa, :, t * 128:t * 128 + 128]
    stacked = jnp.concatenate([jnp.concatenate(
        [rows3[t, pl.ds(gi, nrad, stride=16), :] for t in range(na * tiles)], axis=1) for gi in range(16)], axis=0)
    by_group = permute(stacked, split3[...], 2)
    for gi in range(16):
        for gj in range(4):
            b3[gi, gj] = wide(d3[0, gi], q3) * by_group[gi * nrad:(gi + 1) * nrad, gj * q3:(gj + 1) * q3]

    l3 = Grid(a3, b3, d3, 16, 4, True)
    l4 = Grid(a4, b4, d4, 8, 2, True)
    l5 = Grid(a5, b5, d5, 4, 4, True)
    l6 = Grid(a6, b6, d6, 2, 2, True)
    l3.sweeps(PRE, True)
    l3.restrict(t3, u3, l4.set_source)
    l4.sweeps(PRE, True)
    nat5 = {}

    def put5(gi, gj, value):
        nat5[gi] = value
    l4.restrict(t3, u3, put5)
    x5 = permute(jnp.concatenate([nat5[i] for i in range(4)], axis=0),
                 split5[...], 2)
    for gi in range(4):
        for gj in range(4):
            b5[gi, gj] = d5[0, gi] * x5[gi * nrad:(gi + 1) * nrad, gj * 128:gj * 128 + 128]
    l5.sweeps(PRE, True)
    l5.restrict(tmp_small(t3), tmp_small(u3), l6.set_source)
    l6.sweeps(PRE, True)
    l6.restrict(tmp_small(t3), tmp_small(u3), into(b7))
    a7[0, 0] = apply_operator(b7[0, 0], table7[...], w * na >> 7)
    l7 = Grid(a7, None, None, 1, 1, True)

    l6.add_prolonged(l7, tmp_small(t3), False)
    l6.sweeps(POST, False)
    l5.add_prolonged(l6, tmp_small(t3), False)
    l5.sweeps(POST, False)
    y5 = None
    for gj in range(4):
        x = jnp.concatenate([a5[gi, gj] for gi in range(4)], axis=0)
        r0 = permute(x, join5[gj])
        y5 = r0 if y5 is None else y5 + r0
    for gi in range(4):
        u3[gi, 0] = y5[gi * nrad:(gi + 1) * nrad]
    l4.add_prolonged(Grid(u3, None, None, 4, 1, True), t3, False)
    l4.sweeps(POST, False)
    l3.add_prolonged(l4, t3, False)
    l3.sweeps(POST, False)

    for gj in range(4):
        for t in range(q3 // 128):
            nat3[gj * (q3 // 128) + t, pl.ds(0, 8), :] = jnp.zeros((8, 128), F32)
            nat3[gj * (q3 // 128) + t, pl.ds(8 + 16 * nrad, 8), :] = jnp.zeros((8, 128), F32)
            for gi in range(16):
                nat3[gj * (q3 // 128) + t, pl.ds(8 + gi, nrad, stride=16), :] = a3[gi, gj, :, t * 128:t * 128 + 128]
    begin = pl.multiple_of(r * 16, 8)
    x3 = jnp.concatenate([nat3[t, pl.ds(begin, 32), :] for t in range(w3 // 128)], axis=1)
    x3 = jnp.concatenate([x3[8:24], x3[24:32], x3[0:8]], axis=0)
    y3 = permute(x3, join3[...])
    for aa in range(na):
        wg[aa] = y3[:, aa * lanes:(aa + 1) * lanes]
    v3[0, 0, :, 0:lanes] = wg[a]
    v3[0, 0, :, lanes:ext] = jnp.where(lane((32, 128)) < 64, wg[ar, :, 0:128], wg[al, :, lanes - 128:lanes])

    coarse.add_prolonged(window, t1, True)
    coarse.sweeps(POST, False)
    middle.add_prolonged(coarse, t1, True)
    middle.sweeps(POST, False)
    near_end = lax.broadcasted_iota(jnp.int32, (8, ext), 0) < 4
    fine.add_prolonged(middle, tmp_res, True, lambda x: jnp.concatenate(
        [x[0:blk], jnp.where(near_end, x[blk:blk + 8], x[blk + 8:blk + 16])], axis=0))
    for step in range(2 * POST):
        fine.half_near(step % 2, 2 * POST - step, blk, lanes)

    for gi in range(8):
        for gj in range(8):
            full = fine.coef(4, gi) * (fine.update(gi, gj) - v0[gi, gj])
            for t in range(tiles):
                cols = slice(t * 128, t * 128 + 128)
                sol[gj, t, pl.ds(gi, blk, stride=8), :] = v0[gi, gj, 0:blk, cols]
                resid[gj, t, pl.ds(gi, blk, stride=8), :] = full[0:blk, cols]
    for side in range(2):
        @pl.when(ends[side])
        def _():
            for cp in side_totals(side, r - 1 if side == 0 else r + 1):
                cp.wait_send()
    straight_total.wait_send()
    for side in range(2):
        @pl.when(ends[side])
        def _():
            for cp in totals1(side, r - 1 if side == 0 else r + 1):
                cp.wait_send()
    straight1_total.wait_send()
    sent(gat.at[:, pl.ds(0, nz * blk), :], all_send)

    @pl.when(core == 1)
    def _():
        sent(gat.at[pl.ds(0, na - 1)], relay_send.at[1])
        sent(gat.at[0, pl.ds(0, (nz - 1) * 2 * blk), :], relay_send.at[0])


def join_kernel(grouped_sol, grouped_res, sol, resid, whole, out_sem):
    tiles, h = grouped_sol.shape[1:3]
    join = one_hot(256, 256, lambda c: 32 * (c % 8) + c // 8)
    copies = []
    for k, (x, out) in enumerate(((grouped_sol, sol), (grouped_res, resid))):
        for t in range(tiles):
            halves = [transpose4([x[hf * 4 + p, t] for p in range(4)]) for hf in range(2)]
            for b in range(4):
                cols = pl.ds((4 * t + b) * 256, 256)
                whole[k, :, cols] = permute(jnp.concatenate([halves[0][b], halves[1][b]], axis=1), join, 2)
                copies.append(pltpu.make_async_copy(whole.at[k, :, cols], out.at[:, cols], out_sem.at[k, 4 * t + b]))
                copies[-1].start()
    for cp in copies:
        cp.wait()


def tmp_small(ref):
    return ref.at[:, :, :, 0:128]


def solution(mesh):
    na, nrad = mesh.shape["ang"], mesh.shape["rad"]

    def local(right_side, guess):
        h, w = right_side.shape
        lanes = w // 8
        ext, tiles = lanes + 128, lanes // 128
        blk = h // 8
        s0 = blk + 8
        w3, q3 = lanes * na, lanes * na // 4
        m = lambda *s: pltpu.VMEM(s, F32)
        last = LEVELS - 1
        table = coarsest_operator(h * nrad >> last, w * na >> last, 2.0 * math.pi / (w * na >> last))
        table7 = pltpu.VMEM(table.shape, jnp.bfloat16)
        table = jnp.asarray(np.pad(table, ((0, 0), (0, max(0, 5 * h * w // table.shape[0] - table.shape[1])))))
        scratch = [
            m(h, w), m(h, w), pltpu.SemaphoreType.DMA((2, 3)),
            m(2, 2, HALO, w), m(2, h // 4, 128), m(2, h // 4 + 2 * HALO, 128), m(2, blk, 128), m(2, blk + 16, 128), m(4, 4, 32, ext), m(4, 4, 32, ext),
            m(2, 8, tiles + 1, 8 * s0, 128),
            m(8, 8, s0, ext), m(8, 8, s0, ext), m(6, 8, s0, 128),
            m(4, 4, 32, ext), m(4, 4, 32, ext), m(6, 4, 32, 128),
            m(2, 2, 32, ext), m(2, 2, 32, ext), m(6, 2, 32, 128),
            m(1, 1, 32, ext), m(6, 1, 32, 128),
            m(h // 8, lanes), m(na, 32, lanes), m(8, 8, s0, ext), m(4, 8, s0, ext),
            m(na, nrad * 16, lanes), m(na * tiles, nrad * 16, 128), m(w3 // 128, nrad * 16 + 16, 128),
            m(16, 4, nrad, q3), m(16, 4, nrad, q3), m(6, 16, nrad, 128),
            m(8, 2, nrad, q3), m(8, 2, nrad, q3), m(6, 8, nrad, 128),
            m(4, 4, nrad, 128), m(4, 4, nrad, 128), m(6, 4, nrad, 128),
            m(2, 2, nrad, 128), m(2, 2, nrad, 128), m(6, 2, nrad, 128),
            m(1, 1, nrad, 128), m(1, 1, nrad, 128),
            m(16, 4, nrad, q3), m(8, 4, nrad, q3),
            *[pltpu.SemaphoreType.DMA((n,)) for n in (2, 2, 3, 3, 2, 2, 3, 3)],
            pltpu.SemaphoreType.DMA, pltpu.SemaphoreType.DMA((na, nrad // 2)), pltpu.SemaphoreType.DMA((2,)),
            pltpu.SemaphoreType.REGULAR((max(1, len([k for k in range(nrad.bit_length()) if 2 << k < nrad - 1])), 2)),
            table7, pltpu.SemaphoreType.DMA,
            *[pltpu.VMEM(s, jnp.bfloat16) for s in ((256, 256), (128, 256), (w3, w3), (w3, w3), (q3, 512), (4, 128, q3))],
        ]
        grouped = pl.pallas_call(
            lambda *refs: kernel(na, nrad, h, w, *refs),
            out_shape=[jax.ShapeDtypeStruct((8, tiles, h, 128), F32)] * 2,
            in_specs=[pl.BlockSpec(memory_space=pl.ANY)] * 3,
            out_specs=[pl.BlockSpec(memory_space=pltpu.VMEM)] * 2,
            scratch_shapes=scratch,
            compiler_params=pltpu.CompilerParams(has_side_effects=True, collective_id=0, vmem_limit_bytes=53760 * 1024),
        )(right_side, guess, table)
        return pl.pallas_call(
            join_kernel,
            out_shape=[jax.ShapeDtypeStruct((h, w), F32)] * 2,
            in_specs=[pl.BlockSpec(memory_space=pltpu.VMEM)] * 2,
            out_specs=[pl.BlockSpec(memory_space=pl.ANY)] * 2,
            scratch_shapes=[m(2, h, w), pltpu.SemaphoreType.DMA((2, 4 * tiles))],
            compiler_params=pltpu.CompilerParams(vmem_limit_bytes=16 * 1024 * 1024),
        )(*grouped)

    placed = (P("rad", "ang"), P("rad", "ang"))
    return jax.shard_map(local, mesh=mesh, in_specs=placed, out_specs=placed, check_vma=False)
```

```python
import math

import jax
import jax.numpy as jnp
import numpy as np
from jax import lax
from jax.experimental import pallas as pl
from jax.experimental.pallas import tpu as pltpu
from jax.sharding import PartitionSpec as P

LEVELS = 8
PRE = 2
POST = 2
COARSE_SWEEPS = 8
F32 = jnp.float32
MESH = pl.DeviceIdType.MESH
HALO = 16


def one_hot(rows, cols, source):
    r = lax.broadcasted_iota(jnp.int32, (rows, cols), 0)
    c = lax.broadcasted_iota(jnp.int32, (rows, cols), 1)
    return jnp.where(r == source(c), 1.0, 0.0).astype(jnp.bfloat16)


def permute(x, table, count=3):
    rest, parts = x, []
    for k in range(count):
        parts.append(rest.astype(jnp.bfloat16))
        if k < count - 1:
            rest = rest - parts[-1].astype(F32)
    n = x.shape[0]
    y = jnp.dot(jnp.concatenate(parts, axis=0), table, preferred_element_type=F32)
    total = y[:n] + y[n:2 * n]
    return total + y[2 * n:] if count == 3 else total


def wide(c, lanes):
    return jnp.concatenate([c] * (lanes // c.shape[1]), axis=1) if lanes > c.shape[1] else c


def roll(x, shift, axis):
    return pltpu.roll(x, shift % x.shape[axis], axis)


def coarsest_operator(rows, cols, spacing):
    radius = (1.0 + (np.arange(rows) + 0.5) * spacing)[:, None]
    outward, inward, angular = 1.0 + 0.5 * spacing / radius, 1.0 - 0.5 * spacing / radius, 1.0 / (radius * radius)
    colour = (np.arange(rows)[:, None] + np.arange(cols)[None, :]) % 2
    g = np.eye(rows * cols).reshape(-1, rows, cols)
    v = np.zeros_like(g)
    for step in range(2 * COARSE_SWEEPS):
        p = np.pad(v, ((0, 0), (1, 1), (0, 0)))
        new = (g + outward * p[:, 2:] + inward * p[:, :-2] + angular * (np.roll(v, -1, 2) + np.roll(v, 1, 2))) / (2.0 + 2.0 * angular)
        v = np.where(colour == step % 2, new, v)
    rest, parts = v.reshape(rows * cols, rows * cols), []
    for _ in range(3):
        parts.append(rest.astype(np.float32).astype(jnp.bfloat16))
        rest = rest - parts[-1].astype(np.float64)
    return np.concatenate(parts, axis=1)


def apply_operator(x, table, cols):
    rows, per = x.shape[0], 128 // cols
    tiles = table.shape[0] // 128
    s = lax.broadcasted_iota(jnp.int32, x.shape, 0)
    block = lax.broadcasted_iota(jnp.int32, x.shape, 1) // cols
    flat = jnp.concatenate([jnp.where(s == t * per + block, x, 0.0) for t in range(tiles)], axis=1)
    flat = jnp.broadcast_to(jnp.sum(flat, axis=0, keepdims=True), (rows, flat.shape[1]))
    hi = flat.astype(jnp.bfloat16).astype(F32)
    mid = (flat - hi).astype(jnp.bfloat16).astype(F32)
    low = flat - hi - mid
    lhs = [hi, mid, low] + [jnp.zeros_like(low)] * (3 * rows // 8 % 2)
    y = jnp.dot(jnp.concatenate(lhs, axis=0).astype(jnp.bfloat16), table, preferred_element_type=F32)
    out = None
    for t in range(tiles):
        piece = lambda k, m: y[k * rows:(k + 1) * rows, (m * tiles + t) * 128:(m * tiles + t) * 128 + 128]
        total = (piece(0, 2) + piece(1, 1) + piece(2, 0)) + (piece(0, 1) + piece(1, 0)) + piece(0, 0)
        out = total if out is None else jnp.where(s // per == t, total, out)
    turn = (block + per - s % per) % per
    spread = out
    for k in range(1, per):
        spread = jnp.where(turn == k, roll(out, cols * k, 1), spread)
    return spread


def transpose4(xs):
    ln = lax.broadcasted_iota(jnp.int32, xs[0].shape, 1) // 32

    def mix(pick):
        o = pick(0)
        for q in range(1, 4):
            o = jnp.where(ln == q, pick(q), o)
        return o

    turned = [roll(mix(lambda q: xs[(q + s) % 4]), 32 * s, 1) if s else mix(lambda q: xs[q]) for s in range(4)]
    return [mix(lambda p: turned[(p - b) % 4]) for b in range(4)]


class Grid:
    def __init__(self, v, g, c, nr, nc, closed):
        self.v, self.g, self.c, self.nr, self.nc, self.closed = v, g, c, nr, nc, closed

    def rows_shift(self, x, d):
        y = roll(x, -d, 0)
        if self.closed:
            s = lax.broadcasted_iota(jnp.int32, x.shape, 0)
            y = jnp.where(s == (x.shape[0] - 1 if d > 0 else 0), 0.0, y)
        return y

    def up(self, a, gi, gj):
        return a[gi + 1, gj] if gi + 1 < self.nr else self.rows_shift(a[0, gj], 1)

    def down(self, a, gi, gj):
        return a[gi - 1, gj] if gi > 0 else self.rows_shift(a[self.nr - 1, gj], -1)

    def right(self, a, gi, gj):
        return a[gi, gj + 1] if gj + 1 < self.nc else roll(a[gi, 0], -1, 1)

    def left(self, a, gi, gj):
        return a[gi, gj - 1] if gj > 0 else roll(a[gi, self.nc - 1], 1, 1)

    def coef(self, k, gi):
        return wide(self.c[k, gi], self.v.shape[-1])

    def set_source(self, gi, gj, value):
        self.g[gi, gj] = self.coef(0, gi) * value

    def update(self, gi, gj):
        v = self.v
        return (self.g[gi, gj] + self.coef(1, gi) * self.up(v, gi, gj)
                + self.coef(2, gi) * self.down(v, gi, gj)
                + self.coef(3, gi) * (self.right(v, gi, gj) + self.left(v, gi, gj)))

    def extent(self, gi, gj, depth, rows, cols):
        near = lambda i, n: i < depth or i >= n - depth
        return (self.v.shape[2] if near(gi, self.nr) else rows), (self.v.shape[3] if near(gj, self.nc) else cols)

    def half_near(self, parity, depth, rows, cols):
        for gi in range(self.nr):
            for gj in range(self.nc):
                if (gi + gj) % 2 == parity:
                    m, n = self.extent(gi, gj, depth, rows, cols)
                    self.v[gi, gj, 0:m, 0:n] = self.update(gi, gj)[0:m, 0:n]

    def half_far(self, parity, depth, rows, cols):
        full_m, full_n = self.v.shape[2:]
        for gi in range(self.nr):
            for gj in range(self.nc):
                m, n = self.extent(gi, gj, depth, rows, cols)
                if (gi + gj) % 2 == parity and (m < full_m or n < full_n):
                    value = self.update(gi, gj)
                    if m < full_m:
                        self.v[gi, gj, m:full_m, :] = value[m:full_m]
                    if n < full_n:
                        self.v[gi, gj, 0:m, n:full_n] = value[0:m, n:full_n]

    def half(self, parity, first=False):
        for gi in range(self.nr):
            for gj in range(self.nc):
                if (gi + gj) % 2 == parity:
                    if first:
                        self.v[gi, gj] = self.g[gi, gj]
                    else:
                        self.v[gi, gj] = self.update(gi, gj)

    def sweeps(self, count, zero):
        if zero:
            self.half(0, True)
            self.half(1)
            count -= 1

        for _ in range(count):
            self.half(0)
            self.half(1)

    def restrict(self, res, tmp, out, own=None):
        nr, nc = self.nr, self.nc
        size = lambda gi, gj: self.extent(gi, gj, 1, *own) if own else self.v.shape[2:]
        for gi in range(nr):
            for gj in range(nc):
                if (gi + gj) % 2 == 0:
                    m, n = size(gi, gj)
                    res[gi, gj, 0:m, 0:n] = (self.coef(4, gi) * (self.update(gi, gj) - self.v[gi, gj]))[0:m, 0:n]
        for big in range(nr // 2):
            for gj in range(nc):
                if gj % 2 == 0:
                    a, b = 3.0 * res[2 * big, gj], self.up(res, 2 * big + 1, gj)
                else:
                    a, b = 3.0 * res[2 * big + 1, gj], self.down(res, 2 * big, gj)
                m, n = own[0] if own else self.v.shape[2], size(0, gj)[1]
                tmp[big, gj, 0:m, 0:n] = ((a + b) * 0.125)[0:m, 0:n]
        for big in range(nr // 2):
            for col in range(nc // 2):
                inner = 3.0 * (tmp[big, 2 * col] + tmp[big, 2 * col + 1])
                outer = self.left(tmp, big, 2 * col) + self.right(tmp, big, 2 * col + 1)
                out(big, col, (inner + outer) * 0.5)

    def add_prolonged(self, coarse, tmp, mask, fit=lambda x: x):
        e = coarse.v
        for gi in range(self.nr):
            for col in range(coarse.nc):
                near = e[gi // 2, col]
                far = coarse.down(e, gi // 2, col) if gi % 2 == 0 else coarse.up(e, gi // 2, col)
                value = fit(0.75 * near + 0.25 * far)
                if mask:
                    value = value * self.coef(5, gi)
                tmp[gi, col] = value
        for gi in range(self.nr):
            for gj in range(self.nc):
                if (gi + gj) % 2 == 0:
                    continue
                near = tmp[gi, gj // 2]
                far = coarse.left(tmp, gi, gj // 2) if gj % 2 == 0 else coarse.right(tmp, gi, gj // 2)
                self.v[gi, gj] = self.v[gi, gj] + (0.75 * near + 0.25 * far)


def fill_coefficients(c, nr, rows_per_group, start, total, spacing, wrap):
    for gi in range(nr):
        s = lax.broadcasted_iota(jnp.int32, (rows_per_group, 128), 0)
        if wrap:
            s = jnp.where(s >= wrap, s - rows_per_group, s)
        row = start + nr * s + gi
        inside = jnp.logical_and(row >= 0, row < total)
        radius = 1.0 + (jnp.where(inside, row, 0).astype(F32) + 0.5) * spacing
        ratio = 0.5 * spacing / radius
        angular = 1.0 / (radius * radius)
        centre = 2.0 + 2.0 * angular
        zero = jnp.zeros_like(radius)
        for k, value in enumerate((1.0 / centre, (1.0 + ratio) / centre, (1.0 - ratio) / centre,
                                   angular / centre, centre, jnp.ones_like(radius))):
            c[k, gi] = jnp.where(inside, value, zero)


def kernel(na, nrad, h, w, rs_in, gs_in, table_in, sol, resid, rs, gs, load_sem,
           rowbuf, pack, colbuf, s1, q1, t1, u1, stage, v0, g0, c0, v1, g1, c1, v2, g2, c2, v3, c3, wv, wg, tmp_res, tmp_mid,
           gat, rows3, nat3, a3, b3, d3, a4, b4, d4, a5, b5, d5, a6, b6, d6, a7, b7, t3, u3,
           row_send, row_recv, col_send, col_recv, row1_send, row1_recv, col1_send, col1_recv, all_send, all_recv, relay_send, known, table7, table_sem,
           spread, halo_spread, split3, join3, split5, join5):
    a, r = lax.axis_index("ang"), lax.axis_index("rad")
    ar, al = lax.rem(a + 1, na), lax.rem(a + na - 1, na)
    lanes = w // 8
    ext = lanes + 128
    tiles = lanes // 128
    spacing = [2.0 * math.pi / (w * na >> l) for l in range(LEVELS)]
    lane = lambda shape: lax.broadcasted_iota(jnp.int32, shape, 1)

    spans = (pl.ds(0, 128), pl.ds(w - 128, 128), pl.ds(128, w - 256))
    loads = [[pltpu.make_async_copy(src.at[:, cols], dst.at[:, cols], load_sem.at[k + 1 if n == 2 else 0])
              for k, (src, dst) in enumerate(((gs_in, gs), (rs_in, rs)))] for n, cols in enumerate(spans)]
    for cp in sum(loads, []):
        cp.start()
    load_table = pltpu.make_async_copy(table_in.at[:, 0:table7.shape[1]], table7, table_sem)
    load_table.start()
    blk = h // 8
    s0 = blk + 8
    barrier = pltpu.get_barrier_semaphore()

    ends = (r > 0, r < nrad - 1)

    def greet(to_r, first):
        for da in range(first, na):
            pl.semaphore_signal(barrier, inc=1, device_id=(lax.rem(a + da, na), to_r), device_id_type=MESH)

    for side in range(2):
        @pl.when(ends[side])
        def _():
            greet(r - 1 if side == 0 else r + 1, 0)
    greet(r, 1)
    reach = [2 << k for k in range(nrad.bit_length()) if 2 << k < nrad - 1]

    def announce(k):
        for side, there in ((0, r >= reach[k]), (1, r < nrad - reach[k])):
            @pl.when(there)
            def _():
                to_r = r - reach[k] if side == 0 else r + reach[k]
                pl.semaphore_signal(known.at[k, 1 - side], inc=1, device_id=(a, to_r), device_id_type=MESH)

    def learn(k):
        for side, there in ((0, r >= reach[k]), (1, r < nrad - reach[k])):
            @pl.when(there)
            def _():
                pl.semaphore_wait(known.at[k, side], 1)

    for l, c in ((0, c0), (1, c1), (2, c2)):
        fill_coefficients(c, 8 >> l, s0 if l == 0 else blk + 16, r * (h >> l), (h * nrad) >> l, spacing[l], blk + 4 if l == 0 else blk + 8)
    for l, d, n in ((3, d3, 16), (4, d4, 8), (5, d5, 4), (6, d6, 2)):
        fill_coefficients(d, n, nrad, 0, (h * nrad) >> l, spacing[l], 0)

    pltpu.make_async_copy(gs_in.at[:, 0:512], gs.at[:, 0:512], load_sem.at[0]).wait()

    fold = h // 4
    place16 = lane((fold, 128)) // 16
    for p, (tile, base) in enumerate(((0, 0), (w - 128, 16))):
        folded = None
        for q in range(4):
            for k, x in enumerate((gs, rs)):
                piece = roll(x[q * fold:(q + 1) * fold, tile:tile + 128], 32 * q + 16 * k + base, 1)
                folded = piece if folded is None else jnp.where(place16 == 2 * q + k, piece, folded)
        pack[p] = folded

    def copy(src, dst, send, recv, to_a, to_r):
        return pltpu.make_async_remote_copy(src_ref=src, dst_ref=dst, send_sem=send, recv_sem=recv,
                                            device_id=(to_a, to_r), device_id_type=MESH)

    def row_copies(side):
        to_r = r - 1 if side == 0 else r + 1
        made = [copy(x.at[pl.ds(side * (h - n), n), :], rowbuf.at[k, side, pl.ds(side * (HALO - n), n), :],
                     row_send.at[side], row_recv.at[side], a, to_r) for k, (x, n) in enumerate(((gs, HALO), (rs, HALO // 2)))]
        for p, to_a in ((0, al), (1, ar)):
            made.append(copy(pack.at[p, pl.ds(side * (fold - HALO), HALO), :], colbuf.at[p, pl.ds(fold + side * HALO, HALO), :],
                             col_send.at[1 + side], col_recv.at[1 + side], to_a, to_r))
        return made

    def side_totals(side, to_r):
        rows, corners = gs.at[pl.ds(0, HALO + HALO // 2), :], colbuf.at[0, pl.ds(0, 2 * HALO), :]
        return [copy(rows, rows, row_send.at[side], row_recv.at[side], a, to_r),
                copy(corners, corners, col_send.at[1 + side], col_recv.at[1 + side], a, to_r)]

    pl.semaphore_wait(barrier, na * (1 + (r > 0).astype(jnp.int32) + (r < nrad - 1).astype(jnp.int32)) - 1)
    for side in range(2):
        @pl.when(ends[side])
        def _():
            for cp in row_copies(side)[2:]:
                cp.start()
    straight = [copy(pack.at[p], colbuf.at[p, pl.ds(0, fold), :], col_send.at[0], col_recv.at[0], to_a, r)
                for p, to_a in ((0, al), (1, ar))]
    straight_total = copy(pack, pack, col_send.at[0], col_recv.at[0], al, r)
    for cp in straight:
        cp.start()
    for cp in loads[2]:
        cp.wait()
    for side in range(2):
        @pl.when(ends[side])
        def _():
            for cp in row_copies(side)[:2]:
                cp.start()

    spread[...] = one_hot(256, 256, lambda c: 8 * (c % 32) + c // 32)
    halo_spread[...] = one_hot(128, 256, lambda c: jnp.where(
        (c + 2) % 16 < 8, -1, jnp.where((c + 2) % 16 >= 12, -1,
                                        (c // 128) * 16 + (c % 128) // 16 + jnp.where(c % 16 >= 8, 8 * (c % 16 - 8), 8 * (c % 16 - 6) + 32))))

    def split_rows(x, count, put):
        for t in range(tiles):
            y = permute(jnp.concatenate([x(slice((4 * t + b) * 256, (4 * t + b) * 256 + 256)) for b in range(4)], axis=0), spread[...])
            parts = [y[b * count:(b + 1) * count] for b in range(4)]
            for half in range(2):
                for g, o in enumerate(transpose4([p[:, half * 128:half * 128 + 128] for p in parts])):
                    put(4 * half + g, t, o)

    def scaled(k, gi, first, last, x):
        return c0[0, gi, first:last] * x if k else x

    def put_own(k):
        def put(gj, t, value):
            stage[k, gj, t, pl.ds(0, h), :] = value
        return put

    for k, x in enumerate((gs, rs)):
        split_rows(lambda cols, x=x: x[:, cols], h, put_own(k))
    for k, dst in enumerate((v0, g0)):
        for gj in range(8):
            for gi in range(8):
                for t in range(tiles):
                    dst[gi, gj, 0:blk, t * 128:t * 128 + 128] = scaled(k, gi, 0, blk, stage[k, gj, t, pl.ds(gi, blk, stride=8), :])
    for k in range(2):
        for gj in range(8):
            for t in range(tiles + 1):
                stage[k, gj, t, pl.ds(h + HALO, 8 * s0 - h - 2 * HALO), :] = jnp.zeros((8 * s0 - h - 2 * HALO, 128), F32)

    for side in range(2):
        @pl.when(ends[1 - side])
        def _():
            for cp in side_totals(side, r + 1 if side == 0 else r - 1):
                cp.wait_recv()
    straight_total.wait_recv()
    announce(0)
    at = (h, 8 * s0 - HALO)
    def put_edges(gj, t, value):
        for k in range(2):
            for side in range(2):
                n = 2 * k + side
                stage[k, gj, t, pl.ds(at[side], HALO), :] = value[n * HALO:(n + 1) * HALO]

    def edge(k, side, cols):
        if k == 0:
            return [jnp.where(ends[1 - side], rowbuf[k, side, :, cols], 0.0)]
        half = HALO // 2
        x = jnp.where(ends[1 - side], rowbuf[k, side, side * half:side * half + half, cols], 0.0)
        return [jnp.zeros_like(x), x] if side else [x, jnp.zeros_like(x)]

    split_rows(lambda cols: jnp.concatenate(sum((edge(k, side, cols) for k in range(2) for side in range(2)), []), axis=0),
               4 * HALO, put_edges)

    def beside(first, count, shift):
        right, left = colbuf[0, pl.ds(first, count), :], colbuf[1, pl.ds(first, count), :]
        return jnp.where(lane((count, 128)) < 32, roll(right, -shift, 1), roll(left, 32 - shift, 1))

    strips = [beside(0, fold, 32 * q) for q in range(4)]
    strips.append(jnp.where(ends[1], beside(fold, HALO, 0), 0.0))
    strips.append(jnp.where(ends[0], beside(fold + HALO, HALO, 96), 0.0))
    strips = jnp.concatenate(strips, axis=0)
    y = permute(strips, halo_spread[...])
    for k in range(2):
        for gj in range(8):
            piece = roll(y[:, k * 128:k * 128 + 128], -16 * gj - 8, 1)
            stage[k, gj, tiles, pl.ds(0, h + HALO), :] = piece[0:h + HALO]
            stage[k, gj, tiles, pl.ds(at[1], HALO), :] = piece[h + HALO:]
    for k, dst in enumerate((v0, g0)):
        for gj in range(8):
            for gi in range(8):
                for t in range(tiles):
                    dst[gi, gj, blk:s0, t * 128:t * 128 + 128] = scaled(k, gi, blk, s0, stage[k, gj, t, pl.ds(h + gi, s0 - blk, stride=8), :])
                dst[gi, gj, :, lanes:ext] = scaled(k, gi, 0, s0, stage[k, gj, tiles, pl.ds(gi, s0, stride=8), :])

    fine = Grid(v0, g0, c0, 8, 8, False)
    middle = Grid(v1, g1, c1, 4, 4, False)
    coarse = Grid(v2, g2, c2, 2, 2, False)
    window = Grid(v3, None, None, 1, 1, False)

    def into(ref):
        def put(gi, gj, value):
            ref[gi, gj] = value
        return put

    for step in range(2 * PRE):
        fine.half_near(step % 2, 2 * PRE + 1 - step, blk, lanes)

    def put1(gi, gj, value):
        g1[gi, gj, 0:blk, 0:lanes] = wide(c1[0, gi, 0:blk], lanes) * value[0:blk, 0:lanes]
    fine.restrict(tmp_res, tmp_mid, put1, (blk, lanes))

    for side, first in ((0, blk), (1, blk + 8)):
        @pl.when(jnp.logical_not(ends[1 - side]))
        def _():
            g1[:, :, first:first + 8, 0:lanes] = jnp.zeros((4, 4, 8, lanes), F32)
    slot = lane((blk, 128)) // 8
    left_edge = right_edge = None
    for g in range(16):
        lo = roll(g1[g // 4, g % 4, 0:blk, 0:128], 8 * g, 1)
        hi = roll(g1[g // 4, g % 4, 0:blk, lanes - 128:lanes], 8 * g + 8, 1)
        left_edge = lo if g == 0 else jnp.where(slot == g, lo, left_edge)
        right_edge = hi if g == 0 else jnp.where(slot == g, hi, right_edge)
    s1[0] = left_edge
    s1[1] = right_edge

    def copies1(side, to_r):
        first = 0 if side == 0 else blk - 8
        made = [copy(g1.at[:, :, pl.ds(first, 8), pl.ds(0, lanes)], g1.at[:, :, pl.ds(blk + 8 * side, 8), pl.ds(0, lanes)],
                     row1_send.at[side], row1_recv.at[side], a, to_r)]
        for p, to_a in ((0, al), (1, ar)):
            made.append(copy(s1.at[p, pl.ds(first, 8), :], q1.at[p, pl.ds(blk + 8 * side, 8), :],
                             col1_send.at[1 + side], col1_recv.at[1 + side], to_a, to_r))
        return made

    def totals1(side, to_r):
        corners = q1.at[0, pl.ds(0, 16), :]
        return [copies1(side, to_r)[0], copy(corners, corners, col1_send.at[1 + side], col1_recv.at[1 + side], a, to_r)]

    straight1 = [copy(s1.at[p], q1.at[p, pl.ds(0, blk), :], col1_send.at[0], col1_recv.at[0], to_a, r)
                 for p, to_a in ((0, al), (1, ar))]
    straight1_total = copy(s1, s1, col1_send.at[0], col1_recv.at[0], al, r)
    for side in range(2):
        @pl.when(ends[side])
        def _():
            for cp in copies1(side, r - 1 if side == 0 else r + 1)[1:]:
                cp.start()
    for cp in straight1:
        cp.start()
    for side in range(2):
        @pl.when(ends[side])
        def _():
            copies1(side, r - 1 if side == 0 else r + 1)[0].start()
    w3 = lanes * na
    q3, w5 = w3 // 4, w3 // 4
    q5 = w5 // 4
    split3[...] = one_hot(w3, w3, lambda c: 4 * (c % q3) + c // q3)
    join3[...] = one_hot(w3, w3, lambda c: (c % 4) * q3 + c // 4)
    split5[...] = one_hot(w5, 512, lambda c: 4 * (c % q5) + c // 128)
    for gj in range(4):
        join5[gj] = one_hot(128, w5, lambda c, gj=gj: jnp.where(c % 4 == gj, c // 4, -1))
    learn(0)
    for k in range(1, len(reach)):
        announce(k)
        if k < len(reach) - 1:
            learn(k)
    for side in range(2):
        @pl.when(ends[1 - side])
        def _():
            for cp in totals1(side, r + 1 if side == 0 else r - 1):
                cp.wait_recv()
    straight1_total.wait_recv()
    wl = lane((blk + 16, 128))
    sub = lax.broadcasted_iota(jnp.int32, (blk + 16, 128), 0)
    got = jnp.where(sub < blk, 1, jnp.where(sub < blk + 8, nrad - 1 - r, r)) > 0
    strip_r, strip_l = jnp.where(got, q1[0], 0.0), jnp.where(got, q1[1], 0.0)
    for g in range(16):
        g1[g // 4, g % 4, :, lanes:ext] = jnp.where(
            wl < 8, roll(strip_r, -8 * g, 1), jnp.where(wl >= 120, roll(strip_l, 120 - 8 * g, 1), 0.0))
    middle.sweeps(PRE, True)
    middle.restrict(t1, u1, coarse.set_source)
    coarse.sweeps(PRE, True)

    def put3(gi, gj, value):
        wv[...] = value[0:blk, 0:lanes]
    coarse.restrict(t1, u1, put3)

    place = gat.at[a, pl.ds(pl.multiple_of(r * blk, 8), blk), :]
    gat[a, pl.ds(pl.multiple_of(r * blk, 8), blk), :] = wv[...]

    z, core, nz = lax.div(r, 2), lax.rem(r, 2), nrad // 2

    def hand(da, zt):
        to_a = lax.rem(a + da, na)
        return copy(wv, place, all_send, all_recv.at[a, z], to_a, 2 * zt + 1)

    def relay(da, zs):
        from_a = lax.rem(a + na - da, na)
        came = gat.at[from_a, pl.ds(pl.multiple_of(2 * zs * blk, 8), 2 * blk), :]
        return copy(came, came, relay_send.at[1 if da else 0], all_recv.at[from_a, zs], a, r + 1 - 2 * core)

    own = copy(wv, place, all_send, all_recv.at[a, z], a, r + 1 - 2 * core)

    def sent(ref, send):
        copy(ref, ref, send, all_recv.at[0, 0], a, r + 1 - 2 * core).wait_send()

    def each_chip(near_first, do):
        for k in reversed(range(nz)) if near_first else range(nz):
            zt = jnp.where(z < nz // 2, nz - 1 - k, k)
            for da in reversed(range(na)):
                if da:
                    do(da, zt)
                else:
                    pl.when(zt != z)(lambda: do(0, zt))

    def pass_on(da, zs):
        relay(da, zs).wait_recv()
        relay(da, zs).start()

    learn(len(reach) - 1)
    own.start()
    each_chip(False, lambda da, zt: hand(da, zt).start())
    load_table.wait()
    for step in range(2 * PRE):
        fine.half_far(step % 2, 2 * PRE + 1 - step, blk, lanes)

    pl.when(core == 1)(lambda: each_chip(True, pass_on))
    pl.when(core == 0)(lambda: each_chip(True, lambda da, zs: relay(da, zs).wait_recv()))
    own.wait_recv()

    for aa in range(na):
        for t in range(tiles):
            rows3[aa * tiles + t] = gat[aa, :, t * 128:t * 128 + 128]
    stacked = jnp.concatenate([jnp.concatenate(
        [rows3[t, pl.ds(gi, nrad, stride=16), :] for t in range(na * tiles)], axis=1) for gi in range(16)], axis=0)
    by_group = permute(stacked, split3[...], 2)
    for gi in range(16):
        for gj in range(4):
            b3[gi, gj] = wide(d3[0, gi], q3) * by_group[gi * nrad:(gi + 1) * nrad, gj * q3:(gj + 1) * q3]

    l3 = Grid(a3, b3, d3, 16, 4, True)
    l4 = Grid(a4, b4, d4, 8, 2, True)
    l5 = Grid(a5, b5, d5, 4, 4, True)
    l6 = Grid(a6, b6, d6, 2, 2, True)
    l3.sweeps(PRE, True)
    l3.restrict(t3, u3, l4.set_source)
    l4.sweeps(PRE, True)
    nat5 = {}

    def put5(gi, gj, value):
        nat5[gi] = value
    l4.restrict(t3, u3, put5)
    x5 = permute(jnp.concatenate([nat5[i] for i in range(4)], axis=0),
                 split5[...], 2)
    for gi in range(4):
        for gj in range(4):
            b5[gi, gj] = d5[0, gi] * x5[gi * nrad:(gi + 1) * nrad, gj * 128:gj * 128 + 128]
    l5.sweeps(PRE, True)
    l5.restrict(tmp_small(t3), tmp_small(u3), l6.set_source)
    l6.sweeps(PRE, True)
    l6.restrict(tmp_small(t3), tmp_small(u3), into(b7))
    a7[0, 0] = apply_operator(b7[0, 0], table7[...], w * na >> 7)
    l7 = Grid(a7, None, None, 1, 1, True)

    l6.add_prolonged(l7, tmp_small(t3), False)
    l6.sweeps(POST, False)
    l5.add_prolonged(l6, tmp_small(t3), False)
    l5.sweeps(POST, False)
    y5 = None
    for gj in range(4):
        x = jnp.concatenate([a5[gi, gj] for gi in range(4)], axis=0)
        r0 = permute(x, join5[gj])
        y5 = r0 if y5 is None else y5 + r0
    for gi in range(4):
        u3[gi, 0] = y5[gi * nrad:(gi + 1) * nrad]
    l4.add_prolonged(Grid(u3, None, None, 4, 1, True), t3, False)
    l4.sweeps(POST, False)
    l3.add_prolonged(l4, t3, False)
    l3.sweeps(POST, False)

    for gj in range(4):
        for t in range(q3 // 128):
            nat3[gj * (q3 // 128) + t, pl.ds(0, 8), :] = jnp.zeros((8, 128), F32)
            nat3[gj * (q3 // 128) + t, pl.ds(8 + 16 * nrad, 8), :] = jnp.zeros((8, 128), F32)
            for gi in range(16):
                nat3[gj * (q3 // 128) + t, pl.ds(8 + gi, nrad, stride=16), :] = a3[gi, gj, :, t * 128:t * 128 + 128]
    begin = pl.multiple_of(r * 16, 8)
    x3 = jnp.concatenate([nat3[t, pl.ds(begin, 32), :] for t in range(w3 // 128)], axis=1)
    x3 = jnp.concatenate([x3[8:24], x3[24:32], x3[0:8]], axis=0)
    y3 = permute(x3, join3[...])
    for aa in range(na):
        wg[aa] = y3[:, aa * lanes:(aa + 1) * lanes]
    v3[0, 0, :, 0:lanes] = wg[a]
    v3[0, 0, :, lanes:ext] = jnp.where(lane((32, 128)) < 64, wg[ar, :, 0:128], wg[al, :, lanes - 128:lanes])

    coarse.add_prolonged(window, t1, True)
    coarse.sweeps(POST, False)
    middle.add_prolonged(coarse, t1, True)
    middle.sweeps(POST, False)
    near_end = lax.broadcasted_iota(jnp.int32, (8, ext), 0) < 4
    fine.add_prolonged(middle, tmp_res, True, lambda x: jnp.concatenate(
        [x[0:blk], jnp.where(near_end, x[blk:blk + 8], x[blk + 8:blk + 16])], axis=0))
    for step in range(2 * POST):
        fine.half_near(step % 2, 2 * POST - step, blk, lanes)

    for gi in range(8):
        for gj in range(8):
            full = fine.coef(4, gi) * (fine.update(gi, gj) - v0[gi, gj])
            for t in range(tiles):
                cols = slice(t * 128, t * 128 + 128)
                sol[gj, t, pl.ds(gi, blk, stride=8), :] = v0[gi, gj, 0:blk, cols]
                resid[gj, t, pl.ds(gi, blk, stride=8), :] = full[0:blk, cols]
    for side in range(2):
        @pl.when(ends[side])
        def _():
            for cp in side_totals(side, r - 1 if side == 0 else r + 1):
                cp.wait_send()
    straight_total.wait_send()
    for side in range(2):
        @pl.when(ends[side])
        def _():
            for cp in totals1(side, r - 1 if side == 0 else r + 1):
                cp.wait_send()
    straight1_total.wait_send()
    sent(gat.at[:, pl.ds(0, nz * blk), :], all_send)

    @pl.when(core == 1)
    def _():
        sent(gat.at[pl.ds(0, na - 1)], relay_send.at[1])
        sent(gat.at[0, pl.ds(0, (nz - 1) * 2 * blk), :], relay_send.at[0])


def join_kernel(grouped_sol, grouped_res, sol, resid, whole, out_sem):
    tiles, h = grouped_sol.shape[1:3]
    join = one_hot(256, 256, lambda c: 32 * (c % 8) + c // 8)
    copies = []
    for k, (x, out) in enumerate(((grouped_sol, sol), (grouped_res, resid))):
        for t in range(tiles):
            halves = [transpose4([x[hf * 4 + p, t] for p in range(4)]) for hf in range(2)]
            for b in range(4):
                cols = pl.ds((4 * t + b) * 256, 256)
                whole[k, :, cols] = permute(jnp.concatenate([halves[0][b], halves[1][b]], axis=1), join, 2)
                copies.append(pltpu.make_async_copy(whole.at[k, :, cols], out.at[:, cols], out_sem.at[k, 4 * t + b]))
                copies[-1].start()
    for cp in copies:
        cp.wait()


def tmp_small(ref):
    return ref.at[:, :, :, 0:128]


def solution(mesh):
    na, nrad = mesh.shape["ang"], mesh.shape["rad"]

    def local(right_side, guess):
        h, w = right_side.shape
        lanes = w // 8
        ext, tiles = lanes + 128, lanes // 128
        blk = h // 8
        s0 = blk + 8
        w3, q3 = lanes * na, lanes * na // 4
        m = lambda *s: pltpu.VMEM(s, F32)
        last = LEVELS - 1
        table = coarsest_operator(h * nrad >> last, w * na >> last, 2.0 * math.pi / (w * na >> last))
        table7 = pltpu.VMEM(table.shape, jnp.bfloat16)
        table = jnp.asarray(np.pad(table, ((0, 0), (0, max(0, 5 * h * w // table.shape[0] - table.shape[1])))))
        scratch = [
            m(h, w), m(h, w), pltpu.SemaphoreType.DMA((3,)),
            m(2, 2, HALO, w), m(2, h // 4, 128), m(2, h // 4 + 2 * HALO, 128), m(2, blk, 128), m(2, blk + 16, 128), m(4, 4, 32, ext), m(4, 4, 32, ext),
            m(2, 8, tiles + 1, 8 * s0, 128),
            m(8, 8, s0, ext), m(8, 8, s0, ext), m(6, 8, s0, 128),
            m(4, 4, 32, ext), m(4, 4, 32, ext), m(6, 4, 32, 128),
            m(2, 2, 32, ext), m(2, 2, 32, ext), m(6, 2, 32, 128),
            m(1, 1, 32, ext), m(6, 1, 32, 128),
            m(h // 8, lanes), m(na, 32, lanes), m(8, 8, s0, ext), m(4, 8, s0, ext),
            m(na, nrad * 16, lanes), m(na * tiles, nrad * 16, 128), m(w3 // 128, nrad * 16 + 16, 128),
            m(16, 4, nrad, q3), m(16, 4, nrad, q3), m(6, 16, nrad, 128),
            m(8, 2, nrad, q3), m(8, 2, nrad, q3), m(6, 8, nrad, 128),
            m(4, 4, nrad, 128), m(4, 4, nrad, 128), m(6, 4, nrad, 128),
            m(2, 2, nrad, 128), m(2, 2, nrad, 128), m(6, 2, nrad, 128),
            m(1, 1, nrad, 128), m(1, 1, nrad, 128),
            m(16, 4, nrad, q3), m(8, 4, nrad, q3),
            *[pltpu.SemaphoreType.DMA((n,)) for n in (2, 2, 3, 3, 2, 2, 3, 3)],
            pltpu.SemaphoreType.DMA, pltpu.SemaphoreType.DMA((na, nrad // 2)), pltpu.SemaphoreType.DMA((2,)),
            pltpu.SemaphoreType.REGULAR((max(1, len([k for k in range(nrad.bit_length()) if 2 << k < nrad - 1])), 2)),
            table7, pltpu.SemaphoreType.DMA,
            *[pltpu.VMEM(s, jnp.bfloat16) for s in ((256, 256), (128, 256), (w3, w3), (w3, w3), (q3, 512), (4, 128, q3))],
        ]
        grouped = pl.pallas_call(
            lambda *refs: kernel(na, nrad, h, w, *refs),
            out_shape=[jax.ShapeDtypeStruct((8, tiles, h, 128), F32)] * 2,
            in_specs=[pl.BlockSpec(memory_space=pl.ANY)] * 3,
            out_specs=[pl.BlockSpec(memory_space=pltpu.VMEM)] * 2,
            scratch_shapes=scratch,
            compiler_params=pltpu.CompilerParams(has_side_effects=True, collective_id=0, vmem_limit_bytes=53760 * 1024),
        )(right_side, guess, table)
        return pl.pallas_call(
            join_kernel,
            out_shape=[jax.ShapeDtypeStruct((h, w), F32)] * 2,
            in_specs=[pl.BlockSpec(memory_space=pltpu.VMEM)] * 2,
            out_specs=[pl.BlockSpec(memory_space=pl.ANY)] * 2,
            scratch_shapes=[m(2, h, w), pltpu.SemaphoreType.DMA((2, 4 * tiles))],
            compiler_params=pltpu.CompilerParams(vmem_limit_bytes=16 * 1024 * 1024),
        )(*grouped)

    placed = (P("rad", "ang"), P("rad", "ang"))
    return jax.shard_map(local, mesh=mesh, in_specs=placed, out_specs=placed, check_vma=False)
```
